256 devices in a mesh: band: 16 (over x_hi, z), grid: 16 (over y, x_lo, core).
Axes of the slice: x: 4 (x_hi: 2, x_lo: 2; x = x_hi * 2 + x_lo), y: 4, z: 8, core: 2. Of those that a mesh axis runs over, the one named last changes fastest.
Arguments:
- partial_density: float32 [16, 128, 128, 128], P('band', 'grid'), may hold values from 0.01 to 1
- node_index: int32 [128, 128, 128], P('grid'), may hold values from 0 to 19
- node_weight: float32 [4, 128, 128, 128], P(None, 'grid'), may hold values from 0 to 1
- node_slope: float32 [4, 128, 128, 128], P(None, 'grid'), may hold values from -6 to 6
- kernel_table: float32 [20, 20, 114], replicated, may hold values from -0.8 to 0.8, as said below
Outputs:
- potential: float32 [128, 128, 128], P('grid')
The draws below stay inside these ranges and needn't reach their ends.
Inputs may be any that keep to these rules, and one draw needn't show every extreme that they name: node_index(r) is the node at the lower end of the interval of q0 at r; nodes node_index - 1 to node_index + 2 carry the four weights. `kernel_table`: symmetric in its first two indices.
All inputs are finite; a program needn't handle non-finite values.
Results may differ from the reference program's by a relative error of at most 0.0003.
Values sent between devices are 32-bit elements; how exact they have to be, the bound alone decides.
A program may use at most 64 MiB of HBM per device.

```python
import math
import jax
import jax.numpy as jnp
from jax import lax

N = 128
NA = 20
SHELLS = 114
GROUPS = 16


def draw_kernel_table(key, part):
    sample_values = jax.random.truncated_normal(key, -4.0, 4.0, (NA, NA, SHELLS), jnp.float32) * 0.2
    symmetric = 0.5 * (sample_values + jnp.transpose(sample_values, (1, 0, 2)))
    return symmetric


def touch_ends(array, own_key, least, largest):
    place = [jax.random.randint(jax.random.fold_in(own_key, axis), (), 0, length) for axis, length in enumerate(array.shape)]
    widest = array.shape.index(max(array.shape))
    next_to = place[:widest] + [(place[widest] + 1) % array.shape[widest]] + place[widest + 1:]
    return array.at[tuple(place)].set(least).at[tuple(next_to)].set(largest)


def block_scale(own_key, extent, split, smallest, high):
    level = 1.0
    for position, parts in split:
        steps = jax.random.uniform(jax.random.fold_in(jax.random.fold_in(own_key, 6), position), (parts,), jnp.float32, smallest / len(split), high / len(split))
        level = level * jnp.repeat(jnp.exp(steps), extent[position] // parts).reshape((-1,) + (1,) * (len(extent) - 1 - position))
    return level


def noise(key, shape, width, reach, pieces=(), kind=jnp.bfloat16):
    drawn = width * jax.random.normal(key, shape, jnp.float32)
    if pieces:
        drawn = drawn * block_scale(key, shape, pieces, -0.22, 0.18)
    return jnp.clip(drawn, -reach, reach).astype(kind)


def setup_inputs(seed: int = 0) -> dict:
    seeds = jax.random.split(jax.random.key(seed), 6)
    partial_density = jnp.clip(jnp.exp(math.log(1.0) - 4.6051702 * jax.random.uniform(seeds[0], (GROUPS, N, N, N), jnp.float32) ** block_scale(seeds[0], (GROUPS, N, N, N), ((0, 16), (1, 16)), -0.2, 0.2)), 0.01, 1.0)
    node_index = touch_ends(jax.random.randint(seeds[1], (N, N, N), 0, NA), jax.random.fold_in(seeds[1], 1), 0, NA - 1).astype(jnp.int32)
    node_weight = jnp.clip(1.0 * jax.random.uniform(seeds[2], (4, N, N, N), jnp.float32) ** block_scale(seeds[2], (4, N, N, N), ((1, 16),), -0.2, 0.2), 0.0, 1.0)
    node_slope = noise(seeds[3], (4, N, N, N), 1.0, 6.0, ((1, 16),), jnp.float32)
    kernel_table = draw_kernel_table(jax.random.fold_in(seeds[5], 71), 0)
    return {"partial_density": partial_density, "node_index": node_index, "node_weight": node_weight, "node_slope": node_slope, "kernel_table": kernel_table}


def frequency(length):
    positions = jnp.arange(length, dtype=jnp.int32)
    return jnp.where(positions < length // 2, positions, positions - length)

def shell_split(square_norm):
    root_value = jnp.sqrt(square_norm.astype(jnp.float32))
    shell_idx = root_value.astype(jnp.int32)
    shell_idx = shell_idx - (shell_idx * shell_idx > square_norm).astype(jnp.int32)
    shell_idx = shell_idx + ((shell_idx + 1) * (shell_idx + 1) <= square_norm).astype(jnp.int32)
    fraction = root_value - shell_idx.astype(jnp.float32)
    return (shell_idx, fraction)

def node_fields(count_nodes, intervals, weights):
    node_ids = jnp.arange(count_nodes, dtype=jnp.int32)
    summed = jnp.zeros((count_nodes,) + intervals.shape, jnp.float32)
    for offset in range(4):
        matched = node_ids[:, None, None, None] == (intervals + (offset - 1))[None]
        summed = summed + jnp.where(matched, weights[offset][None], jnp.zeros((), jnp.float32))
    return summed

def reference(partial_density, node_index, node_weight, node_slope, kernel_table):
    density = lax.optimization_barrier(jnp.sum(partial_density, axis=0))
    theta_fields = density[None] * node_fields(NA, node_index, node_weight)
    spectrum = jnp.fft.fftn(theta_fields, axes=(1, 2, 3))
    spec_real = jnp.real(spectrum)
    spec_imag = jnp.imag(spectrum)
    freq_all = frequency(N)
    plane_norm = freq_all[:, None] * freq_all[:, None] + freq_all[None, :] * freq_all[None, :]

    def mix_plane(plane_idx):
        freq_x = freq_all[plane_idx]
        shell_idx, fraction = shell_split(plane_norm + freq_x * freq_x)
        lower_values = kernel_table[:, :, shell_idx]
        upper_values = kernel_table[:, :, shell_idx + 1]
        kernel = (1.0 - fraction) * lower_values + fraction * upper_values
        plane_real = lax.dynamic_index_in_dim(spec_real, plane_idx, 1, keepdims=False)
        plane_imag = lax.dynamic_index_in_dim(spec_imag, plane_idx, 1, keepdims=False)
        out_real = jnp.einsum('abyz,ayz->byz', kernel, plane_real, precision=lax.Precision.HIGHEST)
        out_imag = jnp.einsum('abyz,ayz->byz', kernel, plane_imag, precision=lax.Precision.HIGHEST)
        return (out_real, out_imag)
    mixed_real, mixed_imag = lax.map(mix_plane, jnp.arange(N, dtype=jnp.int32))
    mixed = jnp.moveaxis(mixed_real + 1j * mixed_imag, 0, 1)
    fields = jnp.real(jnp.fft.ifftn(mixed, axes=(1, 2, 3)))
    return lax.optimization_barrier(jnp.sum(fields * node_fields(NA, node_index, node_slope), axis=0))
```

```python
import functools

import jax
import jax.numpy as jnp
import numpy as np
from jax import lax
from jax.experimental import pallas as pl
from jax.experimental.pallas import tpu as pltpu
from jax.sharding import PartitionSpec as P

N = 128
NA = 20
CHUNKS = 5
F32 = jnp.float32
BF16 = jnp.bfloat16


def halves(table):
    table = np.asarray(table, np.float32)
    high = table.astype(BF16)
    low = (table - high.astype(np.float32)).astype(BF16)
    return high, low


def lane_wave():
    lane = np.arange(128)
    bit = [(lane >> b) & 1 for b in range(7)]
    owner = bit[6] * 8 + bit[5] * 4 + bit[2] * 2 + bit[1]
    plane = bit[4] * 2 + bit[3]
    return owner * 4 + plane, bit[0]


def z_tables():
    wave, part = lane_wave()
    z = np.arange(N)
    angle = 2 * np.pi * ((z[:, None] * wave[None]) % N) / N
    sign = np.where(z % 2 == 0, 1.0, -1.0)[:, None]
    forward = np.where(part == 0, np.cos(angle), np.where(wave == 0, sign, -np.sin(angle)))
    twice = np.where(part == 0, 2 * np.cos(angle), -2 * np.sin(angle))
    back = np.where(wave == 0, forward, twice).T / float(N) ** 3

    def packed(table):
        high, low = halves(table)
        return np.block([[high, low], [high, np.zeros_like(low)]])

    return packed(forward), packed(back)


def wave_tables():
    k = np.arange(N)
    angle = 2 * np.pi * ((k[:, None] * k[None]) % N) / N
    cos, sin = np.cos(angle), np.sin(angle)
    forward = np.zeros((2, N, 2, N))
    forward[0, :, 0] = cos
    forward[0, :, 1] = sin
    forward[1, :, 0] = -sin
    forward[1, :, 1] = cos
    packed = np.zeros((2, N, 2, N))
    lower, upper = (k > 0) & (k < 64), k > 64
    ends = (k == 0) | (k == 64)
    for rows, part in ((lower, 0), (upper, 1)):
        packed[0, rows, part] = cos[rows]
        packed[1, rows, part] = -sin[rows]
    packed[0, ends, 0] = cos[ends]
    packed[1, ends, 1] = cos[ends]
    back = np.zeros((2, N, 2, N))
    back[0, :, 0] = cos
    back[0, :, 1] = -sin
    back[1, :, 0] = sin
    back[1, :, 1] = cos
    unpacked = np.zeros((2, N, 2, N))
    for cols, part in ((lower, 0), (upper, 1)):
        unpacked[part][:, 0, cols] = 2 * cos[:, cols]
        unpacked[part][:, 1, cols] = -2 * sin[:, cols]
    unpacked[0][:, 0, ends] = cos[:, ends]
    unpacked[1][:, 1, ends] = cos[:, ends]
    return forward, packed, back, unpacked


def left_form(table):
    return table.reshape(2, 16, 8, 2, 16, 8).transpose(1, 0, 2, 4, 3, 5).reshape(256, 256)


def right_form(table):
    return table.reshape(256, 256).T


def tables():
    z_forward, z_back = z_tables()
    forward, packed, back, unpacked = wave_tables()
    y_forward = np.stack(halves(np.concatenate([left_form(forward), left_form(packed)])))
    y_back = np.stack(halves(np.concatenate([left_form(back), left_form(unpacked)])))
    x_forward = np.stack([np.stack(halves(right_form(t))) for t in (forward, packed)])
    x_back = np.stack([np.stack(halves(right_form(t))) for t in (back, unpacked)])
    return z_forward, z_back, y_forward, y_back, x_forward, x_back


def split(value):
    high = value.astype(BF16)
    low = (value - high.astype(F32)).astype(BF16)
    return high, low


def mm(a, b):
    return jnp.dot(a, b, preferred_element_type=F32)


def lanes_of(shape):
    return lax.broadcasted_iota(jnp.int32, shape, len(shape) - 1)


def exchange(v, pairs):
    count = v.shape[0]
    for index_bit, lane_bit in pairs:
        inner, step = 1 << index_bit, 1 << lane_bit
        rows = count // 2 * 8
        w = v.reshape(count // (2 * inner), 2, inner, 8, 128)
        a = w[:, 0].reshape(rows, 128)
        b = w[:, 1].reshape(rows, 128)
        keep = (lanes_of((rows, 128)) >> lane_bit) & 1 == 0
        new_a = jnp.where(keep, a, pltpu.roll(b, step, 1))
        new_b = jnp.where(keep, pltpu.roll(a, 128 - step, 1), b)
        shape = (count // (2 * inner), 1, inner, 8, 128)
        v = jnp.concatenate([new_a.reshape(shape), new_b.reshape(shape)], axis=1).reshape(count, 8, 128)
    return v


Z_PAIRS = ((4, 6), (3, 5), (2, 2), (1, 1), (0, 0))
X_PAIRS = ((3, 6), (2, 5), (1, 4), (0, 3))


def node_coefficient(node, index, weights):
    total = None
    for offset in range(4):
        term = jnp.where(index + (offset - 1) == node, weights[offset], 0.0)
        total = term if total is None else total + term
    return total


def z_forward_chunk(density, index, weights, table, chunk):
    fields = [density * node_coefficient(4 * chunk + i, index, weights) for i in range(4)]
    theta = jnp.concatenate(fields, axis=0).reshape(256, 128)
    high, low = split(theta)
    wide = mm(jnp.concatenate([high, low], axis=1), table)
    waves = (wide[:, :128] + wide[:, 128:]).reshape(32, 8, 128)
    return exchange(waves, Z_PAIRS).reshape(16, 2, 8, 128)


def z_back_chunk(block, index, slopes, table, chunk):
    waves = exchange(block.reshape(32, 8, 128), Z_PAIRS).reshape(256, 128)
    high, low = split(waves)
    wide = mm(jnp.concatenate([high, low], axis=1), table)
    field = (wide[:, :128] + wide[:, 128:]).reshape(4, 8, 8, 128)
    total = None
    for i in range(4):
        term = field[i] * node_coefficient(4 * chunk + i, index, slopes)
        total = term if total is None else total + term
    return total


def y_chunk(block, table):
    high, low = split(block.reshape(256, 128))
    wide = mm(table[0], jnp.concatenate([high, low], axis=1))
    both = wide[:, :128] + wide[:, 128:] + mm(table[1], high)
    at = lanes_of((256, 128))
    mask = ((at >> 3) & 3 == 0) & (lax.axis_index("band") == 0)
    return jnp.where(mask, both[256:], both[:256]).reshape(16, 2, 8, 128)


def x_waves(rows, table):
    high, low = split(rows)
    count = rows.shape[0]
    wide = mm(jnp.concatenate([high, low], axis=0), table[0])
    return wide[:count] + wide[count:] + mm(high, table[1])


def x_mixed_waves(rows, table):
    general = x_waves(rows, table[0]).reshape(4, 4, 8, 256)
    first = rows.reshape(4, 4, 8, 256)[:, 0].reshape(32, 256)
    packed = x_waves(first, table[1]).reshape(4, 1, 8, 256)
    sub = lax.broadcasted_iota(jnp.int32, (4, 1, 8, 256), 2)
    at = lax.axis_index("grid")
    special = (sub == 0) & (lax.axis_index("band") == 0) & (lax.rem(at, 8) == 0)
    return jnp.concatenate([jnp.where(special, packed, general[:, :1]), general[:, 1:]], axis=1)


def x_forward_chunk(block, table):
    parts = [exchange(block[:, c], X_PAIRS).reshape(128, 128) for c in range(2)]
    return x_mixed_waves(jnp.concatenate(parts, axis=1), table)


def x_back_chunk(waves, table):
    out = x_mixed_waves(waves.reshape(128, 256), table).reshape(128, 256)
    parts = [exchange(out[:, 128 * c : 128 * c + 128].reshape(16, 8, 128), X_PAIRS) for c in range(2)]
    return jnp.concatenate([part[:, None] for part in parts], axis=1)


def shell_tile(plane, row):
    band, grid = lax.axis_index("band"), lax.axis_index("grid")
    own = jnp.where(plane == 4, 0, plane)
    kz = 4 * band + own
    ky = 8 * grid + row
    fy = jnp.where(ky < 64, ky, ky - 128)
    kx = lanes_of((128, 128))
    fx = jnp.where(kx < 64, kx, kx - 128)
    packed = (band == 0) & (own == 0)
    ends = (ky == 0) | (ky == 64)
    by_row = packed & (ky > 64)
    by_lane = (kx > 64) | (((kx == 0) | (kx == 64)) & (plane == 4))
    last = by_row | (packed & ends & by_lane)
    norm = jnp.where(last, 64 * 64, kz * kz) + fy * fy + fx * fx
    root = jnp.sqrt(norm.astype(F32))
    shell = lax.broadcasted_iota(jnp.int32, (128, 128), 0).astype(F32)
    return jnp.maximum(1.0 - jnp.abs(root - shell), 0.0)


def make_phi(kernel_high, kernel_low, phi):
    wide = jnp.concatenate([kernel_high, kernel_low], axis=1)

    def step(i, carry):
        plane, row = i // 8, i % 8
        high, low = split(shell_tile(plane, row))
        values = mm(wide, jnp.concatenate([high, high], axis=0)) + mm(kernel_high, low)
        phi[pl.ds(plane * 3200 + row, 400, stride=8), :] = values
        return carry

    lax.fori_loop(0, 40, step, 0)


def mix(phi, spec, mixed):
    for half in range(2):
        for plane in range(4):

            def add(a, carry):
                real, imag = carry
                at = a * 160 + half * 80
                kernel = phi[pl.ds(plane * 3200 + at, 80), :].reshape(10, 8, 128)
                other = kernel
                if plane == 0:
                    other = phi[pl.ds(4 * 3200 + at, 80), :].reshape(10, 8, 128)
                wave = spec[a, plane]
                real = real + kernel * wave[:, :128][None]
                imag = imag + other * wave[:, 128:][None]
                return real, imag

            zero = jnp.zeros((10, 8, 128), F32)
            real, imag = lax.fori_loop(0, NA, add, (zero, zero))
            mixed[pl.ds(half * 10, 10), plane] = jnp.concatenate([real, imag], axis=2)


def kernel_z_forward(parts, index, weights, table, out):
    density = jnp.sum(parts[...], axis=0)

    def step(chunk, carry):
        out[:, chunk] = z_forward_chunk(density, index[...], [weights[i] for i in range(4)], table[...], chunk)
        return carry

    lax.fori_loop(0, CHUNKS, step, 0)


def kernel_y(block, table, out):
    def step(chunk, carry):
        out[:, chunk] = y_chunk(block[:, chunk], table)
        return carry

    lax.fori_loop(0, CHUNKS, step, 0)


def kernel_x(block, kernel_high, kernel_low, forward, back, out, phi, spec, mixed):
    make_phi(kernel_high[...], kernel_low[...], phi)

    def step(chunk, carry):
        spec[pl.ds(4 * chunk, 4)] = x_forward_chunk(block[:, chunk], forward)
        return carry

    lax.fori_loop(0, CHUNKS, step, 0)
    mix(phi, spec, mixed)

    def step_back(chunk, carry):
        out[:, chunk] = x_back_chunk(mixed[pl.ds(4 * chunk, 4)], back)
        return carry

    lax.fori_loop(0, CHUNKS, step_back, 0)


def kernel_z_back(block, index, slopes, table, out):
    def step(chunk, total):
        return total + z_back_chunk(block[:, chunk], index[...], [slopes[i] for i in range(4)], table[...], chunk)

    out[...] = lax.fori_loop(0, CHUNKS, step, jnp.zeros((8, 8, 128), F32))


def run(kernel, shape, *args, scratch=()):
    return pl.pallas_call(
        kernel,
        out_shape=jax.ShapeDtypeStruct(shape, F32),
        scratch_shapes=list(scratch),
        compiler_params=pltpu.CompilerParams(vmem_limit_bytes=60000 * 1024),
    )(*args)


BLOCKS = (16, CHUNKS, 2, 8, 128)


def swap(x, axis):
    return lax.all_to_all(x, axis, 0, 0, tiled=True)


def per_device(partial_density, node_index, node_weight, node_slope, kernel_table):
    z_forward, z_back, y_forward, y_back, x_forward, x_back = [jnp.asarray(t) for t in tables()]
    band = lax.axis_index("band")
    rows = 8 * band
    index = lax.dynamic_slice_in_dim(node_index, rows, 8, 1)
    weights = lax.dynamic_slice_in_dim(node_weight, rows, 8, 2)
    slopes = lax.dynamic_slice_in_dim(node_slope, rows, 8, 2)
    wide_table = jnp.pad(kernel_table.reshape(400, -1), ((0, 0), (0, 128 - kernel_table.shape[2])))
    kernel_high = lax.reduce_precision(wide_table, 8, 7)
    kernel_low = (wide_table - kernel_high).astype(BF16)
    kernel_high = kernel_high.astype(BF16)
    parts = swap(partial_density[0].reshape(8, 16, 8, 128).transpose(1, 0, 2, 3), "band")
    sent = run(kernel_z_forward, BLOCKS, parts, index, weights, z_forward)
    sent = run(kernel_y, BLOCKS, swap(sent, "band"), y_forward)
    sent = run(
        kernel_x, BLOCKS, swap(sent, "grid"), kernel_high, kernel_low, x_forward, x_back,
        scratch=(pltpu.VMEM((16000, 128), F32), pltpu.VMEM((NA, 4, 8, 256), F32), pltpu.VMEM((NA, 4, 8, 256), F32)),
    )
    sent = run(kernel_y, BLOCKS, swap(sent, "grid"), y_back)
    own = run(kernel_z_back, (8, 8, 128), swap(sent, "band"), index, slopes, z_back)
    whole = lax.all_gather(own, "band", axis=0)
    return whole.transpose(1, 0, 2, 3).reshape(8, 128, 128)


def solution(mesh):
    placed = (
        P("band", "grid", None, None),
        P("grid", None, None),
        P(None, "grid", None, None),
        P(None, "grid", None, None),
        P(),
    )
    return jax.shard_map(
        per_device, mesh=mesh, in_specs=placed, out_specs=P("grid", None, None), check_vma=False
    )
```

```python
import functools

import jax
import jax.numpy as jnp
import numpy as np
from jax import lax
from jax.experimental import pallas as pl
from jax.experimental.pallas import tpu as pltpu
from jax.sharding import PartitionSpec as P

N = 128
NA = 20
CHUNKS = 5
F32 = jnp.float32
BF16 = jnp.bfloat16


def halves(table):
    table = np.asarray(table, np.float32)
    high = table.astype(BF16)
    low = (table - high.astype(np.float32)).astype(BF16)
    return high, low


def lane_wave():
    lane = np.arange(128)
    bit = [(lane >> b) & 1 for b in range(7)]
    owner = bit[6] * 8 + bit[5] * 4 + bit[2] * 2 + bit[1]
    plane = bit[4] * 2 + bit[3]
    return owner * 4 + plane, bit[0]


def z_tables():
    wave, part = lane_wave()
    z = np.arange(N)
    angle = 2 * np.pi * ((z[:, None] * wave[None]) % N) / N
    sign = np.where(z % 2 == 0, 1.0, -1.0)[:, None]
    forward = np.where(part == 0, np.cos(angle), np.where(wave == 0, sign, -np.sin(angle)))
    twice = np.where(part == 0, 2 * np.cos(angle), -2 * np.sin(angle))
    back = np.where(wave == 0, forward, twice).T / float(N) ** 3

    def packed(table):
        high, low = halves(table)
        return np.block([[high, low], [high, np.zeros_like(low)]])

    return packed(forward), packed(back)


def wave_tables():
    k = np.arange(N)
    angle = 2 * np.pi * ((k[:, None] * k[None]) % N) / N
    cos, sin = np.cos(angle), np.sin(angle)
    forward = np.zeros((2, N, 2, N))
    forward[0, :, 0] = cos
    forward[0, :, 1] = sin
    forward[1, :, 0] = -sin
    forward[1, :, 1] = cos
    packed = np.zeros((2, N, 2, N))
    lower, upper = (k > 0) & (k < 64), k > 64
    ends = (k == 0) | (k == 64)
    for rows, part in ((lower, 0), (upper, 1)):
        packed[0, rows, part] = cos[rows]
        packed[1, rows, part] = -sin[rows]
    packed[0, ends, 0] = cos[ends]
    packed[1, ends, 1] = cos[ends]
    back = np.zeros((2, N, 2, N))
    back[0, :, 0] = cos
    back[0, :, 1] = -sin
    back[1, :, 0] = sin
    back[1, :, 1] = cos
    unpacked = np.zeros((2, N, 2, N))
    for cols, part in ((lower, 0), (upper, 1)):
        unpacked[part][:, 0, cols] = 2 * cos[:, cols]
        unpacked[part][:, 1, cols] = -2 * sin[:, cols]
    unpacked[0][:, 0, ends] = cos[:, ends]
    unpacked[1][:, 1, ends] = cos[:, ends]
    return forward, packed, back, unpacked


def left_form(table):
    return table.reshape(2, 16, 8, 2, 16, 8).transpose(1, 0, 2, 4, 3, 5).reshape(256, 256)


def right_form(table):
    return table.reshape(256, 256).T


def tables():
    z_forward, z_back = z_tables()
    forward, packed, back, unpacked = wave_tables()
    y_forward = np.stack(halves(np.concatenate([left_form(forward), left_form(packed)])))
    y_back = np.stack(halves(np.concatenate([left_form(back), left_form(unpacked)])))
    x_forward = np.stack([np.stack(halves(right_form(t))) for t in (forward, packed)])
    x_back = np.stack([np.stack(halves(right_form(t))) for t in (back, unpacked)])
    return z_forward, z_back, y_forward, y_back, x_forward, x_back


def split(value):
    high = value.astype(BF16)
    low = (value - high.astype(F32)).astype(BF16)
    return high, low


def mm(a, b):
    return jnp.dot(a, b, preferred_element_type=F32)


def lanes_of(shape):
    return lax.broadcasted_iota(jnp.int32, shape, len(shape) - 1)


def exchange(v, pairs):
    count = v.shape[0]
    for index_bit, lane_bit in pairs:
        inner, step = 1 << index_bit, 1 << lane_bit
        rows = count // 2 * 8
        w = v.reshape(count // (2 * inner), 2, inner, 8, 128)
        a = w[:, 0].reshape(rows, 128)
        b = w[:, 1].reshape(rows, 128)
        keep = (lanes_of((rows, 128)) >> lane_bit) & 1 == 0
        new_a = jnp.where(keep, a, pltpu.roll(b, step, 1))
        new_b = jnp.where(keep, pltpu.roll(a, 128 - step, 1), b)
        shape = (count // (2 * inner), 1, inner, 8, 128)
        v = jnp.concatenate([new_a.reshape(shape), new_b.reshape(shape)], axis=1).reshape(count, 8, 128)
    return v


Z_PAIRS = ((4, 6), (3, 5), (2, 2), (1, 1), (0, 0))
X_PAIRS = ((3, 6), (2, 5), (1, 4), (0, 3))


def node_coefficient(node, index, weights):
    total = None
    for offset in range(4):
        term = jnp.where(index + (offset - 1) == node, weights[offset], 0.0)
        total = term if total is None else total + term
    return total


def z_forward_chunk(density, index, weights, table, chunk):
    fields = [density * node_coefficient(4 * chunk + i, index, weights) for i in range(4)]
    theta = jnp.concatenate(fields, axis=0).reshape(256, 128)
    high, low = split(theta)
    wide = mm(jnp.concatenate([high, low], axis=1), table)
    waves = (wide[:, :128] + wide[:, 128:]).reshape(32, 8, 128)
    return exchange(waves, Z_PAIRS).reshape(16, 2, 8, 128)


def z_back_chunk(block, index, slopes, table, chunk):
    waves = exchange(block.reshape(32, 8, 128), Z_PAIRS).reshape(256, 128)
    high, low = split(waves)
    wide = mm(jnp.concatenate([high, low], axis=1), table)
    field = (wide[:, :128] + wide[:, 128:]).reshape(4, 8, 8, 128)
    total = None
    for i in range(4):
        term = field[i] * node_coefficient(4 * chunk + i, index, slopes)
        total = term if total is None else total + term
    return total


def y_chunk(block, table):
    high, low = split(block.reshape(256, 128))
    wide = mm(table[0], jnp.concatenate([high, low], axis=1))
    both = wide[:, :128] + wide[:, 128:] + mm(table[1], high)
    at = lanes_of((256, 128))
    mask = ((at >> 3) & 3 == 0) & (lax.axis_index("band") == 0)
    return jnp.where(mask, both[256:], both[:256]).reshape(16, 2, 8, 128)


def x_waves(rows, table):
    high, low = split(rows)
    count = rows.shape[0]
    wide = mm(jnp.concatenate([high, low], axis=0), table[0])
    return wide[:count] + wide[count:] + mm(high, table[1])


def x_mixed_waves(rows, table):
    general = x_waves(rows, table[0]).reshape(4, 4, 8, 256)
    first = rows.reshape(4, 4, 8, 256)[:, 0].reshape(32, 256)
    packed = x_waves(first, table[1]).reshape(4, 1, 8, 256)
    sub = lax.broadcasted_iota(jnp.int32, (4, 1, 8, 256), 2)
    at = lax.axis_index("grid")
    special = (sub == 0) & (lax.axis_index("band") == 0) & (lax.rem(at, 8) == 0)
    return jnp.concatenate([jnp.where(special, packed, general[:, :1]), general[:, 1:]], axis=1)


def x_forward_chunk(block, table):
    parts = [exchange(block[:, c], X_PAIRS).reshape(128, 128) for c in range(2)]
    return x_mixed_waves(jnp.concatenate(parts, axis=1), table)


def x_back_chunk(waves, table):
    out = x_mixed_waves(waves.reshape(128, 256), table).reshape(128, 256)
    parts = [exchange(out[:, 128 * c : 128 * c + 128].reshape(16, 8, 128), X_PAIRS) for c in range(2)]
    return jnp.concatenate([part[:, None] for part in parts], axis=1)


def shell_tile(tile):
    band, grid = lax.axis_index("band"), lax.axis_index("grid")
    imag = tile >= 32
    own = jnp.where(imag, 0, tile // 8)
    kz = 4 * band + own
    ky = 8 * grid + jnp.where(imag, 0, lax.rem(tile, 8))
    fy = jnp.where(ky < 64, ky, ky - 128)
    kx = lanes_of((128, 128))
    fx = jnp.where(kx < 64, kx, kx - 128)
    packed = (band == 0) & (own == 0)
    ends = (ky == 0) | (ky == 64)
    by_row = packed & (ky > 64)
    by_lane = (kx > 64) | (((kx == 0) | (kx == 64)) & imag)
    last = by_row | (packed & ends & by_lane)
    norm = jnp.where(last, 64 * 64, kz * kz) + fy * fy + fx * fx
    root = jnp.sqrt(norm.astype(F32))
    shell = lax.broadcasted_iota(jnp.int32, (128, 128), 0).astype(F32)
    return jnp.maximum(1.0 - jnp.abs(root - shell), 0.0)


def make_phi(kernel_table, wide_table, phi):
    wide_table[...] = jnp.zeros((480, 128), F32)
    for a in range(NA):
        wide_table[24 * a : 24 * a + NA, : kernel_table.shape[2]] = kernel_table[a]
    high, low = split(wide_table[...])
    wide = jnp.concatenate([high, low], axis=1)

    def step(i, carry):
        tiles = jnp.concatenate([shell_tile(2 * i), shell_tile(2 * i + 1)], axis=1)
        tiles_high, tiles_low = split(tiles)
        values = mm(wide, jnp.concatenate([tiles_high, tiles_high], axis=0)) + mm(high, tiles_low)
        phi[2 * i] = values[:, :128]
        phi[2 * i + 1] = values[:, 128:]
        return carry

    lax.fori_loop(0, 17, step, 0)


def mix_tile(tile, imag_tile, phi, spec, mixed_real, mixed_imag):
    plane, row = tile // 8, lax.rem(tile, 8)
    real = imag = None
    for a in range(NA):
        kernel = phi[tile, 24 * a : 24 * a + 24]
        other = kernel if imag_tile is None else phi[imag_tile, 24 * a : 24 * a + 24]
        wave = spec[a, plane, pl.ds(row, 1), :]
        more_real, more_imag = kernel * wave[:, :128], other * wave[:, 128:]
        real = more_real if real is None else real + more_real
        imag = more_imag if imag is None else imag + more_imag
    mixed_real[pl.ds(tile, 24, stride=32), :] = real
    mixed_imag[pl.ds(tile, 24, stride=32), :] = imag


def mix(phi, spec, mixed_real, mixed_imag):
    mix_tile(0, 32, phi, spec, mixed_real, mixed_imag)

    def step(tile, carry):
        mix_tile(tile, None, phi, spec, mixed_real, mixed_imag)
        return carry

    lax.fori_loop(1, 32, step, 0)


MESH = pl.DeviceIdType.MESH
PARTS = 16


def peers(me):
    return lambda step: lax.rem(me + step, PARTS)


def greet(barrier, axis):
    peer = peers(lax.axis_index(axis))

    def one(step, carry):
        pl.semaphore_signal(barrier, inc=1, device_id={axis: peer(step)}, device_id_type=MESH)
        return carry

    lax.fori_loop(1, PARTS, one, 0)


def remote(src, dst, send_sem, recv_sem, axis, target):
    return pltpu.make_async_remote_copy(
        src_ref=src, dst_ref=dst, send_sem=send_sem, recv_sem=recv_sem, device_id={axis: target}, device_id_type=MESH
    )


def send_chunk(axis, sent, got, chunk, send_sem, recv_sem):
    me = lax.axis_index(axis)
    peer = peers(me)
    got[me, chunk] = sent[me, chunk]

    def one(step, carry):
        to = peer(step)
        remote(sent.at[to, chunk], got.at[me, chunk], send_sem, recv_sem.at[chunk], axis, to).start()
        return carry

    lax.fori_loop(1, PARTS, one, 0)


def wait_chunk(axis, got, chunk, send_sem, recv_sem):
    rest = got.at[pl.ds(0, PARTS - 1), chunk]
    remote(rest, rest, send_sem, recv_sem.at[chunk], axis, 0).wait_recv()


def wait_sent(axis, sent, send_sem, recv_sem):
    rest = sent.at[pl.ds(0, PARTS - 1)]
    remote(rest, rest, send_sem, recv_sem.at[0], axis, 0).wait_send()


def body(
    partial, node_index, node_weight, node_slope, kernel_hbm, zf_hbm, zb_hbm, yf_hbm, yb_hbm, xf_hbm, xb_hbm, out,
    stage, heard, index, weights, slopes, kernel_table, zf, zb, yf, yb, xf, xb,
    sent_a, got_a, sent_b, got_b, sent_c, got_c, sent_d, got_d,
    wide_table, phi, spec, mixed_real, mixed_imag, total,
    load_sem, send_sem, heard_sem, sem_a, sem_b, sem_c, sem_d, out_sem,
):
    band, grid = lax.axis_index("band"), lax.axis_index("grid")
    peer = peers(band)
    barrier = pltpu.get_barrier_semaphore()
    greet(barrier, "band")
    greet(barrier, "grid")
    rows = pl.ds(pl.multiple_of(8 * band, 8), 8)

    def cut(step, carry):
        block = pl.ds(pl.multiple_of(8 * step, 8), 8)
        pltpu.make_async_copy(partial.at[0, :, block, :], stage.at[step], load_sem.at[0]).start()
        return carry

    lax.fori_loop(0, PARTS, cut, 0)
    loads = [
        pltpu.make_async_copy(src, dst, load_sem.at[i + 1])
        for i, (src, dst) in enumerate(
            (
                (kernel_hbm, kernel_table),
                (node_index.at[:, rows, :], index),
                (node_weight.at[:, :, rows, :], weights),
                (node_slope.at[:, :, rows, :], slopes),
                (zf_hbm, zf),
                (yf_hbm, yf),
                (xf_hbm, xf),
                (xb_hbm, xb),
                (yb_hbm, yb),
                (zb_hbm, zb),
            )
        )
    ]
    for load in loads:
        load.start()
    pltpu.make_async_copy(stage, stage, load_sem.at[0]).wait()
    pl.semaphore_wait(barrier, 2 * (PARTS - 1))

    def tell(step, carry):
        to = peer(step)
        remote(stage.at[to], heard.at[band], send_sem.at[0], heard_sem.at[band], "band", to).start()
        return carry

    lax.fori_loop(1, PARTS, tell, 0)
    loads[0].wait()
    make_phi(kernel_table, wide_table, phi)
    for load in loads[1:]:
        load.wait()

    def hear(step, density):
        at = lax.rem(band + PARTS - step, PARTS)
        remote(heard.at[at], heard.at[at], send_sem.at[0], heard_sem.at[at], "band", at).wait_recv()
        return density + heard[at]

    density = lax.fori_loop(1, PARTS, hear, stage[band])

    def z_step(chunk, carry):
        sent_a[:, chunk] = z_forward_chunk(density, index[...], [weights[i] for i in range(4)], zf[...], chunk)
        send_chunk("band", sent_a, got_a, chunk, send_sem.at[1], sem_a)
        return carry

    lax.fori_loop(0, CHUNKS, z_step, 0)

    def y_step(chunk, carry):
        wait_chunk("band", got_a, chunk, send_sem.at[1], sem_a)
        sent_b[:, chunk] = y_chunk(got_a[:, chunk], yf)
        send_chunk("grid", sent_b, got_b, chunk, send_sem.at[2], sem_b)
        return carry

    lax.fori_loop(0, CHUNKS, y_step, 0)

    def x_step(chunk, carry):
        wait_chunk("grid", got_b, chunk, send_sem.at[2], sem_b)
        spec[pl.ds(4 * chunk, 4)] = x_forward_chunk(got_b[:, chunk], xf)
        return carry

    lax.fori_loop(0, CHUNKS, x_step, 0)
    mix(phi, spec, mixed_real, mixed_imag)

    def x_back_step(chunk, carry):
        here = pl.ds(pl.multiple_of(128 * chunk, 128), 128)
        waves = jnp.concatenate([mixed_real[here, :], mixed_imag[here, :]], axis=1)
        sent_c[:, chunk] = x_back_chunk(waves, xb)
        send_chunk("grid", sent_c, got_c, chunk, send_sem.at[3], sem_c)
        return carry

    lax.fori_loop(0, CHUNKS, x_back_step, 0)

    def y_back_step(chunk, carry):
        wait_chunk("grid", got_c, chunk, send_sem.at[3], sem_c)
        sent_d[:, chunk] = y_chunk(got_c[:, chunk], yb)
        send_chunk("band", sent_d, got_d, chunk, send_sem.at[4], sem_d)
        return carry

    lax.fori_loop(0, CHUNKS, y_back_step, 0)

    def z_back_step(chunk, so_far):
        wait_chunk("band", got_d, chunk, send_sem.at[4], sem_d)
        return so_far + z_back_chunk(got_d[:, chunk], index[...], [slopes[i] for i in range(4)], zb[...], chunk)

    total[...] = lax.fori_loop(0, CHUNKS, z_back_step, jnp.zeros((8, 8, 128), F32))
    mine = out.at[:, rows, :]
    keep = pltpu.make_async_copy(total, mine, load_sem.at[0])
    keep.start()

    def give(step, carry):
        remote(total, mine, send_sem.at[5], out_sem, "band", peer(step)).start()
        return carry

    lax.fori_loop(1, PARTS, give, 0)
    wait_sent("grid", sent_b, send_sem.at[2], sem_b)
    wait_sent("grid", sent_c, send_sem.at[3], sem_c)
    wait_sent("band", sent_a, send_sem.at[1], sem_a)
    wait_sent("band", sent_d, send_sem.at[4], sem_d)
    rest = stage.at[pl.ds(0, PARTS - 1)]
    remote(rest, rest, send_sem.at[0], heard_sem.at[0], "band", 0).wait_send()
    others = out.at[:, pl.ds(0, 8 * (PARTS - 1)), :]
    remote(rest, others, send_sem.at[5], out_sem, "band", 0).wait()
    keep.wait()


BLOCKS = (PARTS, CHUNKS, 2, 8, 128)


def per_device(partial_density, node_index, node_weight, node_slope, kernel_table):
    constants = [jnp.asarray(t) for t in tables()]
    args = [partial_density, node_index, node_weight, node_slope, kernel_table, *constants]
    anywhere = pl.BlockSpec(memory_space=pl.ANY)
    vmem = pltpu.VMEM
    return pl.pallas_call(
        body,
        out_shape=jax.ShapeDtypeStruct((8, N, N), F32),
        in_specs=[anywhere] * len(args),
        out_specs=anywhere,
        scratch_shapes=[
            vmem((PARTS, 8, 8, 128), F32),
            vmem((PARTS, 8, 8, 128), F32),
            vmem((8, 8, 128), jnp.int32),
            vmem((4, 8, 8, 128), F32),
            vmem((4, 8, 8, 128), F32),
            vmem(kernel_table.shape, F32),
            *[vmem(t.shape, t.dtype) for t in constants[:3]],
            *[vmem(t.shape, t.dtype) for t in constants[3:]],
            *[vmem(BLOCKS, F32)] * 8,
            vmem((480, 128), F32),
            vmem((34, 480, 128), F32),
            vmem((NA, 4, 8, 256), F32),
            vmem((768, 128), F32),
            vmem((768, 128), F32),
            vmem((8, 8, 128), F32),
            pltpu.SemaphoreType.DMA((11,)),
            pltpu.SemaphoreType.DMA((6,)),
            pltpu.SemaphoreType.DMA((PARTS,)),
            *[pltpu.SemaphoreType.DMA((CHUNKS,))] * 4,
            pltpu.SemaphoreType.DMA,
        ],
        compiler_params=pltpu.CompilerParams(
            collective_id=0, has_side_effects=True, vmem_limit_bytes=60000 * 1024
        ),
    )(*args)


def solution(mesh):
    placed = (
        P("band", "grid", None, None),
        P("grid", None, None),
        P(None, "grid", None, None),
        P(None, "grid", None, None),
        P(),
    )
    return jax.shard_map(
        per_device, mesh=mesh, in_specs=placed, out_specs=P("grid", None, None), check_vma=False
    )
```

```python
import functools

import jax
import jax.numpy as jnp
import numpy as np
from jax import lax
from jax.experimental import pallas as pl
from jax.experimental.pallas import tpu as pltpu
from jax.sharding import PartitionSpec as P

N = 128
NA = 20
CHUNKS = 5
F32 = jnp.float32
BF16 = jnp.bfloat16


def halves(table):
    table = np.asarray(table, np.float32)
    high = table.astype(BF16)
    low = (table - high.astype(np.float32)).astype(BF16)
    return high, low


def lane_wave():
    lane = np.arange(128)
    bit = [(lane >> b) & 1 for b in range(7)]
    owner = bit[6] * 8 + bit[5] * 4 + bit[2] * 2 + bit[1]
    pair = owner * 4 + bit[0] * 2 + bit[4]
    return np.where(bit[3] == 0, pair, np.where(pair == 0, 64, N - pair))


def cas(k, n):
    angle = 2 * np.pi * ((k[:, None] * n[None]) % N) / N
    return np.cos(angle) + np.sin(angle)


def right_form(table):
    high, low = halves(table)
    return np.block([[high, low], [high, np.zeros_like(low)]])


def left_form(table):
    high, low = halves(table)
    return np.block([[high, high], [low, np.zeros_like(low)]])


def tables():
    at = np.arange(N)
    z = cas(at, lane_wave())
    line = cas(at, at)
    return np.stack([right_form(z), right_form(z.T / float(N) ** 3), left_form(line), right_form(line)])


def split(value):
    high = value.astype(BF16)
    low = (value - high.astype(F32)).astype(BF16)
    return high, low


def mm(a, b):
    return jnp.dot(a, b, preferred_element_type=F32)


def lanes_of(shape):
    return lax.broadcasted_iota(jnp.int32, shape, len(shape) - 1)


def exchange(v, pairs):
    count = v.shape[0]
    for index_bit, lane_bit in pairs:
        inner, step = 1 << index_bit, 1 << lane_bit
        rows = count // 2 * 8
        w = v.reshape(count // (2 * inner), 2, inner, 8, 128)
        a = w[:, 0].reshape(rows, 128)
        b = w[:, 1].reshape(rows, 128)
        keep = (lanes_of((rows, 128)) >> lane_bit) & 1 == 0
        new_a = jnp.where(keep, a, pltpu.roll(b, step, 1))
        new_b = jnp.where(keep, pltpu.roll(a, 128 - step, 1), b)
        shape = (count // (2 * inner), 1, inner, 8, 128)
        v = jnp.concatenate([new_a.reshape(shape), new_b.reshape(shape)], axis=1).reshape(count, 8, 128)
    return v


Z_PAIRS = ((4, 6), (3, 5), (2, 2), (1, 1), (0, 0))
X_PAIRS = ((3, 6), (2, 5), (1, 4), (0, 3))


def node_coefficient(node, index, weights):
    total = None
    for offset in range(4):
        term = jnp.where(index + (offset - 1) == node, weights[offset], 0.0)
        total = term if total is None else total + term
    return total


def right(rows, table):
    high, low = split(rows)
    wide = mm(jnp.concatenate([high, low], axis=1), table)
    return wide[:, :128] + wide[:, 128:]


def left(table, columns):
    high, low = split(columns)
    tall = mm(table, jnp.concatenate([high, low], axis=0))
    return tall[:128] + tall[128:]


def z_forward_chunk(density, index, weights, table, chunk):
    fields = [density * node_coefficient(4 * chunk + i, index, weights) for i in range(4)]
    theta = jnp.concatenate(fields, axis=0).reshape(256, 128)
    waves = right(theta, table).reshape(32, 8, 128)
    return exchange(waves, Z_PAIRS).reshape(PARTS, 2, 8, 128)


def z_back_chunk(block, index, slopes, table, chunk):
    waves = exchange(block.reshape(32, 8, 128), Z_PAIRS).reshape(256, 128)
    field = right(waves, table).reshape(4, 8, 8, 128)
    total = None
    for i in range(4):
        term = field[i] * node_coefficient(4 * chunk + i, index, slopes)
        total = term if total is None else total + term
    return total


def y_chunk(block, table):
    return left(table, block.reshape(128, 128)).reshape(PARTS, 8, 128)


def x_forward_chunk(block, table):
    return right(exchange(block, X_PAIRS).reshape(128, 128), table).reshape(4, 2, 2, 8, 128)


def x_back_chunk(waves, table):
    return exchange(right(waves, table).reshape(PARTS, 8, 128), X_PAIRS)


def shell_tile(tile):
    band, grid = lax.axis_index("band"), lax.axis_index("grid")
    second = tile >= 32
    fz = 4 * band + jnp.where(second, 0, tile // 8)
    fz = jnp.where(second & (band == 0), 64, fz)
    ky = 8 * grid + lax.rem(tile, 8)
    fy = jnp.where(ky < 64, ky, ky - 128)
    kx = lanes_of((128, 128))
    fx = jnp.where(kx < 64, kx, kx - 128)
    root = jnp.sqrt((fz * fz + fy * fy + fx * fx).astype(F32))
    shell = lax.broadcasted_iota(jnp.int32, (128, 128), 0).astype(F32)
    return jnp.maximum(1.0 - jnp.abs(root - shell), 0.0)


def make_phi(kernel_table, wide_table, phi):
    wide_table[...] = jnp.zeros((480, 128), F32)
    for a in range(NA):
        wide_table[24 * a : 24 * a + NA, : kernel_table.shape[2]] = kernel_table[a]
    high, low = split(wide_table[...])
    wide = jnp.concatenate([high, low], axis=1)

    def step(i, carry):
        tiles = jnp.concatenate([shell_tile(2 * i), shell_tile(2 * i + 1)], axis=1)
        tiles_high, tiles_low = split(tiles)
        values = mm(wide, jnp.concatenate([tiles_high, tiles_high], axis=0)) + mm(high, tiles_low)
        phi[2 * i] = values[:, :128]
        phi[2 * i + 1] = values[:, 128:]
        return carry

    lax.fori_loop(0, TILES // 2, step, 0)


def mix_tile(half, tile, second_tile, phi, spec, mixed):
    pair, row = tile // 8, lax.rem(tile, 8)
    first = second = None
    for a in range(NA):
        kernel = phi[16 * half + tile, 24 * a : 24 * a + 24]
        other = kernel if second_tile is None else phi[second_tile, 24 * a : 24 * a + 24]
        more_first = kernel * spec[a, 2 * half + pair, 0, pl.ds(row, 1), :]
        more_second = other * spec[a, 2 * half + pair, 1, pl.ds(row, 1), :]
        first = more_first if first is None else first + more_first
        second = more_second if second is None else second + more_second
    mixed[half, pl.ds(16 * pair + row, 24, stride=32), :] = first
    mixed[half, pl.ds(16 * pair + row + 8, 24, stride=32), :] = second


def mix(half, phi, spec, mixed):
    def own(tile, carry):
        mix_tile(half, tile, 32 + tile, phi, spec, mixed)
        return carry

    def shared(tile, carry):
        mix_tile(half, tile, None, phi, spec, mixed)
        return carry

    if half == 0:
        lax.fori_loop(0, 8, own, 0)
        lax.fori_loop(8, 16, shared, 0)
    else:
        lax.fori_loop(0, 16, shared, 0)


MESH = pl.DeviceIdType.MESH
PARTS = 16
TILES = 40


def peers(me):
    return lambda step: lax.rem(me + step, PARTS)


def greet(barrier, axis):
    peer = peers(lax.axis_index(axis))

    def one(step, carry):
        pl.semaphore_signal(barrier, inc=1, device_id={axis: peer(step)}, device_id_type=MESH)
        return carry

    lax.fori_loop(1, PARTS, one, 0)


def remote(src, dst, send_sem, recv_sem, axis, target):
    return pltpu.make_async_remote_copy(
        src_ref=src, dst_ref=dst, send_sem=send_sem, recv_sem=recv_sem, device_id={axis: target}, device_id_type=MESH
    )


def send_chunk(axis, sent, got, half, chunk, send_sem, recv_sem):
    me = lax.axis_index(axis)
    peer = peers(me)
    got[half, me, chunk] = sent[half, me, chunk]

    def one(step, carry):
        to = peer(step)
        remote(sent.at[half, to, chunk], got.at[half, me, chunk], send_sem, recv_sem.at[half, chunk], axis, to).start()
        return carry

    lax.fori_loop(1, PARTS, one, 0)


def wait_chunk(axis, got, half, chunk, send_sem, recv_sem):
    rest = got.at[half, pl.ds(0, PARTS - 1), chunk]
    remote(rest, rest, send_sem, recv_sem.at[half, chunk], axis, 0).wait_recv()


def wait_sent(axis, sent, send_sem, recv_sem):
    rest = sent.at[:, pl.ds(0, PARTS - 1)]
    remote(rest, rest, send_sem, recv_sem.at[0, 0], axis, 0).wait_send()


def each(step):
    def run(chunk, carry):
        step(chunk)
        return carry

    lax.fori_loop(0, CHUNKS, run, 0)


def body(
    partial, node_index, node_weight, node_slope, kernel_hbm, tables_hbm, out,
    stage, heard, index, weights, slopes, kernel_table, table,
    sent_a, got_a, sent_b, got_b, sent_c, got_c, sent_d, got_d,
    wide_table, phi, spec, mixed, total,
    load_sem, send_sem, heard_sem, sem_a, sem_b, sem_c, sem_d, out_sem,
):
    band = lax.axis_index("band")
    peer = peers(band)
    barrier = pltpu.get_barrier_semaphore()
    greet(barrier, "band")
    greet(barrier, "grid")
    rows = pl.ds(pl.multiple_of(8 * band, 8), 8)

    def cut(step, carry):
        block = pl.ds(pl.multiple_of(8 * step, 8), 8)
        pltpu.make_async_copy(partial.at[0, :, block, :], stage.at[step], load_sem.at[0]).start()
        return carry

    lax.fori_loop(0, PARTS, cut, 0)
    loads = [
        pltpu.make_async_copy(src, dst, load_sem.at[i + 1])
        for i, (src, dst) in enumerate(
            (
                (kernel_hbm, kernel_table),
                (node_index.at[:, rows, :], index),
                (node_weight.at[:, :, rows, :], weights),
                (node_slope.at[:, :, rows, :], slopes),
                (tables_hbm, table),
            )
        )
    ]
    for load in loads:
        load.start()
    pltpu.make_async_copy(stage, stage, load_sem.at[0]).wait()
    pl.semaphore_wait(barrier, 2 * (PARTS - 1))

    def tell(step, carry):
        to = peer(step)
        remote(stage.at[to], heard.at[band], send_sem.at[0], heard_sem.at[band], "band", to).start()
        return carry

    lax.fori_loop(1, PARTS, tell, 0)
    loads[0].wait()
    make_phi(kernel_table, wide_table, phi)
    for load in loads[1:]:
        load.wait()

    def hear(step, density):
        at = lax.rem(band + PARTS - step, PARTS)
        remote(heard.at[at], heard.at[at], send_sem.at[0], heard_sem.at[at], "band", at).wait_recv()
        return density + heard[at]

    density = lax.fori_loop(1, PARTS, hear, stage[band])
    z_table, z_back_table, y_table, x_table = (table.at[i] for i in range(4))

    def z_step(chunk):
        waves = z_forward_chunk(density, index[...], [weights[i] for i in range(4)], z_table[...], chunk)
        sent_a[0, :, chunk] = waves[:, 0]
        sent_a[1, :, chunk] = waves[:, 1]
        send_chunk("band", sent_a, got_a, 0, chunk, send_sem.at[1], sem_a)

    def z_later(chunk):
        send_chunk("band", sent_a, got_a, 1, chunk, send_sem.at[1], sem_a)

    def y_step(half):
        def step(chunk):
            wait_chunk("band", got_a, half, chunk, send_sem.at[1], sem_a)
            sent_b[half, :, chunk] = y_chunk(got_a[half, :, chunk], y_table[...])
            send_chunk("grid", sent_b, got_b, half, chunk, send_sem.at[2], sem_b)

        return step

    def x_step(half):
        def step(chunk):
            wait_chunk("grid", got_b, half, chunk, send_sem.at[2], sem_b)
            waves = x_forward_chunk(got_b[half, :, chunk], x_table[...])
            spec[pl.ds(4 * chunk, 4), 2 * half : 2 * half + 2] = waves

        return step

    def x_back_step(half):
        def step(chunk):
            here = pl.ds(pl.multiple_of(128 * chunk, 128), 128)
            sent_c[half, :, chunk] = x_back_chunk(mixed[half, here, :], x_table[...])
            send_chunk("grid", sent_c, got_c, half, chunk, send_sem.at[3], sem_c)

        return step

    def y_back_step(half):
        def step(chunk):
            wait_chunk("grid", got_c, half, chunk, send_sem.at[3], sem_c)
            sent_d[half, :, chunk] = y_chunk(got_c[half, :, chunk], y_table[...])
            send_chunk("band", sent_d, got_d, half, chunk, send_sem.at[4], sem_d)

        return step

    each(z_step)
    each(z_later)
    each(y_step(0))
    each(x_step(0))
    mix(0, phi, spec, mixed)
    each(x_back_step(0))
    each(y_step(1))
    each(y_back_step(0))
    each(x_step(1))
    mix(1, phi, spec, mixed)
    each(x_back_step(1))
    each(y_back_step(1))

    def z_back_step(chunk, so_far):
        for half in range(2):
            wait_chunk("band", got_d, half, chunk, send_sem.at[4], sem_d)
        block = jnp.concatenate([got_d[half, :, chunk][:, None] for half in range(2)], axis=1)
        return so_far + z_back_chunk(block, index[...], [slopes[i] for i in range(4)], z_back_table[...], chunk)

    total[...] = lax.fori_loop(0, CHUNKS, z_back_step, jnp.zeros((8, 8, 128), F32))
    mine = out.at[:, rows, :]
    keep = pltpu.make_async_copy(total, mine, load_sem.at[0])
    keep.start()

    def give(step, carry):
        remote(total, mine, send_sem.at[5], out_sem, "band", peer(step)).start()
        return carry

    lax.fori_loop(1, PARTS, give, 0)
    wait_sent("grid", sent_b, send_sem.at[2], sem_b)
    wait_sent("grid", sent_c, send_sem.at[3], sem_c)
    wait_sent("band", sent_a, send_sem.at[1], sem_a)
    wait_sent("band", sent_d, send_sem.at[4], sem_d)
    rest = stage.at[pl.ds(0, PARTS - 1)]
    remote(rest, rest, send_sem.at[0], heard_sem.at[0], "band", 0).wait_send()
    others = out.at[:, pl.ds(0, 8 * (PARTS - 1)), :]
    remote(rest, others, send_sem.at[5], out_sem, "band", 0).wait()
    keep.wait()


BLOCKS = (2, PARTS, CHUNKS, 8, 128)


def per_device(partial_density, node_index, node_weight, node_slope, kernel_table):
    constants = jnp.asarray(tables())
    args = [partial_density, node_index, node_weight, node_slope, kernel_table, constants]
    anywhere = pl.BlockSpec(memory_space=pl.ANY)
    vmem = pltpu.VMEM
    return pl.pallas_call(
        body,
        out_shape=jax.ShapeDtypeStruct((8, N, N), F32),
        in_specs=[anywhere] * len(args),
        out_specs=anywhere,
        scratch_shapes=[
            vmem((PARTS, 8, 8, 128), F32),
            vmem((PARTS, 8, 8, 128), F32),
            vmem((8, 8, 128), jnp.int32),
            vmem((4, 8, 8, 128), F32),
            vmem((4, 8, 8, 128), F32),
            vmem(kernel_table.shape, F32),
            vmem(constants.shape, constants.dtype),
            *[vmem(BLOCKS, F32)] * 8,
            vmem((480, 128), F32),
            vmem((TILES, 480, 128), F32),
            vmem((NA, 4, 2, 8, 128), F32),
            vmem((2, 768, 128), F32),
            vmem((8, 8, 128), F32),
            pltpu.SemaphoreType.DMA((6,)),
            pltpu.SemaphoreType.DMA((6,)),
            pltpu.SemaphoreType.DMA((PARTS,)),
            *[pltpu.SemaphoreType.DMA((2, CHUNKS))] * 4,
            pltpu.SemaphoreType.DMA,
        ],
        compiler_params=pltpu.CompilerParams(
            collective_id=0, has_side_effects=True, vmem_limit_bytes=60000 * 1024
        ),
    )(*args)


def solution(mesh):
    placed = (
        P("band", "grid", None, None),
        P("grid", None, None),
        P(None, "grid", None, None),
        P(None, "grid", None, None),
        P(),
    )
    return jax.shard_map(
        per_device, mesh=mesh, in_specs=placed, out_specs=P("grid", None, None), check_vma=False
    )
```

```python
import functools

import jax
import jax.numpy as jnp
import numpy as np
from jax import lax
from jax.experimental import pallas as pl
from jax.experimental.pallas import tpu as pltpu
from jax.sharding import PartitionSpec as P

N = 128
NA = 20
CHUNKS = 5
F32 = jnp.float32
BF16 = jnp.bfloat16


def halves(table):
    table = np.asarray(table, np.float32)
    high = table.astype(BF16)
    low = (table - high.astype(np.float32)).astype(BF16)
    return high, low


def lane_wave():
    lane = np.arange(128)
    bit = [(lane >> b) & 1 for b in range(7)]
    owner = bit[6] * 8 + bit[5] * 4 + bit[2] * 2 + bit[1]
    pair = owner * 4 + bit[0] * 2 + bit[4]
    return np.where(bit[3] == 0, pair, np.where(pair == 0, 64, N - pair))


def cas(k, n):
    angle = 2 * np.pi * ((k[:, None] * n[None]) % N) / N
    return np.cos(angle) + np.sin(angle)


def right_form(table):
    high, low = halves(table)
    return np.block([[high, low], [high, np.zeros_like(low)]])


def left_form(table):
    high, low = halves(table)
    return np.block([[high, high], [low, np.zeros_like(low)]])


def tables():
    at = np.arange(N)
    z = cas(at, lane_wave())
    line = cas(at, at)
    return np.stack([right_form(z), right_form(z.T / float(N) ** 3), left_form(line), right_form(line)])


def split(value):
    high = value.astype(BF16)
    low = (value - high.astype(F32)).astype(BF16)
    return high, low


def mm(a, b):
    return jnp.dot(a, b, preferred_element_type=F32)


def lanes_of(shape):
    return lax.broadcasted_iota(jnp.int32, shape, len(shape) - 1)


def exchange(v, pairs):
    count = v.shape[0]
    for index_bit, lane_bit in pairs:
        inner, step = 1 << index_bit, 1 << lane_bit
        rows = count // 2 * 8
        w = v.reshape(count // (2 * inner), 2, inner, 8, 128)
        a = w[:, 0].reshape(rows, 128)
        b = w[:, 1].reshape(rows, 128)
        keep = (lanes_of((rows, 128)) >> lane_bit) & 1 == 0
        new_a = jnp.where(keep, a, pltpu.roll(b, step, 1))
        new_b = jnp.where(keep, pltpu.roll(a, 128 - step, 1), b)
        shape = (count // (2 * inner), 1, inner, 8, 128)
        v = jnp.concatenate([new_a.reshape(shape), new_b.reshape(shape)], axis=1).reshape(count, 8, 128)
    return v


Z_PAIRS = ((4, 6), (3, 5), (2, 2), (1, 1), (0, 0))
X_PAIRS = ((3, 6), (2, 5), (1, 4), (0, 3))


def node_coefficient(node, index, weights):
    total = None
    for offset in range(4):
        term = jnp.where(index + (offset - 1) == node, weights[offset], 0.0)
        total = term if total is None else total + term
    return total


def right(rows, table):
    high, low = split(rows)
    wide = mm(jnp.concatenate([high, low], axis=1), table)
    return wide[:, :128] + wide[:, 128:]


def left(table, columns):
    high, low = split(columns)
    tall = mm(table, jnp.concatenate([high, low], axis=0))
    return tall[:128] + tall[128:]


def z_forward_chunk(density, index, weights, table, chunk):
    fields = [density * node_coefficient(4 * chunk + i, index, weights) for i in range(4)]
    theta = jnp.concatenate(fields, axis=0).reshape(256, 128)
    waves = right(theta, table).reshape(32, 8, 128)
    return exchange(waves, Z_PAIRS).reshape(PARTS, 2, 8, 128)


def z_back_chunk(block, index, slopes, table, chunk):
    waves = exchange(block.reshape(32, 8, 128), Z_PAIRS).reshape(256, 128)
    field = right(waves, table).reshape(4, 8, 8, 128)
    total = None
    for i in range(4):
        term = field[i] * node_coefficient(4 * chunk + i, index, slopes)
        total = term if total is None else total + term
    return total


def y_chunk(block, table):
    return left(table, block.reshape(128, 128)).reshape(PARTS, 8, 128)


def x_forward_chunk(block, table):
    return right(exchange(block, X_PAIRS).reshape(128, 128), table).reshape(4, 2, 2, 8, 128)


def x_back_chunk(waves, table):
    return exchange(right(waves, table).reshape(PARTS, 8, 128), X_PAIRS)


def shell_tile(tile):
    band, grid = lax.axis_index("band"), lax.axis_index("grid")
    second = tile >= 32
    fz = 4 * band + jnp.where(second, 0, tile // 8)
    fz = jnp.where(second & (band == 0), 64, fz)
    ky = 8 * grid + lax.rem(tile, 8)
    fy = jnp.where(ky < 64, ky, ky - 128)
    kx = lanes_of((128, 128))
    fx = jnp.where(kx < 64, kx, kx - 128)
    root = jnp.sqrt((fz * fz + fy * fy + fx * fx).astype(F32))
    shell = lax.broadcasted_iota(jnp.int32, (128, 128), 0).astype(F32)
    return jnp.maximum(1.0 - jnp.abs(root - shell), 0.0)


def start_phi(kernel_table, wide_table, table_pair):
    wide_table[...] = jnp.zeros((480, 128), F32)
    for a in range(NA):
        wide_table[24 * a : 24 * a + NA, : kernel_table.shape[2]] = kernel_table[a]
    high, low = split(wide_table[...])
    table_pair[...] = jnp.concatenate([high, low], axis=1)


def make_phi(first, last, table_pair, phi):
    def step(i, carry):
        wide = table_pair[...]
        tiles = jnp.concatenate([shell_tile(2 * i), shell_tile(2 * i + 1)], axis=1)
        tiles_high, tiles_low = split(tiles)
        values = mm(wide, jnp.concatenate([tiles_high, tiles_high], axis=0)) + mm(wide[:, :128], tiles_low)
        phi[2 * i] = values[:, :128]
        phi[2 * i + 1] = values[:, 128:]
        return carry

    lax.fori_loop(first, last, step, 0)


def mix_tile(half, tile, second_tile, phi, spec, mixed):
    pair, row = tile // 8, lax.rem(tile, 8)
    first = second = None
    for a in range(NA):
        kernel = phi[16 * half + tile, 24 * a : 24 * a + 24]
        other = kernel if second_tile is None else phi[second_tile, 24 * a : 24 * a + 24]
        more_first = kernel * spec[a, 2 * half + pair, 0, pl.ds(row, 1), :]
        more_second = other * spec[a, 2 * half + pair, 1, pl.ds(row, 1), :]
        first = more_first if first is None else first + more_first
        second = more_second if second is None else second + more_second
    mixed[half, pl.ds(16 * pair + row, 24, stride=32), :] = first
    mixed[half, pl.ds(16 * pair + row + 8, 24, stride=32), :] = second


def mix(half, phi, spec, mixed):
    def own(tile, carry):
        mix_tile(half, tile, 32 + tile, phi, spec, mixed)
        return carry

    def shared(tile, carry):
        mix_tile(half, tile, None, phi, spec, mixed)
        return carry

    if half == 0:
        lax.fori_loop(0, 8, own, 0)
        lax.fori_loop(8, 16, shared, 0)
    else:
        lax.fori_loop(0, 16, shared, 0)


MESH = pl.DeviceIdType.MESH
PARTS = 16
TILES = 40


LINE = 8
FAR_FIRST = (4, 3, 5, 2, 6, 1, 7)


def z_peers(band):
    first = band // LINE * LINE
    return lambda step: first + lax.rem(band + step, LINE)


def partner_of(band):
    return lax.rem(band + LINE, PARTS)


def peers(me):
    return lambda step: lax.rem(me + step, PARTS)


def greet(barrier):
    band = lax.axis_index("band")
    peer = peers(lax.axis_index("grid"))
    along = z_peers(band)

    def grid_one(step, carry):
        pl.semaphore_signal(barrier, inc=1, device_id={"grid": peer(step)}, device_id_type=MESH)
        return carry

    def band_one(step, carry):
        pl.semaphore_signal(barrier, inc=1, device_id={"band": along(step)}, device_id_type=MESH)
        return carry

    lax.fori_loop(1, LINE, band_one, 0)
    pl.semaphore_signal(barrier, inc=1, device_id={"band": partner_of(band)}, device_id_type=MESH)
    lax.fori_loop(1, PARTS, grid_one, 0)


def remote(src, dst, send_sem, recv_sem, axis, target):
    return pltpu.make_async_remote_copy(
        src_ref=src, dst_ref=dst, send_sem=send_sem, recv_sem=recv_sem, device_id={axis: target}, device_id_type=MESH
    )


def send_chunk(axis, sent, got, half, chunk, send_sem, recv_sem):
    me = lax.axis_index(axis)
    peer = peers(me)
    got[half, me, chunk] = sent[half, me, chunk]

    def one(step, carry):
        to = peer(step)
        remote(sent.at[half, to, chunk], got.at[half, me, chunk], send_sem, recv_sem.at[half, chunk], axis, to).start()
        return carry

    lax.fori_loop(1, PARTS, one, 0)


def wait_chunk(axis, got, half, chunk, send_sem, recv_sem):
    rest = got.at[half, pl.ds(0, PARTS - 1), chunk]
    remote(rest, rest, send_sem, recv_sem.at[half, chunk], axis, 0).wait_recv()


def wait_sent(axis, sent, send_sem, recv_sem):
    rest = sent.at[:, pl.ds(0, PARTS - 1)]
    remote(rest, rest, send_sem, recv_sem.at[0, 0], axis, 0).wait_send()


def each(*steps, first=0, last=CHUNKS):
    def run(chunk, carry):
        for step in steps:
            step(chunk)
        return carry

    lax.fori_loop(first, last, run, 0)


def body(
    partial, node_index, node_weight, node_slope, kernel_hbm, tables_hbm, out,
    stage, paired, passed, heard, index, weights, slopes, kernel_table, table,
    sent_a, got_a, sent_b, got_b, sent_c, got_c, sent_d, got_d,
    wide_table, table_pair, phi, spec, mixed,
    load_sem, send_sem, pair_sem, heard_sem, sem_a, sem_b, sem_c, sem_d, out_sem,
):
    band = lax.axis_index("band")
    barrier = pltpu.get_barrier_semaphore()
    greet(barrier)
    partner, along = partner_of(band), z_peers(band)

    def rows_of(block):
        return pl.ds(pl.multiple_of(8 * block, 8), 8)

    rows = rows_of(band)

    def cut(step, carry):
        pltpu.make_async_copy(partial.at[0, :, rows_of(step), :], stage.at[step], load_sem.at[0]).start()
        return carry

    lax.fori_loop(0, PARTS, cut, 0)
    loads = [
        pltpu.make_async_copy(src, dst, load_sem.at[i + 1])
        for i, (src, dst) in enumerate(
            (
                (kernel_hbm, kernel_table),
                (node_index.at[:, rows, :], index),
                (node_weight.at[:, :, rows, :], weights),
                (node_slope.at[:, :, rows, :], slopes),
                (tables_hbm, table),
            )
        )
    ]
    for load in loads:
        load.start()
    pltpu.make_async_copy(stage, stage, load_sem.at[0]).wait()
    pl.semaphore_wait(barrier, LINE - 1 + 1 + PARTS - 1)

    def to_partner(step):
        at = partner_of(along(step))
        slot = lax.rem(at, LINE)
        return remote(stage.at[at], paired.at[slot], send_sem.at[0], pair_sem.at[slot], "band", partner)

    for step in (*FAR_FIRST, 0):
        to_partner(step).start()
    loads[0].wait()
    start_phi(kernel_table, wide_table, table_pair)
    make_phi(0, 7, table_pair, phi)
    slot_of_band = lax.rem(band, LINE)
    for i, step in enumerate((*FAR_FIRST, 0)):
        to = along(step)
        slot = lax.rem(to, LINE)
        remote(paired.at[slot], paired.at[slot], send_sem.at[0], pair_sem.at[slot], "band", partner).wait_recv()
        passed[slot] = paired[slot] + stage[to]
        if step:
            remote(
                passed.at[slot], heard.at[slot_of_band], send_sem.at[6], heard_sem.at[slot_of_band], "band", to
            ).start()
            make_phi(7 + i, 8 + i, table_pair, phi)
    make_phi(14, TILES // 2, table_pair, phi)
    for load in loads[1:]:
        load.wait()
    density = passed[slot_of_band]
    for step in FAR_FIRST:
        slot = lax.rem(band + LINE - step, LINE)
        remote(heard.at[slot], heard.at[slot], send_sem.at[6], heard_sem.at[slot], "band", partner).wait_recv()
        density = density + heard[slot]
    z_table, z_back_table, y_table, x_table = (table.at[i] for i in range(4))

    def z_step(chunk):
        waves = z_forward_chunk(density, index[...], [weights[i] for i in range(4)], z_table[...], chunk)
        sent_a[0, :, chunk] = waves[:, 0]
        sent_a[1, :, chunk] = waves[:, 1]
        send_chunk("band", sent_a, got_a, 0, chunk, send_sem.at[1], sem_a)

    def z_later(chunk):
        send_chunk("band", sent_a, got_a, 1, chunk, send_sem.at[1], sem_a)

    def y_step(half):
        def step(chunk):
            wait_chunk("band", got_a, half, chunk, send_sem.at[1], sem_a)
            sent_b[half, :, chunk] = y_chunk(got_a[half, :, chunk], y_table[...])
            send_chunk("grid", sent_b, got_b, half, chunk, send_sem.at[2], sem_b)

        return step

    def x_step(half):
        def step(chunk):
            wait_chunk("grid", got_b, half, chunk, send_sem.at[2], sem_b)
            waves = x_forward_chunk(got_b[half, :, chunk], x_table[...])
            spec[pl.ds(4 * chunk, 4), 2 * half : 2 * half + 2] = waves

        return step

    def x_back_step(half):
        def step(chunk):
            here = pl.ds(pl.multiple_of(128 * chunk, 128), 128)
            sent_c[half, :, chunk] = x_back_chunk(mixed[half, here, :], x_table[...])
            send_chunk("grid", sent_c, got_c, half, chunk, send_sem.at[3], sem_c)

        return step

    def y_back_step(half):
        def step(chunk):
            wait_chunk("grid", got_c, half, chunk, send_sem.at[3], sem_c)
            sent_d[half, :, chunk] = y_chunk(got_c[half, :, chunk], y_table[...])
            send_chunk("band", sent_d, got_d, half, chunk, send_sem.at[4], sem_d)

        return step

    y_a, y_b, x_a, x_b = y_step(0), y_step(1), x_step(0), x_step(1)
    each(z_step)
    each(z_later)
    each(y_a)
    x_a(0)
    each(lambda chunk: x_a(chunk + 1), y_b, last=3)
    x_a(4)
    mix(0, phi, spec, mixed)
    y_b(3)
    each(x_back_step(0), last=2)
    y_b(4)
    each(x_back_step(0), first=2)
    each(y_back_step(0), x_b)
    mix(1, phi, spec, mixed)
    each(x_back_step(1))
    each(y_back_step(1))

    def z_back_step(chunk, so_far):
        for half in range(2):
            wait_chunk("band", got_d, half, chunk, send_sem.at[4], sem_d)
        block = jnp.concatenate([got_d[half, :, chunk][:, None] for half in range(2)], axis=1)
        return so_far + z_back_chunk(block, index[...], [slopes[i] for i in range(4)], z_back_table[...], chunk)

    out[:, rows, :] = lax.fori_loop(0, CHUNKS, z_back_step, jnp.zeros((8, 8, 128), F32))

    def give(block, target):
        piece = out.at[:, rows_of(block), :]
        return remote(piece, piece, send_sem.at[5], out_sem.at[block], "band", target)

    give(band, partner).start()
    for step in FAR_FIRST:
        give(band, along(step)).start()
    for step in FAR_FIRST:
        origin = along(LINE - step)
        give(origin, partner).wait_recv()
        give(origin, partner).start()
    for step in range(LINE):
        give(partner_of(along(step)), partner).wait_recv()
    wait_sent("grid", sent_b, send_sem.at[2], sem_b)
    wait_sent("grid", sent_c, send_sem.at[3], sem_c)
    wait_sent("band", sent_a, send_sem.at[1], sem_a)
    wait_sent("band", sent_d, send_sem.at[4], sem_d)
    remote(paired, paired, send_sem.at[0], pair_sem.at[0], "band", partner).wait_send()
    rest = passed.at[pl.ds(0, LINE - 1)]
    remote(rest, rest, send_sem.at[6], heard_sem.at[0], "band", partner).wait_send()
    rest = stage.at[pl.ds(0, PARTS - 1)]
    remote(rest, rest, send_sem.at[5], out_sem.at[0], "band", partner).wait_send()


BLOCKS = (2, PARTS, CHUNKS, 8, 128)


def per_device(partial_density, node_index, node_weight, node_slope, kernel_table):
    constants = jnp.asarray(tables())
    args = [partial_density, node_index, node_weight, node_slope, kernel_table, constants]
    anywhere = pl.BlockSpec(memory_space=pl.ANY)
    vmem = pltpu.VMEM
    return pl.pallas_call(
        body,
        out_shape=pltpu.VMEM((8, N, N), F32),
        in_specs=[anywhere] * len(args),
        out_specs=pl.BlockSpec(memory_space=pltpu.VMEM),
        scratch_shapes=[
            vmem((PARTS, 8, 8, 128), F32),
            *[vmem((LINE, 8, 8, 128), F32)] * 3,
            vmem((8, 8, 128), jnp.int32),
            vmem((4, 8, 8, 128), F32),
            vmem((4, 8, 8, 128), F32),
            vmem(kernel_table.shape, F32),
            vmem(constants.shape, constants.dtype),
            *[vmem(BLOCKS, F32)] * 8,
            vmem((480, 128), F32),
            vmem((480, 256), BF16),
            vmem((TILES, 480, 128), F32),
            vmem((NA, 4, 2, 8, 128), F32),
            vmem((2, 768, 128), F32),
            pltpu.SemaphoreType.DMA((6,)),
            pltpu.SemaphoreType.DMA((7,)),
            pltpu.SemaphoreType.DMA((LINE,)),
            pltpu.SemaphoreType.DMA((LINE,)),
            *[pltpu.SemaphoreType.DMA((2, CHUNKS))] * 4,
            pltpu.SemaphoreType.DMA((PARTS,)),
        ],
        compiler_params=pltpu.CompilerParams(
            collective_id=0, has_side_effects=True, vmem_limit_bytes=60000 * 1024
        ),
    )(*args)


def solution(mesh):
    placed = (
        P("band", "grid", None, None),
        P("grid", None, None),
        P(None, "grid", None, None),
        P(None, "grid", None, None),
        P(),
    )
    return jax.shard_map(
        per_device, mesh=mesh, in_specs=placed, out_specs=P("grid", None, None), check_vma=False
    )
```

```python
import functools

import jax
import jax.numpy as jnp
import numpy as np
from jax import lax
from jax.experimental import pallas as pl
from jax.experimental.pallas import tpu as pltpu
from jax.sharding import PartitionSpec as P

N = 128
NA = 20
CHUNKS = 5
F32 = jnp.float32
BF16 = jnp.bfloat16


def halves(table):
    table = np.asarray(table, np.float32)
    high = table.astype(BF16)
    low = (table - high.astype(np.float32)).astype(BF16)
    return high, low


def lane_wave():
    lane = np.arange(128)
    bit = [(lane >> b) & 1 for b in range(7)]
    owner = bit[6] * 8 + bit[5] * 4 + bit[2] * 2 + bit[1]
    pair = owner * 4 + bit[0] * 2 + bit[4]
    return np.where(bit[3] == 0, pair, np.where(pair == 0, 64, N - pair))


def cas(k, n):
    angle = 2 * np.pi * ((k[:, None] * n[None]) % N) / N
    return np.cos(angle) + np.sin(angle)


def right_form(table):
    high, low = halves(table)
    return np.block([[high, low], [high, np.zeros_like(low)]])


def left_form(table):
    high, low = halves(table)
    return np.block([[high, high], [low, np.zeros_like(low)]])


def tables():
    at = np.arange(N)
    z = cas(at, lane_wave())
    line = cas(at, at)
    return np.stack([right_form(z), right_form(z.T / float(N) ** 3), left_form(line), right_form(line)])


def split(value):
    high = value.astype(BF16)
    low = (value - high.astype(F32)).astype(BF16)
    return high, low


def mm(a, b):
    return jnp.dot(a, b, preferred_element_type=F32)


def lanes_of(shape):
    return lax.broadcasted_iota(jnp.int32, shape, len(shape) - 1)


def exchange(v, pairs):
    count = v.shape[0]
    for index_bit, lane_bit in pairs:
        inner, step = 1 << index_bit, 1 << lane_bit
        rows = count // 2 * 8
        w = v.reshape(count // (2 * inner), 2, inner, 8, 128)
        a = w[:, 0].reshape(rows, 128)
        b = w[:, 1].reshape(rows, 128)
        keep = (lanes_of((rows, 128)) >> lane_bit) & 1 == 0
        new_a = jnp.where(keep, a, pltpu.roll(b, step, 1))
        new_b = jnp.where(keep, pltpu.roll(a, 128 - step, 1), b)
        shape = (count // (2 * inner), 1, inner, 8, 128)
        v = jnp.concatenate([new_a.reshape(shape), new_b.reshape(shape)], axis=1).reshape(count, 8, 128)
    return v


def exchange_groups(v):
    group = lanes_of((8, 128)) >> 3
    skewed = [v[i] if i == 0 else pltpu.roll(v[i], 8 * i, 1) for i in range(16)]
    for bit in range(4):
        take = (group >> bit) & 1 == 1
        skewed = [jnp.where(take, skewed[(i + (1 << bit)) % 16], skewed[i]) for i in range(16)]
    out = [skewed[-i % 16] if i == 0 else pltpu.roll(skewed[-i % 16], 128 - 8 * i, 1) for i in range(16)]
    return jnp.concatenate([piece[None] for piece in out], axis=0)


Z_PAIRS = ((4, 6), (3, 5), (2, 2), (1, 1), (0, 0))


def node_coefficient(node, index, weights):
    total = None
    for offset in range(4):
        term = jnp.where(index + (offset - 1) == node, weights[offset], 0.0)
        total = term if total is None else total + term
    return total


def right(rows, table):
    high, low = split(rows)
    wide = mm(jnp.concatenate([high, low], axis=1), table)
    return wide[:, :128] + wide[:, 128:]


def left(table, columns):
    high, low = split(columns)
    tall = mm(table, jnp.concatenate([high, low], axis=0))
    return tall[:128] + tall[128:]


def z_forward_chunk(density, index, weights, table, chunk):
    fields = [density * node_coefficient(4 * chunk + i, index, weights) for i in range(4)]
    theta = jnp.concatenate(fields, axis=0).reshape(256, 128)
    waves = right(theta, table).reshape(32, 8, 128)
    return exchange(waves, Z_PAIRS).reshape(PARTS, 2, 8, 128)


def z_back_chunk(block, index, slopes, table, chunk):
    waves = exchange(block.reshape(32, 8, 128), Z_PAIRS).reshape(256, 128)
    field = right(waves, table).reshape(4, 8, 8, 128)
    total = None
    for i in range(4):
        term = field[i] * node_coefficient(4 * chunk + i, index, slopes)
        total = term if total is None else total + term
    return total


def y_chunk(block, table):
    return left(table, block.reshape(128, 128)).reshape(PARTS, 8, 128)


def x_forward_chunk(block, table):
    return right(exchange_groups(block).reshape(128, 128), table).reshape(4, 2, 2, 8, 128)


def x_back_chunk(waves, table):
    return exchange_groups(right(waves, table).reshape(PARTS, 8, 128))


def shell_tile(tile):
    band, grid = lax.axis_index("band"), lax.axis_index("grid")
    second = tile >= 32
    fz = 4 * band + jnp.where(second, 0, tile // 8)
    fz = jnp.where(second & (band == 0), 64, fz)
    ky = 8 * grid + lax.rem(tile, 8)
    fy = jnp.where(ky < 64, ky, ky - 128)
    kx = lanes_of((128, 128))
    fx = jnp.where(kx < 64, kx, kx - 128)
    root = jnp.sqrt((fz * fz + fy * fy + fx * fx).astype(F32))
    shell = lax.broadcasted_iota(jnp.int32, (128, 128), 0).astype(F32)
    return jnp.maximum(1.0 - jnp.abs(root - shell), 0.0)


def start_phi(kernel_table, wide_table, table_pair):
    wide_table[...] = jnp.zeros((480, 128), F32)
    for a in range(NA):
        wide_table[24 * a : 24 * a + NA, : kernel_table.shape[2]] = kernel_table[a]
    high, low = split(wide_table[...])
    table_pair[...] = jnp.concatenate([high, low], axis=1)


def make_phi(first, last, table_pair, phi):
    def step(i, carry):
        wide = table_pair[...]
        tiles = jnp.concatenate([shell_tile(2 * i), shell_tile(2 * i + 1)], axis=1)
        tiles_high, tiles_low = split(tiles)
        values = mm(wide, jnp.concatenate([tiles_high, tiles_high], axis=0)) + mm(wide[:, :128], tiles_low)
        phi[2 * i] = values[:, :128]
        phi[2 * i + 1] = values[:, 128:]
        return carry

    lax.fori_loop(first, last, step, 0)


def mix_tile(half, tile, second_tile, phi, spec, mixed):
    pair, row = tile // 8, lax.rem(tile, 8)
    first = second = None
    for a in range(NA):
        kernel = phi[16 * half + tile, 24 * a : 24 * a + 24]
        other = kernel if second_tile is None else phi[second_tile, 24 * a : 24 * a + 24]
        more_first = kernel * spec[a, 2 * half + pair, 0, pl.ds(row, 1), :]
        more_second = other * spec[a, 2 * half + pair, 1, pl.ds(row, 1), :]
        first = more_first if first is None else first + more_first
        second = more_second if second is None else second + more_second
    mixed[half, pl.ds(16 * pair + row, 24, stride=32), :] = first
    mixed[half, pl.ds(16 * pair + row + 8, 24, stride=32), :] = second


def mix(half, phi, spec, mixed):
    def own(tile, carry):
        mix_tile(half, tile, 32 + tile, phi, spec, mixed)
        return carry

    def shared(tile, carry):
        mix_tile(half, tile, None, phi, spec, mixed)
        return carry

    if half == 0:
        lax.fori_loop(0, 8, own, 0)
        lax.fori_loop(8, 16, shared, 0)
    else:
        lax.fori_loop(0, 16, shared, 0)


MESH = pl.DeviceIdType.MESH
PARTS = 16
TILES = 40


LINE = 8
FAR_FIRST = (4, 3, 5, 2, 6, 1, 7)
BESIDE = (3, 5, 2, 6, 1, 7)
BESIDE_NEAR = (1, 7, 2, 6, 3, 5)
ACROSS = 4


def z_peers(band):
    first = band // LINE * LINE
    return lambda step: first + lax.rem(band + step, LINE)


def partner_of(band):
    return lax.rem(band + LINE, PARTS)


def peers(me):
    return lambda step: lax.rem(me + step, PARTS)


def greet(barrier):
    band = lax.axis_index("band")
    peer = peers(lax.axis_index("grid"))
    along = z_peers(band)

    def grid_one(step, carry):
        pl.semaphore_signal(barrier, inc=1, device_id={"grid": peer(step)}, device_id_type=MESH)
        return carry

    def band_one(step, carry):
        pl.semaphore_signal(barrier, inc=1, device_id={"band": along(step)}, device_id_type=MESH)
        return carry

    lax.fori_loop(1, LINE, band_one, 0)
    pl.semaphore_signal(barrier, inc=1, device_id={"band": partner_of(band)}, device_id_type=MESH)
    lax.fori_loop(1, PARTS, grid_one, 0)


def remote(src, dst, send_sem, recv_sem, axis, target):
    return pltpu.make_async_remote_copy(
        src_ref=src, dst_ref=dst, send_sem=send_sem, recv_sem=recv_sem, device_id={axis: target}, device_id_type=MESH
    )


def wait_given(copy):
    copy.wait_recv()


def send_chunk(axis, sent, got, half, chunk, send_sem, recv_sem):
    me = lax.axis_index(axis)
    peer = peers(me)
    got[half, me, chunk] = sent[half, me, chunk]

    for step in range(1, PARTS):
        to = peer(step)
        remote(sent.at[half, to, chunk], got.at[half, me, chunk], send_sem, recv_sem.at[half, chunk], axis, to).start()


def wait_chunk(axis, got, half, chunk, send_sem, recv_sem):
    rest = got.at[half, pl.ds(0, PARTS - 1), chunk]
    remote(rest, rest, send_sem, recv_sem.at[half, chunk], axis, 0).wait_recv()


def wait_sent(axis, sent, send_sem, recv_sem):
    rest = sent.at[:, pl.ds(0, PARTS - 1)]
    remote(rest, rest, send_sem, recv_sem.at[0, 0], axis, 0).wait_send()


def each(*steps, first=0, last=CHUNKS):
    def run(chunk, carry):
        for step in steps:
            step(chunk)
        return carry

    lax.fori_loop(first, last, run, 0)


def body(
    partial, node_index, node_weight, node_slope, kernel_hbm, tables_hbm, out,
    stage, paired, passed, heard, crossed, index, weights, slopes, kernel_table, table,
    sent_a, got_a, sent_b, got_b, sent_c, got_c, sent_d, got_d,
    wide_table, table_pair, phi, spec, mixed,
    load_sem, send_sem, pair_sem, heard_sem, cross_sem, sem_a, sem_b, sem_c, sem_d, out_sem,
):
    band = lax.axis_index("band")
    barrier = pltpu.get_barrier_semaphore()
    greet(barrier)
    partner, along = partner_of(band), z_peers(band)

    def rows_of(block):
        return pl.ds(pl.multiple_of(8 * block, 8), 8)

    rows = rows_of(band)

    def cut(step, carry):
        pltpu.make_async_copy(partial.at[0, :, rows_of(step), :], stage.at[step], load_sem.at[0]).start()
        return carry

    lax.fori_loop(0, PARTS, cut, 0)
    loads = [
        pltpu.make_async_copy(src, dst, load_sem.at[i + 1])
        for i, (src, dst) in enumerate(
            (
                (kernel_hbm, kernel_table),
                (node_index.at[:, rows, :], index),
                (node_weight.at[:, :, rows, :], weights),
                (node_slope.at[:, :, rows, :], slopes),
                (tables_hbm, table),
            )
        )
    ]
    for load in loads:
        load.start()
    pltpu.make_async_copy(stage, stage, load_sem.at[0]).wait()
    pl.semaphore_wait(barrier, LINE - 1 + 1 + PARTS - 1)

    slot_of_band = lax.rem(band, LINE)
    opposite = along(ACROSS)

    def to_partner(src, slot):
        return remote(src, paired.at[slot], send_sem.at[0], pair_sem.at[slot], "band", partner)

    def onward(src, to):
        return remote(src, heard.at[slot_of_band], send_sem.at[6], heard_sem.at[slot_of_band], "band", to)

    remote(stage.at[partner_of(opposite)], crossed, send_sem.at[7], cross_sem, "band", opposite).start()
    onward(stage.at[opposite], opposite).start()
    for step in BESIDE:
        at = along(step)
        to_partner(stage.at[partner_of(at)], lax.rem(at, LINE)).start()
    loads[0].wait()
    start_phi(kernel_table, wide_table, table_pair)
    make_phi(0, 7, table_pair, phi)
    for i, step in enumerate(BESIDE):
        to = along(step)
        slot = lax.rem(to, LINE)
        wait_given(to_partner(stage.at[to], slot))
        passed[slot] = paired[slot] + stage[to]
        onward(passed.at[slot], to).start()
        make_phi(7 + i, 8 + i, table_pair, phi)
    wait_given(remote(crossed, crossed, send_sem.at[7], cross_sem, "band", opposite))
    passed[slot_of_band] = stage[partner] + crossed[...]
    to_partner(passed.at[slot_of_band], slot_of_band).start()
    make_phi(13, TILES // 2, table_pair, phi)
    for load in loads[1:]:
        load.wait()
    density = stage[band]
    for step in FAR_FIRST:
        slot = lax.rem(band + LINE - step, LINE)
        wait_given(remote(heard.at[slot], heard.at[slot], send_sem.at[6], heard_sem.at[slot], "band", partner))
        density = density + heard[slot]
    wait_given(to_partner(passed.at[slot_of_band], slot_of_band))
    density = density + paired[slot_of_band]
    z_table, z_back_table, y_table, x_table = (table.at[i] for i in range(4))

    def z_step(chunk):
        waves = z_forward_chunk(density, index[...], [weights[i] for i in range(4)], z_table[...], chunk)
        sent_a[0, :, chunk] = waves[:, 0]
        sent_a[1, :, chunk] = waves[:, 1]
        send_chunk("band", sent_a, got_a, 0, chunk, send_sem.at[1], sem_a)

    def z_later(chunk):
        send_chunk("band", sent_a, got_a, 1, chunk, send_sem.at[1], sem_a)

    def y_step(half):
        def step(chunk):
            wait_chunk("band", got_a, half, chunk, send_sem.at[1], sem_a)
            sent_b[half, :, chunk] = y_chunk(got_a[half, :, chunk], y_table[...])
            send_chunk("grid", sent_b, got_b, half, chunk, send_sem.at[2], sem_b)

        return step

    def x_step(half):
        def step(chunk):
            wait_chunk("grid", got_b, half, chunk, send_sem.at[2], sem_b)
            waves = x_forward_chunk(got_b[half, :, chunk], x_table[...])
            spec[pl.ds(4 * chunk, 4), 2 * half : 2 * half + 2] = waves

        return step

    def x_back_step(half):
        def step(chunk):
            here = pl.ds(pl.multiple_of(128 * chunk, 128), 128)
            sent_c[half, :, chunk] = x_back_chunk(mixed[half, here, :], x_table[...])
            send_chunk("grid", sent_c, got_c, half, chunk, send_sem.at[3], sem_c)

        return step

    def y_back_step(half):
        def step(chunk):
            wait_chunk("grid", got_c, half, chunk, send_sem.at[3], sem_c)
            sent_d[half, :, chunk] = y_chunk(got_c[half, :, chunk], y_table[...])
            send_chunk("band", sent_d, got_d, half, chunk, send_sem.at[4], sem_d)

        return step

    y_a, y_b, x_a, x_b = y_step(0), y_step(1), x_step(0), x_step(1)
    x_back_a, x_back_b, y_back_a = x_back_step(0), x_back_step(1), y_back_step(0)
    each(z_step)
    each(z_later)
    each(y_a)
    x_a(0)
    each(lambda chunk: x_a(chunk + 1), y_b, last=3)
    x_a(4)
    mix(0, phi, spec, mixed)
    x_back_a(0)
    y_b(3)
    each(x_back_a, first=1, last=3)
    y_b(4)
    each(x_back_a, first=3)
    each(x_b, last=2)
    each(y_back_a, lambda chunk: x_b(chunk + 2), last=3)
    mix(1, phi, spec, mixed)
    each(x_back_b, lambda chunk: y_back_a(chunk + 3), last=2)
    each(x_back_b, first=2)
    each(y_back_step(1))

    def z_back_step(chunk, so_far):
        for half in range(2):
            wait_chunk("band", got_d, half, chunk, send_sem.at[4], sem_d)
        block = jnp.concatenate([got_d[half, :, chunk][:, None] for half in range(2)], axis=1)
        return so_far + z_back_chunk(block, index[...], [slopes[i] for i in range(4)], z_back_table[...], chunk)

    out[:, rows, :] = lax.fori_loop(0, CHUNKS, z_back_step, jnp.zeros((8, 8, 128), F32))

    def give(block, target):
        piece = out.at[:, rows_of(block), :]
        return remote(piece, piece, send_sem.at[5], out_sem.at[block], "band", target)

    give(band, partner).start()
    for step in (*BESIDE_NEAR, ACROSS):
        give(band, along(step)).start()
    for i, step in enumerate(BESIDE_NEAR):
        origin = along(LINE - step)
        wait_given(give(origin, partner))
        give(origin, partner).start()
        if i == 1:
            wait_given(give(partner, partner))
            give(partner, opposite).start()
    wait_given(give(opposite, partner))
    for step in (*BESIDE_NEAR, ACROSS):
        wait_given(give(partner_of(along(LINE - step)), partner))
    wait_sent("grid", sent_b, send_sem.at[2], sem_b)
    wait_sent("grid", sent_c, send_sem.at[3], sem_c)
    wait_sent("band", sent_a, send_sem.at[1], sem_a)
    wait_sent("band", sent_d, send_sem.at[4], sem_d)
    rest = passed.at[pl.ds(0, LINE - 1)]
    remote(rest, rest, send_sem.at[0], pair_sem.at[0], "band", partner).wait_send()
    remote(rest, rest, send_sem.at[6], heard_sem.at[0], "band", partner).wait_send()
    remote(crossed, crossed, send_sem.at[7], cross_sem, "band", partner).wait_send()
    rest = stage.at[pl.ds(0, PARTS - 1)]
    remote(rest, rest, send_sem.at[5], out_sem.at[0], "band", partner).wait_send()


BLOCKS = (2, PARTS, CHUNKS, 8, 128)


def per_device(partial_density, node_index, node_weight, node_slope, kernel_table):
    constants = jnp.asarray(tables())
    args = [partial_density, node_index, node_weight, node_slope, kernel_table, constants]
    anywhere = pl.BlockSpec(memory_space=pl.ANY)
    vmem = pltpu.VMEM
    return pl.pallas_call(
        body,
        out_shape=pltpu.VMEM((8, N, N), F32),
        in_specs=[anywhere] * len(args),
        out_specs=pl.BlockSpec(memory_space=pltpu.VMEM),
        scratch_shapes=[
            vmem((PARTS, 8, 8, 128), F32),
            *[vmem((LINE, 8, 8, 128), F32)] * 3,
            vmem((8, 8, 128), F32),
            vmem((8, 8, 128), jnp.int32),
            vmem((4, 8, 8, 128), F32),
            vmem((4, 8, 8, 128), F32),
            vmem(kernel_table.shape, F32),
            vmem(constants.shape, constants.dtype),
            *[vmem(BLOCKS, F32)] * 8,
            vmem((480, 128), F32),
            vmem((480, 256), BF16),
            vmem((TILES, 480, 128), F32),
            vmem((NA, 4, 2, 8, 128), F32),
            vmem((2, 768, 128), F32),
            pltpu.SemaphoreType.DMA((6,)),
            pltpu.SemaphoreType.DMA((8,)),
            pltpu.SemaphoreType.DMA((LINE,)),
            pltpu.SemaphoreType.DMA((LINE,)),
            pltpu.SemaphoreType.DMA,
            *[pltpu.SemaphoreType.DMA((2, CHUNKS))] * 4,
            pltpu.SemaphoreType.DMA((PARTS,)),
        ],
        compiler_params=pltpu.CompilerParams(
            collective_id=0, has_side_effects=True, vmem_limit_bytes=60000 * 1024
        ),
    )(*args)


def solution(mesh):
    placed = (
        P("band", "grid", None, None),
        P("grid", None, None),
        P(None, "grid", None, None),
        P(None, "grid", None, None),
        P(),
    )
    return jax.shard_map(
        per_device, mesh=mesh, in_specs=placed, out_specs=P("grid", None, None), check_vma=False
    )
```

```python
import functools

import jax
import jax.numpy as jnp
import numpy as np
from jax import lax
from jax.experimental import pallas as pl
from jax.experimental.pallas import tpu as pltpu
from jax.sharding import PartitionSpec as P

N = 128
NA = 20
F32 = jnp.float32
BF16 = jnp.bfloat16


def halves(table):
    table = np.asarray(table, np.float32)
    high = table.astype(BF16)
    low = (table - high.astype(np.float32)).astype(BF16)
    return high, low


def lane_wave(shared):
    lane = np.arange(128)
    bit = [(lane >> b) & 1 for b in range(7)]
    if shared:
        owner = bit[6] * 8 + bit[5] * 4 + bit[2] * 2 + bit[1]
        pair = owner * 4 + bit[0] * 2 + bit[4]
    else:
        owner = bit[6] * 8 + bit[5] * 4 + bit[4] * 2 + bit[2]
        pair = owner * 4 + bit[1] * 2 + bit[0]
    return np.where(bit[3] == 0, pair, np.where(pair == 0, 64, N - pair))


def cas(k, n):
    angle = 2 * np.pi * ((k[:, None] * n[None]) % N) / N
    return np.cos(angle) + np.sin(angle)


def right_form(table):
    high, low = halves(table)
    return np.block([[high, low], [high, np.zeros_like(low)]])


def left_form(table):
    high, low = halves(table)
    return np.block([[high, high], [low, np.zeros_like(low)]])


def tables():
    at = np.arange(N)
    line = cas(at, at)
    z = [cas(at, lane_wave(shared)) for shared in (False, True)]
    waves = [right_form(table) for table in z] + [right_form(table.T / float(N) ** 3) for table in z]
    return np.stack(waves + [left_form(line), right_form(line)])


def split(value):
    high = value.astype(BF16)
    low = (value - high.astype(F32)).astype(BF16)
    return high, low


def mm(a, b):
    return jnp.dot(a, b, preferred_element_type=F32)


def lanes_of(shape):
    return lax.broadcasted_iota(jnp.int32, shape, len(shape) - 1)


def exchange(v, pairs):
    count = v.shape[0]
    for index_bit, lane_bit in pairs:
        inner, step = 1 << index_bit, 1 << lane_bit
        rows = count // 2 * 8
        w = v.reshape(count // (2 * inner), 2, inner, 8, 128)
        a = w[:, 0].reshape(rows, 128)
        b = w[:, 1].reshape(rows, 128)
        keep = (lanes_of((rows, 128)) >> lane_bit) & 1 == 0
        new_a = jnp.where(keep, a, pltpu.roll(b, step, 1))
        new_b = jnp.where(keep, pltpu.roll(a, 128 - step, 1), b)
        shape = (count // (2 * inner), 1, inner, 8, 128)
        v = jnp.concatenate([new_a.reshape(shape), new_b.reshape(shape)], axis=1).reshape(count, 8, 128)
    return v


def exchange_groups(v):
    group = lanes_of((8, 128)) >> 3
    skewed = [v[i] if i == 0 else pltpu.roll(v[i], 8 * i, 1) for i in range(16)]
    for bit in range(4):
        take = (group >> bit) & 1 == 1
        skewed = [jnp.where(take, skewed[(i + (1 << bit)) % 16], skewed[i]) for i in range(16)]
    out = [skewed[-i % 16] if i == 0 else pltpu.roll(skewed[-i % 16], 128 - 8 * i, 1) for i in range(16)]
    return jnp.concatenate([piece[None] for piece in out], axis=0)


GROUP_START = (0, 8, 16)
GROUP_SIZE = (8, 8, 4)
Z_PAIRS = {8: ((5, 6), (4, 5), (3, 4), (2, 2), (1, 1), (0, 0)), 4: ((4, 6), (3, 5), (2, 2), (1, 1), (0, 0))}


def slot_of(group, pair):
    return 5 * (pair // 2) + (0 if group == 2 else 1 + 2 * (pair % 2) + group)


def pairs_of(group):
    return (0, 2) if group == 2 else (0, 1, 2, 3)


def node_coefficient(node, index, weights):
    total = None
    for offset in range(4):
        term = jnp.where(index + (offset - 1) == node, weights[offset], 0.0)
        total = term if total is None else total + term
    return total


def right(rows, table):
    high, low = split(rows)
    wide = mm(jnp.concatenate([high, low], axis=1), table)
    return wide[:, :128] + wide[:, 128:]


def left(table, columns):
    high, low = split(columns)
    tall = mm(table, jnp.concatenate([high, low], axis=0))
    return tall[:128] + tall[128:]


def z_forward_group(density, index, weights, table, group):
    size = GROUP_SIZE[group]
    fields = [density * node_coefficient(GROUP_START[group] + i, index, weights) for i in range(size)]
    theta = jnp.concatenate(fields, axis=0).reshape(64 * size, 128)
    waves = right(theta, table).reshape(8 * size, 8, 128)
    return exchange(waves, Z_PAIRS[size]).reshape(PARTS, size // 2, 8, 128)


def z_back_group(block, index, slopes, table, group):
    size = GROUP_SIZE[group]
    waves = exchange(block.reshape(8 * size, 8, 128), Z_PAIRS[size]).reshape(64 * size, 128)
    field = right(waves, table).reshape(size, 8, 8, 128)
    total = None
    for i in range(size):
        term = field[i] * node_coefficient(GROUP_START[group] + i, index, slopes)
        total = term if total is None else total + term
    return total


def y_chunk(block, table):
    return left(table, block.reshape(128, 128)).reshape(PARTS, 8, 128)


def x_forward_chunk(block, table):
    return right(exchange_groups(block).reshape(128, 128), table)


def x_back_chunk(waves, table):
    return exchange_groups(right(waves, table).reshape(PARTS, 8, 128))


def shell_tile(tile):
    band, grid = lax.axis_index("band"), lax.axis_index("grid")
    second = tile >= 32
    fz = 4 * band + jnp.where(second, 0, tile // 8)
    fz = jnp.where(second & (band == 0), 64, fz)
    ky = 8 * grid + lax.rem(tile, 8)
    fy = jnp.where(ky < 64, ky, ky - 128)
    kx = lanes_of((128, 128))
    fx = jnp.where(kx < 64, kx, kx - 128)
    root = jnp.sqrt((fz * fz + fy * fy + fx * fx).astype(F32))
    shell = lax.broadcasted_iota(jnp.int32, (128, 128), 0).astype(F32)
    return jnp.maximum(1.0 - jnp.abs(root - shell), 0.0)


def start_phi(kernel_table, wide_table, table_pair):
    wide_table[...] = jnp.zeros((480, 128), F32)
    for a in range(NA):
        wide_table[24 * a : 24 * a + NA, : kernel_table.shape[2]] = kernel_table[a]
    high, low = split(wide_table[...])
    table_pair[...] = jnp.concatenate([high, low], axis=1)


def make_phi(first, last, table_pair, phi):
    def step(i, carry):
        wide = table_pair[...]
        tiles = jnp.concatenate([shell_tile(2 * i), shell_tile(2 * i + 1)], axis=1)
        tiles_high, tiles_low = split(tiles)
        values = mm(wide, jnp.concatenate([tiles_high, tiles_high], axis=0)) + mm(wide[:, :128], tiles_low)
        phi[2 * i] = values[:, :128]
        phi[2 * i + 1] = values[:, 128:]
        return carry

    lax.fori_loop(first, last, step, 0)


def mix(pair, phi, spec, mixed):
    def step(row, carry):
        sums = [None, None]
        for a in range(NA):
            kernel = phi[8 * pair + row, 24 * a : 24 * a + 24]
            kernels = kernel, phi[32 + row, 24 * a : 24 * a + 24] if pair == 0 else kernel
            for member in range(2):
                term = kernels[member] * spec[a, pair, member, pl.ds(row, 1), :]
                sums[member] = term if sums[member] is None else sums[member] + term
        for member in range(2):
            at = row + 8 * member
            for group in range(2):
                mixed[slot_of(group, pair), pl.ds(at, 8, stride=16), :] = sums[member][8 * group : 8 * group + 8]
            mixed[slot_of(2, pair), pl.ds(at + 16 * (pair % 2), 4, stride=32), :] = sums[member][16:20]
        return carry

    lax.fori_loop(0, 8, step, 0)


MESH = pl.DeviceIdType.MESH
PARTS = 16
TILES = 40
SLOTS = 10


LINE = 8
FAR_FIRST = (4, 3, 5, 2, 6, 1, 7)
BESIDE = (3, 5, 2, 6, 1, 7)
BESIDE_NEAR = (1, 7, 2, 6, 3, 5)
ACROSS = 4


def z_peers(band):
    first = band // LINE * LINE
    return lambda step: first + lax.rem(band + step, LINE)


def partner_of(band):
    return lax.rem(band + LINE, PARTS)


def peers(me):
    return lambda step: lax.rem(me + step, PARTS)


def greet(barrier):
    band = lax.axis_index("band")
    peer = peers(lax.axis_index("grid"))
    along = z_peers(band)

    def grid_one(step, carry):
        pl.semaphore_signal(barrier, inc=1, device_id={"grid": peer(step)}, device_id_type=MESH)
        return carry

    def band_one(step, carry):
        pl.semaphore_signal(barrier, inc=1, device_id={"band": along(step)}, device_id_type=MESH)
        return carry

    lax.fori_loop(1, LINE, band_one, 0)
    pl.semaphore_signal(barrier, inc=1, device_id={"band": partner_of(band)}, device_id_type=MESH)
    lax.fori_loop(1, PARTS, grid_one, 0)


def remote(src, dst, send_sem, recv_sem, axis, target):
    return pltpu.make_async_remote_copy(
        src_ref=src, dst_ref=dst, send_sem=send_sem, recv_sem=recv_sem, device_id={axis: target}, device_id_type=MESH
    )


def wait_given(copy):
    copy.wait_recv()


def send_chunk(axis, sent, got, slot, send_sem, recv_sem):
    me = lax.axis_index(axis)
    peer = peers(me)
    got[slot, me] = sent[slot, me]
    for step in range(1, PARTS):
        to = peer(step)
        remote(sent.at[slot, to], got.at[slot, me], send_sem, recv_sem.at[slot], axis, to).start()


def wait_chunk(axis, got, slot, send_sem, recv_sem):
    rest = got.at[slot, pl.ds(0, PARTS - 1)]
    remote(rest, rest, send_sem, recv_sem.at[slot], axis, 0).wait_recv()


def wait_sent(axis, sent, send_sem, recv_sem):
    rest = sent.at[:, pl.ds(0, PARTS - 1)]
    remote(rest, rest, send_sem, recv_sem.at[0], axis, 0).wait_send()


def body(
    partial, node_index, node_weight, node_slope, kernel_hbm, tables_hbm, out,
    stage, paired, passed, heard, crossed, index, weights, slopes, kernel_table, table,
    sent_a, got_a, sent_b, got_b, sent_c, got_c, sent_d, got_d,
    wide_table, table_pair, phi, spec, mixed,
    load_sem, send_sem, pair_sem, heard_sem, cross_sem, sem_a, sem_b, sem_c, sem_d, out_sem,
):
    band = lax.axis_index("band")
    barrier = pltpu.get_barrier_semaphore()
    greet(barrier)
    partner, along = partner_of(band), z_peers(band)

    def rows_of(block):
        return pl.ds(pl.multiple_of(8 * block, 8), 8)

    rows = rows_of(band)

    def cut(step, carry):
        pltpu.make_async_copy(partial.at[0, :, rows_of(step), :], stage.at[step], load_sem.at[0]).start()
        return carry

    lax.fori_loop(0, PARTS, cut, 0)
    loads = [
        pltpu.make_async_copy(src, dst, load_sem.at[i + 1])
        for i, (src, dst) in enumerate(
            (
                (kernel_hbm, kernel_table),
                (node_index.at[:, rows, :], index),
                (node_weight.at[:, :, rows, :], weights),
                (node_slope.at[:, :, rows, :], slopes),
                (tables_hbm, table),
            )
        )
    ]
    for load in loads:
        load.start()
    pltpu.make_async_copy(stage, stage, load_sem.at[0]).wait()
    pl.semaphore_wait(barrier, LINE - 1 + 1 + PARTS - 1)

    slot_of_band = lax.rem(band, LINE)
    opposite = along(ACROSS)

    def to_partner(src, slot):
        return remote(src, paired.at[slot], send_sem.at[0], pair_sem.at[slot], "band", partner)

    def onward(src, to):
        return remote(src, heard.at[slot_of_band], send_sem.at[6], heard_sem.at[slot_of_band], "band", to)

    remote(stage.at[partner_of(opposite)], crossed, send_sem.at[7], cross_sem, "band", opposite).start()
    onward(stage.at[opposite], opposite).start()
    for step in BESIDE:
        at = along(step)
        to_partner(stage.at[partner_of(at)], lax.rem(at, LINE)).start()
    loads[0].wait()
    start_phi(kernel_table, wide_table, table_pair)
    make_phi(0, 7, table_pair, phi)
    for i, step in enumerate(BESIDE):
        to = along(step)
        slot = lax.rem(to, LINE)
        wait_given(to_partner(stage.at[to], slot))
        passed[slot] = paired[slot] + stage[to]
        onward(passed.at[slot], to).start()
        make_phi(7 + i, 8 + i, table_pair, phi)
    wait_given(remote(crossed, crossed, send_sem.at[7], cross_sem, "band", opposite))
    passed[slot_of_band] = stage[partner] + crossed[...]
    to_partner(passed.at[slot_of_band], slot_of_band).start()
    make_phi(13, TILES // 2, table_pair, phi)
    for load in loads[1:]:
        load.wait()
    density = stage[band]
    for step in FAR_FIRST:
        slot = lax.rem(band + LINE - step, LINE)
        wait_given(remote(heard.at[slot], heard.at[slot], send_sem.at[6], heard_sem.at[slot], "band", partner))
        density = density + heard[slot]
    wait_given(to_partner(passed.at[slot_of_band], slot_of_band))
    density = density + paired[slot_of_band]
    tabs = [table.at[i] for i in range(6)]
    y_table, x_table = tabs[4:]
    tabs = {0: (tabs[0], tabs[2]), 1: (tabs[0], tabs[2]), 2: (tabs[1], tabs[3])}

    def z_step(group):
        values = [weights[i] for i in range(4)]
        waves = z_forward_group(density, index[...], values, tabs[group][0][...], group)
        for i, pair in enumerate(pairs_of(group)):
            sent_a[slot_of(group, pair)] = waves[:, i]

    def z_send(slot):
        send_chunk("band", sent_a, got_a, slot, send_sem.at[1], sem_a)

    def y_step(slot):
        wait_chunk("band", got_a, slot, send_sem.at[1], sem_a)
        sent_b[slot] = y_chunk(got_a[slot], y_table[...])
        send_chunk("grid", sent_b, got_b, slot, send_sem.at[2], sem_b)

    def x_step(group, pair):
        slot = slot_of(group, pair)
        wait_chunk("grid", got_b, slot, send_sem.at[2], sem_b)
        waves = x_forward_chunk(got_b[slot], x_table[...])
        if group == 2:
            spec[16:20, pair : pair + 2] = waves.reshape(4, 2, 2, 8, 128)
        else:
            spec[8 * group : 8 * group + 8, pair] = waves.reshape(8, 2, 8, 128)

    def x_back_step(group, pair):
        slot = slot_of(group, pair)
        sent_c[slot] = x_back_chunk(mixed[slot], x_table[...])
        send_chunk("grid", sent_c, got_c, slot, send_sem.at[3], sem_c)

    def y_back_step(group, pair):
        slot = slot_of(group, pair)
        wait_chunk("grid", got_c, slot, send_sem.at[3], sem_c)
        sent_d[slot] = y_chunk(got_c[slot], y_table[...])
        send_chunk("band", sent_d, got_d, slot, send_sem.at[4], sem_d)

    def z_back_step(group):
        blocks = []
        for pair in pairs_of(group):
            slot = slot_of(group, pair)
            wait_chunk("band", got_d, slot, send_sem.at[4], sem_d)
            blocks.append(got_d[slot][:, None])
        block = jnp.concatenate(blocks, axis=1)
        return z_back_group(block, index[...], [slopes[i] for i in range(4)], tabs[group][1][...], group)

    def mix_step(pair):
        mix(pair, phi, spec, mixed)

    z_step(2)
    z_send(0)
    z_step(0)
    z_send(1)
    z_step(1)
    for slot in range(2, SLOTS):
        z_send(slot)
    y, x, xb, yb = y_step, x_step, x_back_step, y_back_step
    plan = (
        (y, 0), (y, 1), (y, 2), (y, 3), (x, 2, 0), (y, 4), (x, 0, 0), (y, 5), (x, 1, 0), (mix_step, 0),
        (xb, 0, 0), (y, 6), (xb, 1, 0), (x, 0, 1), (y, 7), (x, 1, 1), (mix_step, 1),
        (xb, 0, 1), (y, 8), (xb, 1, 1), (xb, 2, 0), (x, 2, 2), (y, 9), (yb, 0, 0), (x, 0, 2), (yb, 1, 0), (x, 1, 2),
        (mix_step, 2), (xb, 0, 2), (yb, 0, 1), (xb, 1, 2), (yb, 1, 1), (x, 0, 3), (yb, 2, 0), (x, 1, 3),
        (mix_step, 3), (xb, 0, 3), (xb, 1, 3), (xb, 2, 2),
        (yb, 0, 2), (yb, 1, 2), (yb, 0, 3), (yb, 1, 3), (yb, 2, 2),
    )
    for step, *what in plan:
        step(*what)
    out[:, rows, :] = z_back_step(0) + z_back_step(1) + z_back_step(2)

    def give(block, target):
        piece = out.at[:, rows_of(block), :]
        return remote(piece, piece, send_sem.at[5], out_sem.at[block], "band", target)

    give(band, partner).start()
    for step in (*BESIDE_NEAR, ACROSS):
        give(band, along(step)).start()
    for i, step in enumerate(BESIDE_NEAR):
        origin = along(LINE - step)
        wait_given(give(origin, partner))
        give(origin, partner).start()
        if i == 1:
            wait_given(give(partner, partner))
            give(partner, opposite).start()
    wait_given(give(opposite, partner))
    for step in (*BESIDE_NEAR, ACROSS):
        wait_given(give(partner_of(along(LINE - step)), partner))
    wait_sent("grid", sent_b, send_sem.at[2], sem_b)
    wait_sent("grid", sent_c, send_sem.at[3], sem_c)
    wait_sent("band", sent_a, send_sem.at[1], sem_a)
    wait_sent("band", sent_d, send_sem.at[4], sem_d)
    rest = passed.at[pl.ds(0, LINE - 1)]
    remote(rest, rest, send_sem.at[0], pair_sem.at[0], "band", partner).wait_send()
    remote(rest, rest, send_sem.at[6], heard_sem.at[0], "band", partner).wait_send()
    remote(crossed, crossed, send_sem.at[7], cross_sem, "band", partner).wait_send()
    rest = stage.at[pl.ds(0, PARTS - 1)]
    remote(rest, rest, send_sem.at[5], out_sem.at[0], "band", partner).wait_send()


BLOCKS = (SLOTS, PARTS, 8, 128)


def per_device(partial_density, node_index, node_weight, node_slope, kernel_table):
    constants = jnp.asarray(tables())
    args = [partial_density, node_index, node_weight, node_slope, kernel_table, constants]
    anywhere = pl.BlockSpec(memory_space=pl.ANY)
    vmem = pltpu.VMEM
    return pl.pallas_call(
        body,
        out_shape=pltpu.VMEM((8, N, N), F32),
        in_specs=[anywhere] * len(args),
        out_specs=pl.BlockSpec(memory_space=pltpu.VMEM),
        scratch_shapes=[
            vmem((PARTS, 8, 8, 128), F32),
            *[vmem((LINE, 8, 8, 128), F32)] * 3,
            vmem((8, 8, 128), F32),
            vmem((8, 8, 128), jnp.int32),
            vmem((4, 8, 8, 128), F32),
            vmem((4, 8, 8, 128), F32),
            vmem(kernel_table.shape, F32),
            vmem(constants.shape, constants.dtype),
            *[vmem(BLOCKS, F32)] * 8,
            vmem((480, 128), F32),
            vmem((480, 256), BF16),
            vmem((TILES, 480, 128), F32),
            vmem((NA, 4, 2, 8, 128), F32),
            vmem((SLOTS, 128, 128), F32),
            pltpu.SemaphoreType.DMA((6,)),
            pltpu.SemaphoreType.DMA((8,)),
            pltpu.SemaphoreType.DMA((LINE,)),
            pltpu.SemaphoreType.DMA((LINE,)),
            pltpu.SemaphoreType.DMA,
            *[pltpu.SemaphoreType.DMA((SLOTS,))] * 4,
            pltpu.SemaphoreType.DMA((PARTS,)),
        ],
        compiler_params=pltpu.CompilerParams(
            collective_id=0, has_side_effects=True, vmem_limit_bytes=60000 * 1024
        ),
    )(*args)


def solution(mesh):
    placed = (
        P("band", "grid", None, None),
        P("grid", None, None),
        P(None, "grid", None, None),
        P(None, "grid", None, None),
        P(),
    )
    return jax.shard_map(
        per_device, mesh=mesh, in_specs=placed, out_specs=P("grid", None, None), check_vma=False
    )
```

```python
import functools

import jax
import jax.numpy as jnp
import numpy as np
from jax import lax
from jax.experimental import pallas as pl
from jax.experimental.pallas import tpu as pltpu
from jax.sharding import PartitionSpec as P

N = 128
NA = 20
F32 = jnp.float32
BF16 = jnp.bfloat16


def halves(table):
    table = np.asarray(table, np.float32)
    high = table.astype(BF16)
    low = (table - high.astype(np.float32)).astype(BF16)
    return high, low


def lane_wave(shared):
    lane = np.arange(128)
    bit = [(lane >> b) & 1 for b in range(7)]
    if shared:
        owner = bit[6] * 8 + bit[5] * 4 + bit[2] * 2 + bit[1]
        pair = owner * 4 + bit[0] * 2 + bit[4]
    else:
        owner = bit[6] * 8 + bit[5] * 4 + bit[4] * 2 + bit[2]
        pair = owner * 4 + bit[1] * 2 + bit[0]
    return np.where(bit[3] == 0, pair, np.where(pair == 0, 64, N - pair))


def cas(k, n):
    angle = 2 * np.pi * ((k[:, None] * n[None]) % N) / N
    return np.cos(angle) + np.sin(angle)


def right_form(table):
    high, low = halves(table)
    return np.block([[high, low], [high, np.zeros_like(low)]])


def left_form(table):
    high, low = halves(table)
    return np.block([[high, high], [low, np.zeros_like(low)]])


def tables():
    at = np.arange(N)
    line = cas(at, at)
    z = [cas(at, lane_wave(shared)) for shared in (False, True)]
    waves = [right_form(table) for table in z] + [right_form(table.T / float(N) ** 3) for table in z]
    return np.stack(waves + [left_form(line), right_form(line)])


def split(value):
    high = value.astype(BF16)
    low = (value - high.astype(F32)).astype(BF16)
    return high, low


def mm(a, b):
    return jnp.dot(a, b, preferred_element_type=F32)


def lanes_of(shape):
    return lax.broadcasted_iota(jnp.int32, shape, len(shape) - 1)


def exchange(v, pairs):
    count = v.shape[0]
    for index_bit, lane_bit in pairs:
        inner, step = 1 << index_bit, 1 << lane_bit
        rows = count // 2 * 8
        w = v.reshape(count // (2 * inner), 2, inner, 8, 128)
        a = w[:, 0].reshape(rows, 128)
        b = w[:, 1].reshape(rows, 128)
        keep = (lanes_of((rows, 128)) >> lane_bit) & 1 == 0
        new_a = jnp.where(keep, a, pltpu.roll(b, step, 1))
        new_b = jnp.where(keep, pltpu.roll(a, 128 - step, 1), b)
        shape = (count // (2 * inner), 1, inner, 8, 128)
        v = jnp.concatenate([new_a.reshape(shape), new_b.reshape(shape)], axis=1).reshape(count, 8, 128)
    return v


def exchange_groups(v):
    group = lanes_of((8, 128)) >> 3
    skewed = [v[i] if i == 0 else pltpu.roll(v[i], 8 * i, 1) for i in range(16)]
    for bit in range(4):
        take = (group >> bit) & 1 == 1
        skewed = [jnp.where(take, skewed[(i + (1 << bit)) % 16], skewed[i]) for i in range(16)]
    out = [skewed[-i % 16] if i == 0 else pltpu.roll(skewed[-i % 16], 128 - 8 * i, 1) for i in range(16)]
    return jnp.concatenate([piece[None] for piece in out], axis=0)


GROUP_START = (0, 8, 16)
GROUP_SIZE = (8, 8, 4)
Z_PAIRS = {8: ((5, 6), (4, 5), (3, 4), (2, 2), (1, 1), (0, 0)), 4: ((4, 6), (3, 5), (2, 2), (1, 1), (0, 0))}


def slot_of(group, pair):
    return 5 * (pair // 2) + (0 if group == 2 else 1 + 2 * (pair % 2) + group)


def pairs_of(group):
    return (0, 2) if group == 2 else (0, 1, 2, 3)


def node_coefficient(node, index, weights):
    total = None
    for offset in range(4):
        term = jnp.where(index + (offset - 1) == node, weights[offset], 0.0)
        total = term if total is None else total + term
    return total


def right(rows, table):
    high, low = split(rows)
    wide = mm(jnp.concatenate([high, low], axis=1), table)
    return wide[:, :128] + wide[:, 128:]


def left(table, columns):
    high, low = split(columns)
    tall = mm(table, jnp.concatenate([high, low], axis=0))
    return tall[:128] + tall[128:]


def z_forward_group(density, index, weights, table, group):
    size = GROUP_SIZE[group]
    fields = [density * node_coefficient(GROUP_START[group] + i, index, weights) for i in range(size)]
    theta = jnp.concatenate(fields, axis=0).reshape(64 * size, 128)
    waves = right(theta, table).reshape(8 * size, 8, 128)
    return exchange(waves, Z_PAIRS[size]).reshape(PARTS, size // 2, 8, 128)


def z_back_group(block, index, slopes, table, group):
    size = GROUP_SIZE[group]
    waves = exchange(block.reshape(8 * size, 8, 128), Z_PAIRS[size]).reshape(64 * size, 128)
    field = right(waves, table).reshape(size, 8, 8, 128)
    total = None
    for i in range(size):
        term = field[i] * node_coefficient(GROUP_START[group] + i, index, slopes)
        total = term if total is None else total + term
    return total


def y_chunk(block, table):
    return left(table, block.reshape(128, 128)).reshape(PARTS, 8, 128)


def x_forward_chunk(block, table):
    return right(exchange_groups(block).reshape(128, 128), table)


def x_back_chunk(waves, table):
    return exchange_groups(right(waves, table).reshape(PARTS, 8, 128))


def shell_tile(tile):
    band, grid = lax.axis_index("band"), lax.axis_index("grid")
    second = tile >= 32
    fz = 4 * band + jnp.where(second, 0, tile // 8)
    fz = jnp.where(second & (band == 0), 64, fz)
    ky = 8 * grid + lax.rem(tile, 8)
    fy = jnp.where(ky < 64, ky, ky - 128)
    kx = lanes_of((128, 128))
    fx = jnp.where(kx < 64, kx, kx - 128)
    root = jnp.sqrt((fz * fz + fy * fy + fx * fx).astype(F32))
    shell = lax.broadcasted_iota(jnp.int32, (128, 128), 0).astype(F32)
    return jnp.maximum(1.0 - jnp.abs(root - shell), 0.0)


def start_phi(kernel_table, wide_table, table_pair):
    wide_table[...] = jnp.zeros((480, 128), F32)
    for a in range(NA):
        wide_table[24 * a : 24 * a + NA, : kernel_table.shape[2]] = kernel_table[a]
    high, low = split(wide_table[...])
    table_pair[...] = jnp.concatenate([high, low], axis=1)


def make_phi(first, last, table_pair, phi):
    def step(i, carry):
        wide = table_pair[...]
        tiles = jnp.concatenate([shell_tile(2 * i), shell_tile(2 * i + 1)], axis=1)
        tiles_high, tiles_low = split(tiles)
        values = mm(wide, jnp.concatenate([tiles_high, tiles_high], axis=0)) + mm(wide[:, :128], tiles_low)
        phi[2 * i] = values[:, :128]
        phi[2 * i + 1] = values[:, 128:]
        return carry

    lax.fori_loop(first, last, step, 0)


def mix(pair, phi, spec, mixed):
    def step(row, carry):
        sums = [None, None]
        for a in range(NA):
            kernel = phi[8 * pair + row, 24 * a : 24 * a + 24]
            kernels = kernel, phi[32 + row, 24 * a : 24 * a + 24] if pair == 0 else kernel
            for member in range(2):
                term = kernels[member] * spec[a, pair, member, pl.ds(row, 1), :]
                sums[member] = term if sums[member] is None else sums[member] + term
        for member in range(2):
            at = row + 8 * member
            for group in range(2):
                mixed[slot_of(group, pair), pl.ds(at, 8, stride=16), :] = sums[member][8 * group : 8 * group + 8]
            mixed[slot_of(2, pair), pl.ds(at + 16 * (pair % 2), 4, stride=32), :] = sums[member][16:20]
        return carry

    lax.fori_loop(0, 8, step, 0)


MESH = pl.DeviceIdType.MESH
PARTS = 16
TILES = 40
SLOTS = 10


LINE = 8
SUM_BESIDE, SUM_ACROSS, SUM_PIECES = (4, 3, 5, 1, 7), (2, 6), 2
GIVE_BESIDE, GIVE_ACROSS, GIVE_PIECES = (4, 1, 7, 3, 5), (2, 6), 2


def z_peers(band):
    first = band // LINE * LINE
    return lambda step: first + lax.rem(band + step, LINE)


def partner_of(band):
    return lax.rem(band + LINE, PARTS)


def peers(me):
    return lambda step: lax.rem(me + step, PARTS)


def far_first(axis):
    me = lax.axis_index(axis)
    if axis == "band":
        column, z = me // LINE, lax.rem(me, LINE)
        order = sorted(
            ((dz, dx) for dz in range(LINE) for dx in range(2) if dz or dx), key=lambda d: -(min(d[0], LINE - d[0]) + 2 * d[1])
        )
        return [lax.rem(column + dx, 2) * LINE + lax.rem(z + dz, LINE) for dz, dx in order]
    y, x, core = me // 4, lax.rem(me // 2, 2), lax.rem(me, 2)
    order = sorted(
        ((dy, dx, dc) for dy in range(4) for dx in range(2) for dc in range(2) if dy or dx or dc),
        key=lambda d: -(min(d[0], 4 - d[0]) + d[1]),
    )
    return [lax.rem(y + dy, 4) * 4 + lax.rem(x + dx, 2) * 2 + lax.rem(core + dc, 2) for dy, dx, dc in order]


def greet(barrier):
    band = lax.axis_index("band")
    peer = peers(lax.axis_index("grid"))
    along = z_peers(band)

    def grid_one(step, carry):
        pl.semaphore_signal(barrier, inc=1, device_id={"grid": peer(step)}, device_id_type=MESH)
        return carry

    def band_one(step, carry):
        pl.semaphore_signal(barrier, inc=1, device_id={"band": along(step)}, device_id_type=MESH)
        return carry

    lax.fori_loop(1, LINE, band_one, 0)
    pl.semaphore_signal(barrier, inc=1, device_id={"band": partner_of(band)}, device_id_type=MESH)
    lax.fori_loop(1, PARTS, grid_one, 0)


def remote(src, dst, send_sem, recv_sem, axis, target):
    return pltpu.make_async_remote_copy(
        src_ref=src, dst_ref=dst, send_sem=send_sem, recv_sem=recv_sem, device_id={axis: target}, device_id_type=MESH
    )


def wait_given(copy):
    copy.wait_recv()


def send_chunk(axis, sent, got, slot, send_sem, recv_sem):
    me = lax.axis_index(axis)
    got[slot, me] = sent[slot, me]
    for to in far_first(axis):
        remote(sent.at[slot, to], got.at[slot, me], send_sem, recv_sem.at[slot], axis, to).start()


def wait_chunk(axis, got, slot, send_sem, recv_sem):
    rest = got.at[slot, pl.ds(0, PARTS - 1)]
    remote(rest, rest, send_sem, recv_sem.at[slot], axis, 0).wait_recv()


def wait_sent(axis, sent, send_sem, recv_sem):
    rest = sent.at[:, pl.ds(0, PARTS - 1)]
    remote(rest, rest, send_sem, recv_sem.at[0], axis, 0).wait_send()


def body(
    partial, node_index, node_weight, node_slope, kernel_hbm, tables_hbm, out,
    stage, paired, passed, heard, crossed, index, weights, slopes, kernel_table, table,
    sent_a, got_a, sent_b, got_b, sent_c, got_c, sent_d, got_d,
    wide_table, table_pair, phi, spec, mixed,
    load_sem, send_sem, pair_sem, heard_sem, cross_sem, sem_a, sem_b, sem_c, sem_d, out_sem,
):
    band = lax.axis_index("band")
    barrier = pltpu.get_barrier_semaphore()
    greet(barrier)
    partner, along = partner_of(band), z_peers(band)

    def rows_of(block):
        return pl.ds(pl.multiple_of(8 * block, 8), 8)

    rows = rows_of(band)

    def cut(step, carry):
        pltpu.make_async_copy(partial.at[0, :, rows_of(step), :], stage.at[step], load_sem.at[0]).start()
        return carry

    lax.fori_loop(0, PARTS, cut, 0)
    loads = [
        pltpu.make_async_copy(src, dst, load_sem.at[i + 1])
        for i, (src, dst) in enumerate(
            (
                (kernel_hbm, kernel_table),
                (node_index.at[:, rows, :], index),
                (node_weight.at[:, :, rows, :], weights),
                (node_slope.at[:, :, rows, :], slopes),
                (tables_hbm, table),
            )
        )
    ]
    for load in loads:
        load.start()
    pltpu.make_async_copy(stage, stage, load_sem.at[0]).wait()
    pl.semaphore_wait(barrier, LINE - 1 + 1 + PARTS - 1)

    slot_of_band = lax.rem(band, LINE)

    def piece_of(ref, i):
        return ref.at[pl.ds(8 // SUM_PIECES * i, 8 // SUM_PIECES)]

    pieces = range(SUM_PIECES)

    def to_partner(src, slot, i):
        return remote(
            piece_of(src, i), piece_of(paired.at[slot], i), send_sem.at[0], pair_sem.at[slot, i], "band", partner
        )

    def onward(src, to):
        return remote(src, heard.at[slot_of_band], send_sem.at[6], heard_sem.at[slot_of_band], "band", to)

    for step in SUM_ACROSS:
        to = along(step)
        cross = crossed.at[slot_of_band]
        remote(stage.at[partner_of(to)], cross, send_sem.at[7], cross_sem.at[slot_of_band], "band", to).start()
    for step in SUM_ACROSS:
        onward(stage.at[along(step)], along(step)).start()
    for step in SUM_BESIDE:
        at = along(step)
        for i in pieces:
            to_partner(stage.at[partner_of(at)], lax.rem(at, LINE), i).start()
    loads[0].wait()
    start_phi(kernel_table, wide_table, table_pair)
    make_phi(0, 7, table_pair, phi)
    for count, step in enumerate(SUM_BESIDE):
        to = along(step)
        slot = lax.rem(to, LINE)
        for i in pieces:
            wait_given(to_partner(stage.at[to], slot, i))
            part = pl.ds(8 // SUM_PIECES * i, 8 // SUM_PIECES)
            passed[slot, part] = paired[slot, part] + stage[to, part]
            remote(
                piece_of(passed.at[slot], i),
                piece_of(heard.at[slot_of_band], i),
                send_sem.at[6],
                heard_sem.at[slot_of_band],
                "band",
                to,
            ).start()
        make_phi(7 + count, 8 + count, table_pair, phi)
    own = stage[partner]
    for step in SUM_ACROSS:
        slot = lax.rem(band + LINE - step, LINE)
        cross = crossed.at[slot]
        wait_given(remote(cross, cross, send_sem.at[7], cross_sem.at[slot], "band", partner))
        own = own + crossed[slot]
    passed[slot_of_band] = own
    for i in pieces:
        to_partner(passed.at[slot_of_band], slot_of_band, i).start()
    make_phi(7 + len(SUM_BESIDE), TILES // 2, table_pair, phi)
    for load in loads[1:]:
        load.wait()
    density = stage[band]
    for step in (*SUM_ACROSS, *SUM_BESIDE):
        slot = lax.rem(band + LINE - step, LINE)
        wait_given(remote(heard.at[slot], heard.at[slot], send_sem.at[6], heard_sem.at[slot], "band", partner))
        density = density + heard[slot]
    for i in pieces:
        wait_given(to_partner(passed.at[slot_of_band], slot_of_band, i))
    density = density + paired[slot_of_band]
    tabs = [table.at[i] for i in range(6)]
    y_table, x_table = tabs[4:]
    tabs = {0: (tabs[0], tabs[2]), 1: (tabs[0], tabs[2]), 2: (tabs[1], tabs[3])}

    def z_step(group):
        values = [weights[i] for i in range(4)]
        waves = z_forward_group(density, index[...], values, tabs[group][0][...], group)
        for i, pair in enumerate(pairs_of(group)):
            sent_a[slot_of(group, pair)] = waves[:, i]

    def z_send(slot):
        send_chunk("band", sent_a, got_a, slot, send_sem.at[1], sem_a)

    def y_step(slot):
        wait_chunk("band", got_a, slot, send_sem.at[1], sem_a)
        sent_b[slot] = y_chunk(got_a[slot], y_table[...])
        send_chunk("grid", sent_b, got_b, slot, send_sem.at[2], sem_b)

    def x_step(group, pair):
        slot = slot_of(group, pair)
        wait_chunk("grid", got_b, slot, send_sem.at[2], sem_b)
        waves = x_forward_chunk(got_b[slot], x_table[...])
        if group == 2:
            spec[16:20, pair : pair + 2] = waves.reshape(4, 2, 2, 8, 128)
        else:
            spec[8 * group : 8 * group + 8, pair] = waves.reshape(8, 2, 8, 128)

    def x_back_step(group, pair):
        slot = slot_of(group, pair)
        sent_c[slot] = x_back_chunk(mixed[slot], x_table[...])
        send_chunk("grid", sent_c, got_c, slot, send_sem.at[3], sem_c)

    def y_back_step(group, pair):
        slot = slot_of(group, pair)
        wait_chunk("grid", got_c, slot, send_sem.at[3], sem_c)
        sent_d[slot] = y_chunk(got_c[slot], y_table[...])
        send_chunk("band", sent_d, got_d, slot, send_sem.at[4], sem_d)

    def z_back_step(group):
        blocks = []
        for pair in pairs_of(group):
            slot = slot_of(group, pair)
            wait_chunk("band", got_d, slot, send_sem.at[4], sem_d)
            blocks.append(got_d[slot][:, None])
        block = jnp.concatenate(blocks, axis=1)
        return z_back_group(block, index[...], [slopes[i] for i in range(4)], tabs[group][1][...], group)

    def mix_step(pair):
        mix(pair, phi, spec, mixed)

    z_step(2)
    z_send(0)
    z_step(0)
    z_send(1)
    z_step(1)
    for slot in range(2, SLOTS):
        z_send(slot)
    y, x, xb, yb = y_step, x_step, x_back_step, y_back_step
    plan = (
        (y, 0), (y, 1), (y, 2), (y, 3), (x, 2, 0), (y, 4), (x, 0, 0), (y, 5), (x, 1, 0), (mix_step, 0),
        (xb, 0, 0), (y, 6), (xb, 1, 0), (x, 0, 1), (y, 7), (x, 1, 1), (mix_step, 1),
        (xb, 0, 1), (y, 8), (xb, 1, 1), (xb, 2, 0), (x, 2, 2), (y, 9), (yb, 0, 0), (x, 0, 2), (yb, 1, 0), (x, 1, 2),
        (mix_step, 2), (xb, 0, 2), (yb, 0, 1), (xb, 1, 2), (yb, 1, 1), (x, 0, 3), (yb, 2, 0), (x, 1, 3),
        (mix_step, 3), (xb, 0, 3), (xb, 1, 3), (xb, 2, 2),
        (yb, 0, 2), (yb, 1, 2), (yb, 0, 3), (yb, 1, 3), (yb, 2, 2),
    )
    for step, *what in plan:
        step(*what)
    out[:, rows, :] = z_back_step(0) + z_back_step(1) + z_back_step(2)

    given = range(GIVE_PIECES)

    def give(block, i, target):
        piece = out.at[pl.ds(8 // GIVE_PIECES * i, 8 // GIVE_PIECES), rows_of(block), :]
        return remote(piece, piece, send_sem.at[5], out_sem.at[block, i], "band", target)

    for to in (partner, *[along(step) for step in (*GIVE_BESIDE, *GIVE_ACROSS)]):
        for i in given:
            give(band, i, to).start()
    for count, step in enumerate(GIVE_BESIDE):
        origin = along(LINE - step)
        for i in given:
            wait_given(give(origin, i, partner))
            give(origin, i, partner).start()
        if count == 1:
            for i in given:
                wait_given(give(partner, i, partner))
                for across in GIVE_ACROSS:
                    give(partner, i, along(across)).start()
    for step in GIVE_ACROSS:
        for i in given:
            wait_given(give(along(LINE - step), i, partner))
    for step in (*GIVE_BESIDE, *GIVE_ACROSS):
        for i in given:
            wait_given(give(partner_of(along(LINE - step)), i, partner))
    wait_sent("grid", sent_b, send_sem.at[2], sem_b)
    wait_sent("grid", sent_c, send_sem.at[3], sem_c)
    wait_sent("band", sent_a, send_sem.at[1], sem_a)
    wait_sent("band", sent_d, send_sem.at[4], sem_d)
    rest = passed.at[pl.ds(0, len(SUM_BESIDE) + 1)]
    remote(rest, rest, send_sem.at[0], pair_sem.at[0, 0], "band", partner).wait_send()
    rest = passed.at[pl.ds(0, LINE - 1)]
    remote(rest, rest, send_sem.at[6], heard_sem.at[0], "band", partner).wait_send()
    rest = crossed.at[pl.ds(0, len(SUM_ACROSS))]
    remote(rest, rest, send_sem.at[7], cross_sem.at[0], "band", partner).wait_send()
    rest = stage.at[pl.ds(0, PARTS - 1)]
    remote(rest, rest, send_sem.at[5], out_sem.at[0, 0], "band", partner).wait_send()


BLOCKS = (SLOTS, PARTS, 8, 128)


def per_device(partial_density, node_index, node_weight, node_slope, kernel_table):
    constants = jnp.asarray(tables())
    args = [partial_density, node_index, node_weight, node_slope, kernel_table, constants]
    anywhere = pl.BlockSpec(memory_space=pl.ANY)
    vmem = pltpu.VMEM
    return pl.pallas_call(
        body,
        out_shape=pltpu.VMEM((8, N, N), F32),
        in_specs=[anywhere] * len(args),
        out_specs=pl.BlockSpec(memory_space=pltpu.VMEM),
        scratch_shapes=[
            vmem((PARTS, 8, 8, 128), F32),
            *[vmem((LINE, 8, 8, 128), F32)] * 4,
            vmem((8, 8, 128), jnp.int32),
            vmem((4, 8, 8, 128), F32),
            vmem((4, 8, 8, 128), F32),
            vmem(kernel_table.shape, F32),
            vmem(constants.shape, constants.dtype),
            *[vmem(BLOCKS, F32)] * 8,
            vmem((480, 128), F32),
            vmem((480, 256), BF16),
            vmem((TILES, 480, 128), F32),
            vmem((NA, 4, 2, 8, 128), F32),
            vmem((SLOTS, 128, 128), F32),
            pltpu.SemaphoreType.DMA((6,)),
            pltpu.SemaphoreType.DMA((8,)),
            pltpu.SemaphoreType.DMA((LINE, SUM_PIECES)),
            pltpu.SemaphoreType.DMA((LINE,)),
            pltpu.SemaphoreType.DMA((LINE,)),
            *[pltpu.SemaphoreType.DMA((SLOTS,))] * 4,
            pltpu.SemaphoreType.DMA((PARTS, GIVE_PIECES)),
        ],
        compiler_params=pltpu.CompilerParams(
            collective_id=0, has_side_effects=True, vmem_limit_bytes=60000 * 1024
        ),
    )(*args)


def solution(mesh):
    placed = (
        P("band", "grid", None, None),
        P("grid", None, None),
        P(None, "grid", None, None),
        P(None, "grid", None, None),
        P(),
    )
    return jax.shard_map(
        per_device, mesh=mesh, in_specs=placed, out_specs=P("grid", None, None), check_vma=False
    )
```

```python
import functools

import jax
import jax.numpy as jnp
import numpy as np
from jax import lax
from jax.experimental import pallas as pl
from jax.experimental.pallas import tpu as pltpu
from jax.sharding import PartitionSpec as P

N = 128
NA = 20
F32 = jnp.float32
BF16 = jnp.bfloat16


def halves(table):
    table = np.asarray(table, np.float32)
    high = table.astype(BF16)
    low = (table - high.astype(np.float32)).astype(BF16)
    return high, low


def lane_wave(shared):
    lane = np.arange(128)
    bit = [(lane >> b) & 1 for b in range(7)]
    if shared:
        owner = bit[6] * 8 + bit[5] * 4 + bit[2] * 2 + bit[1]
        pair = owner * 4 + bit[0] * 2 + bit[4]
    else:
        owner = bit[6] * 8 + bit[5] * 4 + bit[4] * 2 + bit[2]
        pair = owner * 4 + bit[1] * 2 + bit[0]
    return np.where(bit[3] == 0, pair, np.where(pair == 0, 64, N - pair))


def cas(k, n):
    angle = 2 * np.pi * ((k[:, None] * n[None]) % N) / N
    return np.cos(angle) + np.sin(angle)


def right_form(table):
    high, low = halves(table)
    return np.block([[high, low], [high, np.zeros_like(low)]])


def left_form(table):
    high, low = halves(table)
    return np.block([[high, high], [low, np.zeros_like(low)]])


def tables():
    at = np.arange(N)
    line = cas(at, at)
    z = [cas(at, lane_wave(shared)) for shared in (False, True)]
    waves = [right_form(table) for table in z] + [right_form(table.T / float(N) ** 3) for table in z]
    return np.stack(waves + [left_form(line), right_form(line)])


def split(value):
    high = value.astype(BF16)
    low = (value - high.astype(F32)).astype(BF16)
    return high, low


def mm(a, b):
    return jnp.dot(a, b, preferred_element_type=F32)


def lanes_of(shape):
    return lax.broadcasted_iota(jnp.int32, shape, len(shape) - 1)


def exchange(v, pairs):
    count = v.shape[0]
    for index_bit, lane_bit in pairs:
        inner, step = 1 << index_bit, 1 << lane_bit
        rows = count // 2 * 8
        w = v.reshape(count // (2 * inner), 2, inner, 8, 128)
        a = w[:, 0].reshape(rows, 128)
        b = w[:, 1].reshape(rows, 128)
        keep = (lanes_of((rows, 128)) >> lane_bit) & 1 == 0
        new_a = jnp.where(keep, a, pltpu.roll(b, step, 1))
        new_b = jnp.where(keep, pltpu.roll(a, 128 - step, 1), b)
        shape = (count // (2 * inner), 1, inner, 8, 128)
        v = jnp.concatenate([new_a.reshape(shape), new_b.reshape(shape)], axis=1).reshape(count, 8, 128)
    return v


def exchange_groups(v):
    group = lanes_of((8, 128)) >> 3
    skewed = [v[i] if i == 0 else pltpu.roll(v[i], 8 * i, 1) for i in range(16)]
    for bit in range(4):
        take = (group >> bit) & 1 == 1
        skewed = [jnp.where(take, skewed[(i + (1 << bit)) % 16], skewed[i]) for i in range(16)]
    out = [skewed[-i % 16] if i == 0 else pltpu.roll(skewed[-i % 16], 128 - 8 * i, 1) for i in range(16)]
    return jnp.concatenate([piece[None] for piece in out], axis=0)


GROUP_START = (0, 8, 16)
GROUP_SIZE = (8, 8, 4)
Z_PAIRS = {8: ((5, 6), (4, 5), (3, 4), (2, 2), (1, 1), (0, 0)), 4: ((4, 6), (3, 5), (2, 2), (1, 1), (0, 0))}


def slot_of(group, pair):
    return 5 * (pair // 2) + (0 if group == 2 else 1 + 2 * (pair % 2) + group)


def pairs_of(group):
    return (0, 2) if group == 2 else (0, 1, 2, 3)


def node_coefficient(node, index, weights):
    total = None
    for offset in range(4):
        term = jnp.where(index + (offset - 1) == node, weights[offset], 0.0)
        total = term if total is None else total + term
    return total


def right(rows, table):
    high, low = split(rows)
    wide = mm(jnp.concatenate([high, low], axis=1), table)
    return wide[:, :128] + wide[:, 128:]


def left(table, columns):
    high, low = split(columns)
    tall = mm(table, jnp.concatenate([high, low], axis=0))
    return tall[:128] + tall[128:]


def z_forward_group(density, index, weights, table, group):
    size = GROUP_SIZE[group]
    fields = [density * node_coefficient(GROUP_START[group] + i, index, weights) for i in range(size)]
    theta = jnp.concatenate(fields, axis=0).reshape(64 * size, 128)
    waves = right(theta, table).reshape(8 * size, 8, 128)
    return exchange(waves, Z_PAIRS[size]).reshape(PARTS, size // 2, 8, 128)


def z_back_group(block, index, slopes, table, group):
    size = GROUP_SIZE[group]
    waves = exchange(block.reshape(8 * size, 8, 128), Z_PAIRS[size]).reshape(64 * size, 128)
    field = right(waves, table).reshape(size, 8, 8, 128)
    total = None
    for i in range(size):
        term = field[i] * node_coefficient(GROUP_START[group] + i, index, slopes)
        total = term if total is None else total + term
    return total


def y_chunk(block, table):
    return left(table, block.reshape(128, 128)).reshape(PARTS, 8, 128)


def x_forward_chunk(block, table):
    return right(exchange_groups(block).reshape(128, 128), table)


def x_back_chunk(waves, table):
    return exchange_groups(right(waves, table).reshape(PARTS, 8, 128))


def shell_tile(tile):
    band, grid = lax.axis_index("band"), lax.axis_index("grid")
    second = tile >= 32
    fz = 4 * band + jnp.where(second, 0, tile // 8)
    fz = jnp.where(second & (band == 0), 64, fz)
    ky = 8 * grid + lax.rem(tile, 8)
    fy = jnp.where(ky < 64, ky, ky - 128)
    kx = lanes_of((128, 128))
    fx = jnp.where(kx < 64, kx, kx - 128)
    root = jnp.sqrt((fz * fz + fy * fy + fx * fx).astype(F32))
    shell = lax.broadcasted_iota(jnp.int32, (128, 128), 0).astype(F32)
    return jnp.maximum(1.0 - jnp.abs(root - shell), 0.0)


def start_phi(kernel_table, wide_table, table_pair):
    wide_table[...] = jnp.zeros((480, 128), F32)
    for a in range(NA):
        wide_table[24 * a : 24 * a + NA, : kernel_table.shape[2]] = kernel_table[a]
    high, low = split(wide_table[...])
    table_pair[...] = jnp.concatenate([high, low], axis=1)


def make_phi(first, last, table_pair, phi):
    def step(i, carry):
        wide = table_pair[...]
        tiles = jnp.concatenate([shell_tile(2 * i), shell_tile(2 * i + 1)], axis=1)
        tiles_high, tiles_low = split(tiles)
        values = mm(wide, jnp.concatenate([tiles_high, tiles_high], axis=0)) + mm(wide[:, :128], tiles_low)
        phi[2 * i] = values[:, :128]
        phi[2 * i + 1] = values[:, 128:]
        return carry

    lax.fori_loop(first, last, step, 0)


def mix(pair, phi, spec, mixed):
    def step(row, carry):
        sums = [None, None]
        for a in range(NA):
            kernel = phi[8 * pair + row, 24 * a : 24 * a + 24]
            kernels = kernel, phi[32 + row, 24 * a : 24 * a + 24] if pair == 0 else kernel
            for member in range(2):
                term = kernels[member] * spec[a, pair, member, pl.ds(row, 1), :]
                sums[member] = term if sums[member] is None else sums[member] + term
        for member in range(2):
            at = row + 8 * member
            for group in range(2):
                mixed[slot_of(group, pair), pl.ds(at, 8, stride=16), :] = sums[member][8 * group : 8 * group + 8]
            mixed[slot_of(2, pair), pl.ds(at + 16 * (pair % 2), 4, stride=32), :] = sums[member][16:20]
        return carry

    lax.fori_loop(0, 8, step, 0)


MESH = pl.DeviceIdType.MESH
PARTS = 16
TILES = 40
SLOTS = 10


LINE = 8
SUM_BESIDE, SUM_ACROSS, SUM_PIECES = (4, 3, 5, 1, 7), (2, 6), 2
GIVE_BESIDE, GIVE_ACROSS, GIVE_PIECES = (4, 1, 7, 3, 5), (2, 6), 2


def z_peers(band):
    first = band // LINE * LINE
    return lambda step: first + lax.rem(band + step, LINE)


def partner_of(band):
    return lax.rem(band + LINE, PARTS)


def peers(me):
    return lambda step: lax.rem(me + step, PARTS)


def far_first(axis):
    me = lax.axis_index(axis)
    if axis == "band":
        column, z = me // LINE, lax.rem(me, LINE)
        order = sorted(
            ((dz, dx) for dz in range(LINE) for dx in range(2) if dz or dx), key=lambda d: -(min(d[0], LINE - d[0]) + 2 * d[1])
        )
        return [lax.rem(column + dx, 2) * LINE + lax.rem(z + dz, LINE) for dz, dx in order]
    y, x, core = me // 4, lax.rem(me // 2, 2), lax.rem(me, 2)
    order = sorted(
        ((dy, dx, dc) for dy in range(4) for dx in range(2) for dc in range(2) if dy or dx or dc),
        key=lambda d: -(min(d[0], 4 - d[0]) + d[1]),
    )
    return [lax.rem(y + dy, 4) * 4 + lax.rem(x + dx, 2) * 2 + lax.rem(core + dc, 2) for dy, dx, dc in order]


def greet(barrier):
    band = lax.axis_index("band")
    peer = peers(lax.axis_index("grid"))
    along = z_peers(band)

    def grid_one(step, carry):
        pl.semaphore_signal(barrier, inc=1, device_id={"grid": peer(step)}, device_id_type=MESH)
        return carry

    def band_one(step, carry):
        pl.semaphore_signal(barrier, inc=1, device_id={"band": along(step)}, device_id_type=MESH)
        return carry

    lax.fori_loop(1, LINE, band_one, 0)
    pl.semaphore_signal(barrier, inc=1, device_id={"band": partner_of(band)}, device_id_type=MESH)
    lax.fori_loop(1, PARTS, grid_one, 0)


def remote(src, dst, send_sem, recv_sem, axis, target):
    return pltpu.make_async_remote_copy(
        src_ref=src, dst_ref=dst, send_sem=send_sem, recv_sem=recv_sem, device_id={axis: target}, device_id_type=MESH
    )


def wait_given(copy):
    copy.wait_recv()


def send_chunk(axis, sent, got, slot, send_sem, recv_sem):
    me = lax.axis_index(axis)
    got[slot, me] = sent[slot, me]
    for to in far_first(axis):
        remote(sent.at[slot, to], got.at[slot, me], send_sem, recv_sem.at[slot], axis, to).start()


def wait_chunk(axis, got, slot, send_sem, recv_sem):
    rest = got.at[slot, pl.ds(0, PARTS - 1)]
    remote(rest, rest, send_sem, recv_sem.at[slot], axis, 0).wait_recv()


def wait_sent(axis, sent, send_sem, recv_sem):
    rest = sent.at[:, pl.ds(0, PARTS - 1)]
    remote(rest, rest, send_sem, recv_sem.at[0], axis, 0).wait_send()


def body(
    partial, node_index, node_weight, node_slope, kernel_hbm, tables_hbm, out,
    stage, paired, passed, heard, crossed, index, weights, slopes, kernel_table, table,
    sent_a, got_a, sent_b, got_b, sent_c, got_c, sent_d, got_d,
    wide_table, table_pair, phi, spec, mixed,
    load_sem, send_sem, pair_sem, heard_sem, cross_sem, sem_a, sem_b, sem_c, sem_d, out_sem,
):
    band = lax.axis_index("band")
    barrier = pltpu.get_barrier_semaphore()
    greet(barrier)
    partner, along = partner_of(band), z_peers(band)

    def rows_of(block):
        return pl.ds(pl.multiple_of(8 * block, 8), 8)

    rows = rows_of(band)

    def cut(step, carry):
        pltpu.make_async_copy(partial.at[0, :, rows_of(step), :], stage.at[step], load_sem.at[0]).start()
        return carry

    lax.fori_loop(0, PARTS, cut, 0)
    loads = [
        pltpu.make_async_copy(src, dst, load_sem.at[i + 1])
        for i, (src, dst) in enumerate(
            (
                (kernel_hbm, kernel_table),
                (node_index.at[:, rows, :], index),
                (node_weight.at[:, :, rows, :], weights),
                (node_slope.at[:, :, rows, :], slopes),
                (tables_hbm, table),
            )
        )
    ]
    for load in loads:
        load.start()
    pltpu.make_async_copy(stage, stage, load_sem.at[0]).wait()
    pl.semaphore_wait(barrier, LINE - 1 + 1 + PARTS - 1)

    slot_of_band = lax.rem(band, LINE)

    def piece_of(ref, i):
        return ref.at[pl.ds(8 // SUM_PIECES * i, 8 // SUM_PIECES)]

    pieces = range(SUM_PIECES)

    def to_partner(src, slot, i):
        return remote(
            piece_of(src, i), piece_of(paired.at[slot], i), send_sem.at[0], pair_sem.at[slot, i], "band", partner
        )

    def onward(src, to):
        return remote(src, heard.at[slot_of_band], send_sem.at[6], heard_sem.at[slot_of_band], "band", to)

    for step in SUM_ACROSS:
        to = along(step)
        cross = crossed.at[slot_of_band]
        remote(stage.at[partner_of(to)], cross, send_sem.at[7], cross_sem.at[slot_of_band], "band", to).start()
    for step in SUM_ACROSS:
        onward(stage.at[along(step)], along(step)).start()
    for step in SUM_BESIDE:
        at = along(step)
        for i in pieces:
            to_partner(stage.at[partner_of(at)], lax.rem(at, LINE), i).start()
    loads[0].wait()
    start_phi(kernel_table, wide_table, table_pair)
    make_phi(0, 7, table_pair, phi)
    for count, step in enumerate(SUM_BESIDE):
        to = along(step)
        slot = lax.rem(to, LINE)
        for i in pieces:
            wait_given(to_partner(stage.at[to], slot, i))
            part = pl.ds(8 // SUM_PIECES * i, 8 // SUM_PIECES)
            passed[slot, part] = paired[slot, part] + stage[to, part]
            remote(
                piece_of(passed.at[slot], i),
                piece_of(heard.at[slot_of_band], i),
                send_sem.at[6],
                heard_sem.at[slot_of_band],
                "band",
                to,
            ).start()
        make_phi(7 + count, 8 + count, table_pair, phi)
    own = stage[partner]
    for step in SUM_ACROSS:
        slot = lax.rem(band + LINE - step, LINE)
        cross = crossed.at[slot]
        wait_given(remote(cross, cross, send_sem.at[7], cross_sem.at[slot], "band", partner))
        own = own + crossed[slot]
    passed[slot_of_band] = own
    for i in pieces:
        to_partner(passed.at[slot_of_band], slot_of_band, i).start()
    make_phi(7 + len(SUM_BESIDE), TILES // 2, table_pair, phi)
    for load in loads[1:]:
        load.wait()
    density = stage[band]
    for step in (*SUM_ACROSS, *SUM_BESIDE):
        slot = lax.rem(band + LINE - step, LINE)
        wait_given(remote(heard.at[slot], heard.at[slot], send_sem.at[6], heard_sem.at[slot], "band", partner))
        density = density + heard[slot]
    for i in pieces:
        wait_given(to_partner(passed.at[slot_of_band], slot_of_band, i))
    density = density + paired[slot_of_band]
    tabs = [table.at[i] for i in range(6)]
    y_table, x_table = tabs[4:]
    tabs = {0: (tabs[0], tabs[2]), 1: (tabs[0], tabs[2]), 2: (tabs[1], tabs[3])}

    def z_step(group):
        values = [weights[i] for i in range(4)]
        waves = z_forward_group(density, index[...], values, tabs[group][0][...], group)
        for i, pair in enumerate(pairs_of(group)):
            sent_a[slot_of(group, pair)] = waves[:, i]

    def z_send(slot):
        send_chunk("band", sent_a, got_a, slot, send_sem.at[1], sem_a)

    def y_step(slot):
        wait_chunk("band", got_a, slot, send_sem.at[1], sem_a)
        sent_b[slot] = y_chunk(got_a[slot], y_table[...])
        send_chunk("grid", sent_b, got_b, slot, send_sem.at[2], sem_b)

    def x_step(group, pair):
        slot = slot_of(group, pair)
        wait_chunk("grid", got_b, slot, send_sem.at[2], sem_b)
        waves = x_forward_chunk(got_b[slot], x_table[...])
        if group == 2:
            spec[16:20, pair : pair + 2] = waves.reshape(4, 2, 2, 8, 128)
        else:
            spec[8 * group : 8 * group + 8, pair] = waves.reshape(8, 2, 8, 128)

    def x_back_step(group, pair):
        slot = slot_of(group, pair)
        sent_c[slot] = x_back_chunk(mixed[slot], x_table[...])
        send_chunk("grid", sent_c, got_c, slot, send_sem.at[3], sem_c)

    def y_back_step(group, pair):
        slot = slot_of(group, pair)
        wait_chunk("grid", got_c, slot, send_sem.at[3], sem_c)
        sent_d[slot] = y_chunk(got_c[slot], y_table[...])
        send_chunk("band", sent_d, got_d, slot, send_sem.at[4], sem_d)

    def z_back_step(group):
        blocks = []
        for pair in pairs_of(group):
            slot = slot_of(group, pair)
            wait_chunk("band", got_d, slot, send_sem.at[4], sem_d)
            blocks.append(got_d[slot][:, None])
        block = jnp.concatenate(blocks, axis=1)
        return z_back_group(block, index[...], [slopes[i] for i in range(4)], tabs[group][1][...], group)

    def mix_step(pair):
        mix(pair, phi, spec, mixed)

    z_step(2)
    z_send(0)
    z_step(0)
    z_send(1)
    z_step(1)
    for slot in range(2, SLOTS):
        z_send(slot)
    y, x, xb, yb = y_step, x_step, x_back_step, y_back_step
    plan = (
        (y, 0), (y, 1), (y, 2), (y, 3), (x, 2, 0), (y, 4), (x, 0, 0), (y, 5), (x, 1, 0), (mix_step, 0),
        (xb, 0, 0), (y, 6), (xb, 1, 0), (x, 0, 1), (y, 7), (x, 1, 1), (mix_step, 1),
        (xb, 0, 1), (y, 8), (y, 9), (xb, 1, 1), (xb, 2, 0), (x, 2, 2), (yb, 0, 0), (x, 0, 2), (yb, 1, 0), (x, 1, 2),
        (mix_step, 2), (xb, 0, 2), (yb, 0, 1), (xb, 1, 2), (yb, 1, 1), (x, 0, 3), (x, 1, 3),
        (mix_step, 3), (xb, 0, 3), (yb, 2, 0), (xb, 1, 3), (xb, 2, 2),
        (yb, 0, 2), (yb, 1, 2), (yb, 0, 3), (yb, 1, 3), (yb, 2, 2),
    )
    for step, *what in plan:
        step(*what)
    out[:, rows, :] = z_back_step(0) + z_back_step(1) + z_back_step(2)

    given = range(GIVE_PIECES)

    def give(block, i, target):
        piece = out.at[pl.ds(8 // GIVE_PIECES * i, 8 // GIVE_PIECES), rows_of(block), :]
        return remote(piece, piece, send_sem.at[5], out_sem.at[block, i], "band", target)

    for to in (partner, *[along(step) for step in (*GIVE_BESIDE, *GIVE_ACROSS)]):
        for i in given:
            give(band, i, to).start()
    for count, step in enumerate(GIVE_BESIDE):
        origin = along(LINE - step)
        for i in given:
            wait_given(give(origin, i, partner))
            give(origin, i, partner).start()
        if count == 1:
            for i in given:
                wait_given(give(partner, i, partner))
                for across in GIVE_ACROSS:
                    give(partner, i, along(across)).start()
    for step in GIVE_ACROSS:
        for i in given:
            wait_given(give(along(LINE - step), i, partner))
    for step in (*GIVE_BESIDE, *GIVE_ACROSS):
        for i in given:
            wait_given(give(partner_of(along(LINE - step)), i, partner))
    wait_sent("grid", sent_b, send_sem.at[2], sem_b)
    wait_sent("grid", sent_c, send_sem.at[3], sem_c)
    wait_sent("band", sent_a, send_sem.at[1], sem_a)
    wait_sent("band", sent_d, send_sem.at[4], sem_d)
    rest = passed.at[pl.ds(0, len(SUM_BESIDE) + 1)]
    remote(rest, rest, send_sem.at[0], pair_sem.at[0, 0], "band", partner).wait_send()
    rest = passed.at[pl.ds(0, LINE - 1)]
    remote(rest, rest, send_sem.at[6], heard_sem.at[0], "band", partner).wait_send()
    rest = crossed.at[pl.ds(0, len(SUM_ACROSS))]
    remote(rest, rest, send_sem.at[7], cross_sem.at[0], "band", partner).wait_send()
    rest = stage.at[pl.ds(0, PARTS - 1)]
    remote(rest, rest, send_sem.at[5], out_sem.at[0, 0], "band", partner).wait_send()


BLOCKS = (SLOTS, PARTS, 8, 128)


def per_device(partial_density, node_index, node_weight, node_slope, kernel_table):
    constants = jnp.asarray(tables())
    args = [partial_density, node_index, node_weight, node_slope, kernel_table, constants]
    anywhere = pl.BlockSpec(memory_space=pl.ANY)
    vmem = pltpu.VMEM
    return pl.pallas_call(
        body,
        out_shape=pltpu.VMEM((8, N, N), F32),
        in_specs=[anywhere] * len(args),
        out_specs=pl.BlockSpec(memory_space=pltpu.VMEM),
        scratch_shapes=[
            vmem((PARTS, 8, 8, 128), F32),
            *[vmem((LINE, 8, 8, 128), F32)] * 4,
            vmem((8, 8, 128), jnp.int32),
            vmem((4, 8, 8, 128), F32),
            vmem((4, 8, 8, 128), F32),
            vmem(kernel_table.shape, F32),
            vmem(constants.shape, constants.dtype),
            *[vmem(BLOCKS, F32)] * 8,
            vmem((480, 128), F32),
            vmem((480, 256), BF16),
            vmem((TILES, 480, 128), F32),
            vmem((NA, 4, 2, 8, 128), F32),
            vmem((SLOTS, 128, 128), F32),
            pltpu.SemaphoreType.DMA((6,)),
            pltpu.SemaphoreType.DMA((8,)),
            pltpu.SemaphoreType.DMA((LINE, SUM_PIECES)),
            pltpu.SemaphoreType.DMA((LINE,)),
            pltpu.SemaphoreType.DMA((LINE,)),
            *[pltpu.SemaphoreType.DMA((SLOTS,))] * 4,
            pltpu.SemaphoreType.DMA((PARTS, GIVE_PIECES)),
        ],
        compiler_params=pltpu.CompilerParams(
            collective_id=0, has_side_effects=True, vmem_limit_bytes=60000 * 1024
        ),
    )(*args)


def solution(mesh):
    placed = (
        P("band", "grid", None, None),
        P("grid", None, None),
        P(None, "grid", None, None),
        P(None, "grid", None, None),
        P(),
    )
    return jax.shard_map(
        per_device, mesh=mesh, in_specs=placed, out_specs=P("grid", None, None), check_vma=False
    )
```

```python
import functools

import jax
import jax.numpy as jnp
import numpy as np
from jax import lax
from jax.experimental import pallas as pl
from jax.experimental.pallas import tpu as pltpu
from jax.sharding import PartitionSpec as P

N = 128
NA = 20
F32 = jnp.float32
BF16 = jnp.bfloat16


def halves(table):
    table = np.asarray(table, np.float32)
    high = table.astype(BF16)
    low = (table - high.astype(np.float32)).astype(BF16)
    return high, low


def lane_wave(shared):
    lane = np.arange(128)
    bit = [(lane >> b) & 1 for b in range(7)]
    if shared:
        owner = bit[6] * 8 + bit[5] * 4 + bit[2] * 2 + bit[1]
        pair = owner * 4 + bit[0] * 2 + bit[4]
    else:
        owner = bit[6] * 8 + bit[5] * 4 + bit[4] * 2 + bit[2]
        pair = owner * 4 + bit[1] * 2 + bit[0]
    return np.where(bit[3] == 0, pair, np.where(pair == 0, 64, N - pair))


def cas(k, n):
    angle = 2 * np.pi * ((k[:, None] * n[None]) % N) / N
    return np.cos(angle) + np.sin(angle)


def right_form(table):
    high, low = halves(table)
    return np.block([[high, low], [high, np.zeros_like(low)]])


def left_form(table):
    high, low = halves(table)
    return np.block([[high, high], [low, np.zeros_like(low)]])


def tables():
    at = np.arange(N)
    line = cas(at, at)
    z = [cas(at, lane_wave(shared)) for shared in (False, True)]
    waves = [right_form(table) for table in z] + [right_form(table.T / float(N) ** 3) for table in z]
    return np.stack(waves + [left_form(line), right_form(line)])


def split(value):
    high = value.astype(BF16)
    low = (value - high.astype(F32)).astype(BF16)
    return high, low


def mm(a, b):
    return jnp.dot(a, b, preferred_element_type=F32)


def lanes_of(shape):
    return lax.broadcasted_iota(jnp.int32, shape, len(shape) - 1)


def exchange(v, pairs):
    count = v.shape[0]
    for index_bit, lane_bit in pairs:
        inner, step = 1 << index_bit, 1 << lane_bit
        rows = count // 2 * 8
        w = v.reshape(count // (2 * inner), 2, inner, 8, 128)
        a = w[:, 0].reshape(rows, 128)
        b = w[:, 1].reshape(rows, 128)
        keep = (lanes_of((rows, 128)) >> lane_bit) & 1 == 0
        new_a = jnp.where(keep, a, pltpu.roll(b, step, 1))
        new_b = jnp.where(keep, pltpu.roll(a, 128 - step, 1), b)
        shape = (count // (2 * inner), 1, inner, 8, 128)
        v = jnp.concatenate([new_a.reshape(shape), new_b.reshape(shape)], axis=1).reshape(count, 8, 128)
    return v


def exchange_groups(v):
    group = lanes_of((8, 128)) >> 3
    skewed = [v[i] if i == 0 else pltpu.roll(v[i], 8 * i, 1) for i in range(16)]
    for bit in range(4):
        take = (group >> bit) & 1 == 1
        skewed = [jnp.where(take, skewed[(i + (1 << bit)) % 16], skewed[i]) for i in range(16)]
    out = [skewed[-i % 16] if i == 0 else pltpu.roll(skewed[-i % 16], 128 - 8 * i, 1) for i in range(16)]
    return jnp.concatenate([piece[None] for piece in out], axis=0)


GROUP_START = (0, 8, 16)
GROUP_SIZE = (8, 8, 4)
Z_PAIRS = {8: ((5, 6), (4, 5), (3, 4), (2, 2), (1, 1), (0, 0)), 4: ((4, 6), (3, 5), (2, 2), (1, 1), (0, 0))}


def slot_of(group, pair):
    return 5 * (pair // 2) + (0 if group == 2 else 1 + 2 * (pair % 2) + group)


def pairs_of(group):
    return (0, 2) if group == 2 else (0, 1, 2, 3)


def node_coefficient(node, index, weights):
    total = None
    for offset in range(4):
        term = jnp.where(index + (offset - 1) == node, weights[offset], 0.0)
        total = term if total is None else total + term
    return total


def right(rows, table):
    high, low = split(rows)
    wide = mm(jnp.concatenate([high, low], axis=1), table)
    return wide[:, :128] + wide[:, 128:]


def left(table, columns):
    high, low = split(columns)
    tall = mm(table, jnp.concatenate([high, low], axis=0))
    return tall[:128] + tall[128:]


def z_forward_group(density, index, weights, table, group):
    size = GROUP_SIZE[group]
    fields = [density * node_coefficient(GROUP_START[group] + i, index, weights) for i in range(size)]
    theta = jnp.concatenate(fields, axis=0).reshape(64 * size, 128)
    waves = right(theta, table).reshape(8 * size, 8, 128)
    return exchange(waves, Z_PAIRS[size]).reshape(PARTS, size // 2, 8, 128)


def z_back_group(block, index, slopes, table, group):
    size = GROUP_SIZE[group]
    waves = exchange(block.reshape(8 * size, 8, 128), Z_PAIRS[size]).reshape(64 * size, 128)
    field = right(waves, table).reshape(size, 8, 8, 128)
    total = None
    for i in range(size):
        term = field[i] * node_coefficient(GROUP_START[group] + i, index, slopes)
        total = term if total is None else total + term
    return total


def y_chunk(block, table):
    return left(table, block.reshape(128, 128)).reshape(PARTS, 8, 128)


def x_forward_chunk(block, table):
    return right(exchange_groups(block).reshape(128, 128), table)


def x_back_chunk(waves, table):
    return exchange_groups(right(waves, table).reshape(PARTS, 8, 128))


def shell_tile(tile):
    band, grid = lax.axis_index("band"), lax.axis_index("grid")
    second = tile >= 32
    fz = 4 * band + jnp.where(second, 0, tile // 8)
    fz = jnp.where(second & (band == 0), 64, fz)
    ky = 8 * grid + lax.rem(tile, 8)
    fy = jnp.where(ky < 64, ky, ky - 128)
    kx = lanes_of((128, 128))
    fx = jnp.where(kx < 64, kx, kx - 128)
    root = jnp.sqrt((fz * fz + fy * fy + fx * fx).astype(F32))
    shell = lax.broadcasted_iota(jnp.int32, (128, 128), 0).astype(F32)
    return jnp.maximum(1.0 - jnp.abs(root - shell), 0.0)


def start_phi(kernel_table, wide_table, table_pair):
    wide_table[...] = jnp.zeros((480, 128), F32)
    for a in range(NA):
        wide_table[24 * a : 24 * a + NA, : kernel_table.shape[2]] = kernel_table[a]
    high, low = split(wide_table[...])
    table_pair[...] = jnp.concatenate([high, low], axis=1)


def make_phi(first, last, table_pair, phi):
    def step(i, carry):
        wide = table_pair[...]
        tiles = jnp.concatenate([shell_tile(2 * i), shell_tile(2 * i + 1)], axis=1)
        tiles_high, tiles_low = split(tiles)
        values = mm(wide, jnp.concatenate([tiles_high, tiles_high], axis=0)) + mm(wide[:, :128], tiles_low)
        phi[2 * i] = values[:, :128]
        phi[2 * i + 1] = values[:, 128:]
        return carry

    lax.fori_loop(first, last, step, 0)


def mix(group, pair, phi, spec, mixed):
    def step(row, carry):
        sums = [None, None]
        for a in range(NA):
            part = slice(24 * a + 8 * group, 24 * a + 8 * group + 8)
            kernel = phi[8 * pair + row, part]
            kernels = kernel, phi[32 + row, part] if pair == 0 else kernel
            for member in range(2):
                term = kernels[member] * spec[a, pair, member, pl.ds(row, 1), :]
                sums[member] = term if sums[member] is None else sums[member] + term
        for member in range(2):
            at = row + 8 * member
            if group == 2:
                mixed[slot_of(2, pair), pl.ds(at + 16 * (pair % 2), 4, stride=32), :] = sums[member][:4]
            else:
                mixed[slot_of(group, pair), pl.ds(at, 8, stride=16), :] = sums[member]
        return carry

    lax.fori_loop(0, 8, step, 0, unroll=2)


MESH = pl.DeviceIdType.MESH
PARTS = 16
TILES = 40
SLOTS = 10


LINE = 8
SUM_BESIDE, SUM_ACROSS, SUM_PIECES = (4, 3, 5, 1, 7), (2, 6), 2
GIVE_BESIDE, GIVE_ACROSS, GIVE_PIECES = (4, 3, 5, 1, 7), (2, 6), 2


def z_peers(band):
    first = band // LINE * LINE
    return lambda step: first + lax.rem(band + step, LINE)


def partner_of(band):
    return lax.rem(band + LINE, PARTS)


def peers(me):
    return lambda step: lax.rem(me + step, PARTS)


def far_first(axis):
    me = lax.axis_index(axis)
    if axis == "band":
        column, z = me // LINE, lax.rem(me, LINE)
        order = sorted(
            ((dz, dx) for dz in range(LINE) for dx in range(2) if dz or dx), key=lambda d: -(min(d[0], LINE - d[0]) + 2 * d[1])
        )
        return [lax.rem(column + dx, 2) * LINE + lax.rem(z + dz, LINE) for dz, dx in order]
    y, x, core = me // 4, lax.rem(me // 2, 2), lax.rem(me, 2)
    order = sorted(
        ((dy, dx, dc) for dy in range(4) for dx in range(2) for dc in range(2) if dy or dx or dc),
        key=lambda d: -(min(d[0], 4 - d[0]) + d[1]),
    )
    return [lax.rem(y + dy, 4) * 4 + lax.rem(x + dx, 2) * 2 + lax.rem(core + dc, 2) for dy, dx, dc in order]


def greet(barrier):
    band = lax.axis_index("band")
    peer = peers(lax.axis_index("grid"))
    along = z_peers(band)

    def grid_one(step, carry):
        pl.semaphore_signal(barrier, inc=1, device_id={"grid": peer(step)}, device_id_type=MESH)
        return carry

    def band_one(step, carry):
        pl.semaphore_signal(barrier, inc=1, device_id={"band": along(step)}, device_id_type=MESH)
        return carry

    lax.fori_loop(1, LINE, band_one, 0)
    pl.semaphore_signal(barrier, inc=1, device_id={"band": partner_of(band)}, device_id_type=MESH)
    lax.fori_loop(1, PARTS, grid_one, 0)


def remote(src, dst, send_sem, recv_sem, axis, target):
    return pltpu.make_async_remote_copy(
        src_ref=src, dst_ref=dst, send_sem=send_sem, recv_sem=recv_sem, device_id={axis: target}, device_id_type=MESH
    )


def wait_given(copy):
    copy.wait_recv()


def send_chunk(axis, sent, got, slot, send_sem, recv_sem):
    me = lax.axis_index(axis)
    got[slot, me] = sent[slot, me]
    for to in far_first(axis):
        remote(sent.at[slot, to], got.at[slot, me], send_sem, recv_sem.at[slot], axis, to).start()


def wait_chunk(axis, got, slot, send_sem, recv_sem):
    rest = got.at[slot, pl.ds(0, PARTS - 1)]
    remote(rest, rest, send_sem, recv_sem.at[slot], axis, 0).wait_recv()


def wait_sent(axis, sent, send_sem, recv_sem):
    rest = sent.at[:, pl.ds(0, PARTS - 1)]
    remote(rest, rest, send_sem, recv_sem.at[0], axis, 0).wait_send()


def body(
    partial, node_index, node_weight, node_slope, kernel_hbm, tables_hbm, out,
    stage, paired, passed, heard, crossed, index, weights, slopes, kernel_table, table,
    sent_a, got_a, sent_b, got_b, sent_c, got_c, sent_d, got_d,
    wide_table, table_pair, phi, spec, mixed,
    load_sem, send_sem, pair_sem, heard_sem, cross_sem, sem_a, sem_b, sem_c, sem_d, out_sem,
):
    band = lax.axis_index("band")
    barrier = pltpu.get_barrier_semaphore()
    greet(barrier)
    partner, along = partner_of(band), z_peers(band)

    def rows_of(block):
        return pl.ds(pl.multiple_of(8 * block, 8), 8)

    rows = rows_of(band)

    def cut(step, carry):
        pltpu.make_async_copy(partial.at[0, :, rows_of(step), :], stage.at[step], load_sem.at[0]).start()
        return carry

    lax.fori_loop(0, PARTS, cut, 0)
    loads = [
        pltpu.make_async_copy(src, dst, load_sem.at[i + 1])
        for i, (src, dst) in enumerate(
            (
                (kernel_hbm, kernel_table),
                (node_index.at[:, rows, :], index),
                (node_weight.at[:, :, rows, :], weights),
                (node_slope.at[:, :, rows, :], slopes),
                (tables_hbm, table),
            )
        )
    ]
    for load in loads:
        load.start()
    pltpu.make_async_copy(stage, stage, load_sem.at[0]).wait()
    pl.semaphore_wait(barrier, LINE - 1 + 1 + PARTS - 1)

    slot_of_band = lax.rem(band, LINE)

    def piece_of(ref, i):
        return ref.at[pl.ds(8 // SUM_PIECES * i, 8 // SUM_PIECES)]

    pieces = range(SUM_PIECES)

    def to_partner(src, slot, i):
        return remote(
            piece_of(src, i), piece_of(paired.at[slot], i), send_sem.at[0], pair_sem.at[slot, i], "band", partner
        )

    def onward(src, to):
        return remote(src, heard.at[slot_of_band], send_sem.at[6], heard_sem.at[slot_of_band], "band", to)

    for step in SUM_ACROSS:
        to = along(step)
        cross = crossed.at[slot_of_band]
        remote(stage.at[partner_of(to)], cross, send_sem.at[7], cross_sem.at[slot_of_band], "band", to).start()
    for step in SUM_ACROSS:
        onward(stage.at[along(step)], along(step)).start()
    for step in SUM_BESIDE:
        at = along(step)
        for i in pieces:
            to_partner(stage.at[partner_of(at)], lax.rem(at, LINE), i).start()
    loads[0].wait()
    start_phi(kernel_table, wide_table, table_pair)
    make_phi(0, 7, table_pair, phi)
    for count, step in enumerate(SUM_BESIDE):
        to = along(step)
        slot = lax.rem(to, LINE)
        for i in pieces:
            wait_given(to_partner(stage.at[to], slot, i))
            part = pl.ds(8 // SUM_PIECES * i, 8 // SUM_PIECES)
            passed[slot, part] = paired[slot, part] + stage[to, part]
            remote(
                piece_of(passed.at[slot], i),
                piece_of(heard.at[slot_of_band], i),
                send_sem.at[6],
                heard_sem.at[slot_of_band],
                "band",
                to,
            ).start()
        make_phi(7 + count, 8 + count, table_pair, phi)
    own = stage[partner]
    for step in SUM_ACROSS:
        slot = lax.rem(band + LINE - step, LINE)
        cross = crossed.at[slot]
        wait_given(remote(cross, cross, send_sem.at[7], cross_sem.at[slot], "band", partner))
        own = own + crossed[slot]
    passed[slot_of_band] = own
    for i in pieces:
        to_partner(passed.at[slot_of_band], slot_of_band, i).start()
    make_phi(7 + len(SUM_BESIDE), TILES // 2, table_pair, phi)
    for load in loads[1:]:
        load.wait()
    density = stage[band]
    for step in (*SUM_ACROSS, *SUM_BESIDE):
        slot = lax.rem(band + LINE - step, LINE)
        wait_given(remote(heard.at[slot], heard.at[slot], send_sem.at[6], heard_sem.at[slot], "band", partner))
        density = density + heard[slot]
    for i in pieces:
        wait_given(to_partner(passed.at[slot_of_band], slot_of_band, i))
    density = density + paired[slot_of_band]
    tabs = [table.at[i] for i in range(6)]
    y_table, x_table = tabs[4:]
    tabs = {0: (tabs[0], tabs[2]), 1: (tabs[0], tabs[2]), 2: (tabs[1], tabs[3])}

    def z_step(group):
        values = [weights[i] for i in range(4)]
        waves = z_forward_group(density, index[...], values, tabs[group][0][...], group)
        for i, pair in enumerate(pairs_of(group)):
            sent_a[slot_of(group, pair)] = waves[:, i]

    def z_send(slot):
        send_chunk("band", sent_a, got_a, slot, send_sem.at[1], sem_a)

    def y_step(slot):
        wait_chunk("band", got_a, slot, send_sem.at[1], sem_a)
        sent_b[slot] = y_chunk(got_a[slot], y_table[...])
        send_chunk("grid", sent_b, got_b, slot, send_sem.at[2], sem_b)

    def x_step(group, pair):
        slot = slot_of(group, pair)
        wait_chunk("grid", got_b, slot, send_sem.at[2], sem_b)
        waves = x_forward_chunk(got_b[slot], x_table[...])
        if group == 2:
            spec[16:20, pair : pair + 2] = waves.reshape(4, 2, 2, 8, 128)
        else:
            spec[8 * group : 8 * group + 8, pair] = waves.reshape(8, 2, 8, 128)

    def x_back_step(group, pair):
        slot = slot_of(group, pair)
        sent_c[slot] = x_back_chunk(mixed[slot], x_table[...])
        send_chunk("grid", sent_c, got_c, slot, send_sem.at[3], sem_c)

    def y_back_step(group, pair):
        slot = slot_of(group, pair)
        wait_chunk("grid", got_c, slot, send_sem.at[3], sem_c)
        sent_d[slot] = y_chunk(got_c[slot], y_table[...])
        send_chunk("band", sent_d, got_d, slot, send_sem.at[4], sem_d)

    def z_back_step(group):
        blocks = []
        for pair in pairs_of(group):
            slot = slot_of(group, pair)
            wait_chunk("band", got_d, slot, send_sem.at[4], sem_d)
            blocks.append(got_d[slot][:, None])
        block = jnp.concatenate(blocks, axis=1)
        return z_back_group(block, index[...], [slopes[i] for i in range(4)], tabs[group][1][...], group)

    def mix_step(group, pair):
        mix(group, pair, phi, spec, mixed)

    z_step(2)
    z_send(0)
    z_step(0)
    z_send(1)
    z_step(1)
    for slot in range(2, SLOTS):
        z_send(slot)
    y, x, xb, yb = y_step, x_step, x_back_step, y_back_step
    m = mix_step
    plan = (
        (y, 0), (y, 1), (y, 2), (y, 3), (x, 2, 0), (y, 4), (x, 0, 0), (y, 5), (x, 1, 0),
        (m, 0, 0), (xb, 0, 0), (m, 1, 0), (xb, 1, 0), (y, 6), (m, 2, 0), (x, 0, 1), (y, 7), (x, 1, 1),
        (m, 0, 1), (xb, 0, 1), (y, 8), (y, 9), (m, 1, 1), (xb, 1, 1), (m, 2, 1), (xb, 2, 0),
        (x, 2, 2), (yb, 0, 0), (x, 0, 2), (yb, 1, 0), (x, 1, 2),
        (m, 0, 2), (xb, 0, 2), (yb, 0, 1), (m, 1, 2), (xb, 1, 2), (m, 2, 2), (x, 0, 3), (x, 1, 3), (yb, 1, 1),
        (m, 0, 3), (xb, 0, 3), (yb, 2, 0), (m, 1, 3), (xb, 1, 3), (m, 2, 3), (xb, 2, 2),
        (yb, 0, 2), (yb, 1, 2), (yb, 0, 3), (yb, 1, 3), (yb, 2, 2),
    )
    for step, *what in plan:
        step(*what)
    out[:, rows, :] = z_back_step(0) + z_back_step(1) + z_back_step(2)

    given = range(GIVE_PIECES)

    def give(block, i, target):
        piece = out.at[pl.ds(8 // GIVE_PIECES * i, 8 // GIVE_PIECES), rows_of(block), :]
        return remote(piece, piece, send_sem.at[5], out_sem.at[block, i], "band", target)

    for to in (partner, *[along(step) for step in (*GIVE_BESIDE, *GIVE_ACROSS)]):
        for i in given:
            give(band, i, to).start()
    for count, step in enumerate(GIVE_BESIDE):
        origin = along(LINE - step)
        for i in given:
            wait_given(give(origin, i, partner))
            give(origin, i, partner).start()
        if count == 1:
            for i in given:
                wait_given(give(partner, i, partner))
                for across in GIVE_ACROSS:
                    give(partner, i, along(across)).start()
    for step in GIVE_ACROSS:
        for i in given:
            wait_given(give(along(LINE - step), i, partner))
    for step in (*GIVE_BESIDE, *GIVE_ACROSS):
        for i in given:
            wait_given(give(partner_of(along(LINE - step)), i, partner))
    wait_sent("grid", sent_b, send_sem.at[2], sem_b)
    wait_sent("grid", sent_c, send_sem.at[3], sem_c)
    wait_sent("band", sent_a, send_sem.at[1], sem_a)
    wait_sent("band", sent_d, send_sem.at[4], sem_d)
    rest = passed.at[pl.ds(0, len(SUM_BESIDE) + 1)]
    remote(rest, rest, send_sem.at[0], pair_sem.at[0, 0], "band", partner).wait_send()
    rest = passed.at[pl.ds(0, LINE - 1)]
    remote(rest, rest, send_sem.at[6], heard_sem.at[0], "band", partner).wait_send()
    rest = crossed.at[pl.ds(0, len(SUM_ACROSS))]
    remote(rest, rest, send_sem.at[7], cross_sem.at[0], "band", partner).wait_send()
    rest = stage.at[pl.ds(0, PARTS - 1)]
    remote(rest, rest, send_sem.at[5], out_sem.at[0, 0], "band", partner).wait_send()


BLOCKS = (SLOTS, PARTS, 8, 128)


def per_device(partial_density, node_index, node_weight, node_slope, kernel_table):
    constants = jnp.asarray(tables())
    args = [partial_density, node_index, node_weight, node_slope, kernel_table, constants]
    anywhere = pl.BlockSpec(memory_space=pl.ANY)
    vmem = pltpu.VMEM
    return pl.pallas_call(
        body,
        out_shape=pltpu.VMEM((8, N, N), F32),
        in_specs=[anywhere] * len(args),
        out_specs=pl.BlockSpec(memory_space=pltpu.VMEM),
        scratch_shapes=[
            vmem((PARTS, 8, 8, 128), F32),
            *[vmem((LINE, 8, 8, 128), F32)] * 4,
            vmem((8, 8, 128), jnp.int32),
            vmem((4, 8, 8, 128), F32),
            vmem((4, 8, 8, 128), F32),
            vmem(kernel_table.shape, F32),
            vmem(constants.shape, constants.dtype),
            *[vmem(BLOCKS, F32)] * 8,
            vmem((480, 128), F32),
            vmem((480, 256), BF16),
            vmem((TILES, 480, 128), F32),
            vmem((NA, 4, 2, 8, 128), F32),
            vmem((SLOTS, 128, 128), F32),
            pltpu.SemaphoreType.DMA((6,)),
            pltpu.SemaphoreType.DMA((8,)),
            pltpu.SemaphoreType.DMA((LINE, SUM_PIECES)),
            pltpu.SemaphoreType.DMA((LINE,)),
            pltpu.SemaphoreType.DMA((LINE,)),
            *[pltpu.SemaphoreType.DMA((SLOTS,))] * 4,
            pltpu.SemaphoreType.DMA((PARTS, GIVE_PIECES)),
        ],
        compiler_params=pltpu.CompilerParams(
            collective_id=0, has_side_effects=True, vmem_limit_bytes=60000 * 1024
        ),
    )(*args)


def solution(mesh):
    placed = (
        P("band", "grid", None, None),
        P("grid", None, None),
        P(None, "grid", None, None),
        P(None, "grid", None, None),
        P(),
    )
    return jax.shard_map(
        per_device, mesh=mesh, in_specs=placed, out_specs=P("grid", None, None), check_vma=False
    )
```

```python
import functools

import jax
import jax.numpy as jnp
import numpy as np
from jax import lax
from jax.experimental import pallas as pl
from jax.experimental.pallas import tpu as pltpu
from jax.sharding import PartitionSpec as P

N = 128
NA = 20
F32 = jnp.float32
BF16 = jnp.bfloat16


def halves(table):
    table = np.asarray(table, np.float32)
    high = table.astype(BF16)
    low = (table - high.astype(np.float32)).astype(BF16)
    return high, low


def lane_wave(shared):
    lane = np.arange(128)
    bit = [(lane >> b) & 1 for b in range(7)]
    if shared:
        owner = bit[6] * 8 + bit[5] * 4 + bit[2] * 2 + bit[1]
        pair = owner * 4 + bit[0] * 2 + bit[4]
    else:
        owner = bit[6] * 8 + bit[5] * 4 + bit[4] * 2 + bit[2]
        pair = owner * 4 + bit[1] * 2 + bit[0]
    return np.where(bit[3] == 0, pair, np.where(pair == 0, 64, N - pair))


def cas(k, n):
    angle = 2 * np.pi * ((k[:, None] * n[None]) % N) / N
    return np.cos(angle) + np.sin(angle)


def right_form(table):
    high, low = halves(table)
    return np.block([[high, low], [high, np.zeros_like(low)]])


def left_form(table):
    high, low = halves(table)
    return np.block([[high, high], [low, np.zeros_like(low)]])


def tables():
    at = np.arange(N)
    line = cas(at, at)
    z = [cas(at, lane_wave(shared)) for shared in (False, True)]
    waves = [right_form(table) for table in z] + [right_form(table.T / float(N) ** 3) for table in z]
    return np.stack(waves + [left_form(line), right_form(line)])


def split(value):
    high = value.astype(BF16)
    low = (value - high.astype(F32)).astype(BF16)
    return high, low


def mm(a, b):
    return jnp.dot(a, b, preferred_element_type=F32)


def lanes_of(shape):
    return lax.broadcasted_iota(jnp.int32, shape, len(shape) - 1)


def exchange(v, pairs):
    count = v.shape[0]
    for index_bit, lane_bit in pairs:
        inner, step = 1 << index_bit, 1 << lane_bit
        rows = count // 2 * 8
        w = v.reshape(count // (2 * inner), 2, inner, 8, 128)
        a = w[:, 0].reshape(rows, 128)
        b = w[:, 1].reshape(rows, 128)
        keep = (lanes_of((rows, 128)) >> lane_bit) & 1 == 0
        new_a = jnp.where(keep, a, pltpu.roll(b, step, 1))
        new_b = jnp.where(keep, pltpu.roll(a, 128 - step, 1), b)
        shape = (count // (2 * inner), 1, inner, 8, 128)
        v = jnp.concatenate([new_a.reshape(shape), new_b.reshape(shape)], axis=1).reshape(count, 8, 128)
    return v


def exchange_groups(v):
    group = lanes_of((8, 128)) >> 3
    skewed = [v[i] if i == 0 else pltpu.roll(v[i], 8 * i, 1) for i in range(16)]
    for bit in range(4):
        take = (group >> bit) & 1 == 1
        skewed = [jnp.where(take, skewed[(i + (1 << bit)) % 16], skewed[i]) for i in range(16)]
    out = [skewed[-i % 16] if i == 0 else pltpu.roll(skewed[-i % 16], 128 - 8 * i, 1) for i in range(16)]
    return jnp.concatenate([piece[None] for piece in out], axis=0)


GROUP_START = (0, 8, 16)
GROUP_SIZE = (8, 8, 4)
Z_PAIRS = {8: ((5, 6), (4, 5), (3, 4), (2, 2), (1, 1), (0, 0)), 4: ((4, 6), (3, 5), (2, 2), (1, 1), (0, 0))}


def slot_of(group, pair):
    return 5 * (pair // 2) + (0 if group == 2 else 1 + 2 * (pair % 2) + group)


def pairs_of(group):
    return (0, 2) if group == 2 else (0, 1, 2, 3)


def node_coefficient(node, index, weights):
    total = None
    for offset in range(4):
        term = jnp.where(index + (offset - 1) == node, weights[offset], 0.0)
        total = term if total is None else total + term
    return total


def right(rows, table):
    high, low = split(rows)
    wide = mm(jnp.concatenate([high, low], axis=1), table)
    return wide[:, :128] + wide[:, 128:]


def left(table, columns):
    high, low = split(columns)
    tall = mm(table, jnp.concatenate([high, low], axis=0))
    return tall[:128] + tall[128:]


def z_forward_group(density, index, weights, table, group):
    size = GROUP_SIZE[group]
    fields = [density * node_coefficient(GROUP_START[group] + i, index, weights) for i in range(size)]
    theta = jnp.concatenate(fields, axis=0).reshape(64 * size, 128)
    waves = right(theta, table).reshape(8 * size, 8, 128)
    return exchange(waves, Z_PAIRS[size]).reshape(PARTS, size // 2, 8, 128)


def z_back_group(block, index, slopes, table, group):
    size = GROUP_SIZE[group]
    waves = exchange(block.reshape(8 * size, 8, 128), Z_PAIRS[size]).reshape(64 * size, 128)
    field = right(waves, table).reshape(size, 8, 8, 128)
    total = None
    for i in range(size):
        term = field[i] * node_coefficient(GROUP_START[group] + i, index, slopes)
        total = term if total is None else total + term
    return total


def y_chunk(block, table):
    return left(table, block.reshape(128, 128)).reshape(PARTS, 8, 128)


def x_forward_chunk(block, table):
    return right(exchange_groups(block).reshape(128, 128), table)


def x_back_chunk(waves, table):
    return exchange_groups(right(waves, table).reshape(PARTS, 8, 128))


def shell_tile(tile):
    band, grid = lax.axis_index("band"), lax.axis_index("grid")
    second = tile >= 32
    fz = 4 * band + jnp.where(second, 0, tile // 8)
    fz = jnp.where(second & (band == 0), 64, fz)
    ky = 8 * grid + lax.rem(tile, 8)
    fy = jnp.where(ky < 64, ky, ky - 128)
    kx = lanes_of((128, 128))
    fx = jnp.where(kx < 64, kx, kx - 128)
    root = jnp.sqrt((fz * fz + fy * fy + fx * fx).astype(F32))
    shell = lax.broadcasted_iota(jnp.int32, (128, 128), 0).astype(F32)
    return jnp.maximum(1.0 - jnp.abs(root - shell), 0.0)


def start_phi(kernel_table, wide_table, table_pair):
    wide_table[...] = jnp.zeros((480, 128), F32)
    for a in range(NA):
        wide_table[24 * a : 24 * a + NA, : kernel_table.shape[2]] = kernel_table[a]
    high, low = split(wide_table[...])
    table_pair[...] = jnp.concatenate([high, low], axis=1)


def make_phi(first, last, table_pair, phi):
    def step(i, carry):
        wide = table_pair[...]
        tiles = jnp.concatenate([shell_tile(2 * i), shell_tile(2 * i + 1)], axis=1)
        tiles_high, tiles_low = split(tiles)
        values = mm(wide, jnp.concatenate([tiles_high, tiles_high], axis=0)) + mm(wide[:, :128], tiles_low)
        phi[2 * i] = values[:, :128]
        phi[2 * i + 1] = values[:, 128:]
        return carry

    lax.fori_loop(first, last, step, 0)


def mix(group, pair, phi, spec, mixed):
    def step(row, carry):
        sums = [None, None]
        for a in range(NA):
            part = slice(24 * a + 8 * group, 24 * a + 8 * group + 8)
            kernel = phi[8 * pair + row, part]
            kernels = kernel, phi[32 + row, part] if pair == 0 else kernel
            for member in range(2):
                term = kernels[member] * spec[a, pair, member, pl.ds(row, 1), :]
                sums[member] = term if sums[member] is None else sums[member] + term
        for member in range(2):
            at = row + 8 * member
            if group == 2:
                mixed[slot_of(2, pair), pl.ds(at + 16 * (pair % 2), 4, stride=32), :] = sums[member][:4]
            else:
                mixed[slot_of(group, pair), pl.ds(at, 8, stride=16), :] = sums[member]
        return carry

    lax.fori_loop(0, 8, step, 0, unroll=4)


MESH = pl.DeviceIdType.MESH
PARTS = 16
TILES = 40
SLOTS = 10


LINE = 8
SUM_BESIDE, SUM_ACROSS, SUM_PIECES = (4, 3, 5, 1, 7), (2, 6), 2
GIVE_BESIDE, GIVE_ACROSS, GIVE_PIECES = (4, 3, 5, 1, 7), (2, 6), 2


def z_peers(band):
    first = band // LINE * LINE
    return lambda step: first + lax.rem(band + step, LINE)


def partner_of(band):
    return lax.rem(band + LINE, PARTS)


def peers(me):
    return lambda step: lax.rem(me + step, PARTS)


def far_first(axis):
    me = lax.axis_index(axis)
    if axis == "band":
        column, z = me // LINE, lax.rem(me, LINE)
        order = sorted(
            ((dz, dx) for dz in range(LINE) for dx in range(2) if dz or dx), key=lambda d: -(min(d[0], LINE - d[0]) + 2 * d[1])
        )
        return [lax.rem(column + dx, 2) * LINE + lax.rem(z + dz, LINE) for dz, dx in order]
    y, x, core = me // 4, lax.rem(me // 2, 2), lax.rem(me, 2)
    order = sorted(
        ((dy, dx, dc) for dy in range(4) for dx in range(2) for dc in range(2) if dy or dx or dc),
        key=lambda d: -(min(d[0], 4 - d[0]) + d[1]),
    )
    return [lax.rem(y + dy, 4) * 4 + lax.rem(x + dx, 2) * 2 + lax.rem(core + dc, 2) for dy, dx, dc in order]


def greet(barrier):
    band = lax.axis_index("band")
    peer = peers(lax.axis_index("grid"))
    along = z_peers(band)

    def grid_one(step, carry):
        pl.semaphore_signal(barrier, inc=1, device_id={"grid": peer(step)}, device_id_type=MESH)
        return carry

    def band_one(step, carry):
        pl.semaphore_signal(barrier, inc=1, device_id={"band": along(step)}, device_id_type=MESH)
        return carry

    lax.fori_loop(1, LINE, band_one, 0)
    pl.semaphore_signal(barrier, inc=1, device_id={"band": partner_of(band)}, device_id_type=MESH)
    lax.fori_loop(1, PARTS, grid_one, 0)


def remote(src, dst, send_sem, recv_sem, axis, target):
    return pltpu.make_async_remote_copy(
        src_ref=src, dst_ref=dst, send_sem=send_sem, recv_sem=recv_sem, device_id={axis: target}, device_id_type=MESH
    )


def wait_given(copy):
    copy.wait_recv()


def send_chunk(axis, sent, got, slot, send_sem, recv_sem):
    me = lax.axis_index(axis)
    got[slot, me] = sent[slot, me]
    for to in far_first(axis):
        remote(sent.at[slot, to], got.at[slot, me], send_sem, recv_sem.at[slot], axis, to).start()


def wait_chunk(axis, got, slot, send_sem, recv_sem):
    rest = got.at[slot, pl.ds(0, PARTS - 1)]
    remote(rest, rest, send_sem, recv_sem.at[slot], axis, 0).wait_recv()


def wait_sent(axis, sent, send_sem, recv_sem):
    rest = sent.at[:, pl.ds(0, PARTS - 1)]
    remote(rest, rest, send_sem, recv_sem.at[0], axis, 0).wait_send()


def body(
    partial, node_index, node_weight, node_slope, kernel_hbm, tables_hbm, out,
    stage, paired, passed, heard, crossed, index, weights, slopes, kernel_table, table,
    sent_a, got_a, sent_b, got_b, sent_c, got_c, sent_d, got_d,
    wide_table, table_pair, phi, spec, mixed,
    load_sem, send_sem, pair_sem, heard_sem, cross_sem, sem_a, sem_b, sem_c, sem_d, out_sem,
):
    band = lax.axis_index("band")
    barrier = pltpu.get_barrier_semaphore()
    greet(barrier)
    partner, along = partner_of(band), z_peers(band)

    def rows_of(block):
        return pl.ds(pl.multiple_of(8 * block, 8), 8)

    rows = rows_of(band)

    def cut(step, carry):
        pltpu.make_async_copy(partial.at[0, :, rows_of(step), :], stage.at[step], load_sem.at[0]).start()
        return carry

    lax.fori_loop(0, PARTS, cut, 0)
    loads = [
        pltpu.make_async_copy(src, dst, load_sem.at[i + 1])
        for i, (src, dst) in enumerate(
            (
                (kernel_hbm, kernel_table),
                (node_index.at[:, rows, :], index),
                (node_weight.at[:, :, rows, :], weights),
                (node_slope.at[:, :, rows, :], slopes),
                (tables_hbm, table),
            )
        )
    ]
    for load in loads:
        load.start()
    pltpu.make_async_copy(stage, stage, load_sem.at[0]).wait()
    pl.semaphore_wait(barrier, LINE - 1 + 1 + PARTS - 1)

    slot_of_band = lax.rem(band, LINE)

    def piece_of(ref, i):
        return ref.at[pl.ds(8 // SUM_PIECES * i, 8 // SUM_PIECES)]

    pieces = range(SUM_PIECES)

    def to_partner(src, slot, i):
        return remote(
            piece_of(src, i), piece_of(paired.at[slot], i), send_sem.at[0], pair_sem.at[slot, i], "band", partner
        )

    def onward(src, to):
        return remote(src, heard.at[slot_of_band], send_sem.at[6], heard_sem.at[slot_of_band], "band", to)

    for step in SUM_ACROSS:
        to = along(step)
        cross = crossed.at[slot_of_band]
        remote(stage.at[partner_of(to)], cross, send_sem.at[7], cross_sem.at[slot_of_band], "band", to).start()
    for step in SUM_ACROSS:
        onward(stage.at[along(step)], along(step)).start()
    for step in SUM_BESIDE:
        at = along(step)
        for i in pieces:
            to_partner(stage.at[partner_of(at)], lax.rem(at, LINE), i).start()
    loads[0].wait()
    start_phi(kernel_table, wide_table, table_pair)
    make_phi(0, 7, table_pair, phi)
    for count, step in enumerate(SUM_BESIDE):
        to = along(step)
        slot = lax.rem(to, LINE)
        for i in pieces:
            wait_given(to_partner(stage.at[to], slot, i))
            part = pl.ds(8 // SUM_PIECES * i, 8 // SUM_PIECES)
            passed[slot, part] = paired[slot, part] + stage[to, part]
            remote(
                piece_of(passed.at[slot], i),
                piece_of(heard.at[slot_of_band], i),
                send_sem.at[6],
                heard_sem.at[slot_of_band],
                "band",
                to,
            ).start()
        make_phi(7 + count, 8 + count, table_pair, phi)
    own = stage[partner]
    for step in SUM_ACROSS:
        slot = lax.rem(band + LINE - step, LINE)
        cross = crossed.at[slot]
        wait_given(remote(cross, cross, send_sem.at[7], cross_sem.at[slot], "band", partner))
        own = own + crossed[slot]
    passed[slot_of_band] = own
    for i in pieces:
        to_partner(passed.at[slot_of_band], slot_of_band, i).start()
    make_phi(7 + len(SUM_BESIDE), TILES // 2, table_pair, phi)
    for load in loads[1:]:
        load.wait()
    density = stage[band]
    for step in (*SUM_ACROSS, *SUM_BESIDE):
        slot = lax.rem(band + LINE - step, LINE)
        wait_given(remote(heard.at[slot], heard.at[slot], send_sem.at[6], heard_sem.at[slot], "band", partner))
        density = density + heard[slot]
    for i in pieces:
        wait_given(to_partner(passed.at[slot_of_band], slot_of_band, i))
    density = density + paired[slot_of_band]
    tabs = [table.at[i] for i in range(6)]
    y_table, x_table = tabs[4:]
    tabs = {0: (tabs[0], tabs[2]), 1: (tabs[0], tabs[2]), 2: (tabs[1], tabs[3])}

    def z_step(group):
        values = [weights[i] for i in range(4)]
        waves = z_forward_group(density, index[...], values, tabs[group][0][...], group)
        for i, pair in enumerate(pairs_of(group)):
            sent_a[slot_of(group, pair)] = waves[:, i]

    def z_send(slot):
        send_chunk("band", sent_a, got_a, slot, send_sem.at[1], sem_a)

    def y_step(slot):
        wait_chunk("band", got_a, slot, send_sem.at[1], sem_a)
        sent_b[slot] = y_chunk(got_a[slot], y_table[...])
        send_chunk("grid", sent_b, got_b, slot, send_sem.at[2], sem_b)

    def x_step(group, pair):
        slot = slot_of(group, pair)
        wait_chunk("grid", got_b, slot, send_sem.at[2], sem_b)
        waves = x_forward_chunk(got_b[slot], x_table[...])
        if group == 2:
            spec[16:20, pair : pair + 2] = waves.reshape(4, 2, 2, 8, 128)
        else:
            spec[8 * group : 8 * group + 8, pair] = waves.reshape(8, 2, 8, 128)

    def x_back_step(group, pair):
        slot = slot_of(group, pair)
        sent_c[slot] = x_back_chunk(mixed[slot], x_table[...])
        send_chunk("grid", sent_c, got_c, slot, send_sem.at[3], sem_c)

    def y_back_step(group, pair):
        slot = slot_of(group, pair)
        wait_chunk("grid", got_c, slot, send_sem.at[3], sem_c)
        sent_d[slot] = y_chunk(got_c[slot], y_table[...])
        send_chunk("band", sent_d, got_d, slot, send_sem.at[4], sem_d)

    def z_back_step(group):
        blocks = []
        for pair in pairs_of(group):
            slot = slot_of(group, pair)
            wait_chunk("band", got_d, slot, send_sem.at[4], sem_d)
            blocks.append(got_d[slot][:, None])
        block = jnp.concatenate(blocks, axis=1)
        return z_back_group(block, index[...], [slopes[i] for i in range(4)], tabs[group][1][...], group)

    def mix_step(group, pair):
        mix(group, pair, phi, spec, mixed)

    z_step(2)
    z_send(0)
    z_step(0)
    z_send(1)
    z_step(1)
    for slot in range(2, SLOTS):
        z_send(slot)
    y, x, xb, yb = y_step, x_step, x_back_step, y_back_step
    m = mix_step
    plan = (
        (y, 0), (y, 1), (y, 2), (y, 3), (x, 2, 0), (y, 4), (x, 0, 0), (y, 5), (x, 1, 0),
        (m, 0, 0), (xb, 0, 0), (m, 1, 0), (xb, 1, 0), (y, 6), (m, 2, 0), (x, 0, 1), (y, 7), (x, 1, 1),
        (m, 0, 1), (xb, 0, 1), (y, 8), (y, 9), (m, 1, 1), (xb, 1, 1), (m, 2, 1), (xb, 2, 0),
        (x, 2, 2), (yb, 0, 0), (x, 0, 2), (yb, 1, 0), (x, 1, 2),
        (m, 0, 2), (xb, 0, 2), (yb, 0, 1), (m, 1, 2), (xb, 1, 2), (m, 2, 2), (x, 0, 3), (x, 1, 3),
        (m, 0, 3), (xb, 0, 3), (yb, 1, 1), (m, 1, 3), (xb, 1, 3), (yb, 2, 0), (m, 2, 3), (xb, 2, 2),
        (yb, 0, 2), (yb, 1, 2), (yb, 0, 3), (yb, 1, 3), (yb, 2, 2),
    )
    for step, *what in plan:
        step(*what)
    out[:, rows, :] = z_back_step(0) + z_back_step(1) + z_back_step(2)

    given = range(GIVE_PIECES)

    def give(block, i, target):
        piece = out.at[pl.ds(8 // GIVE_PIECES * i, 8 // GIVE_PIECES), rows_of(block), :]
        return remote(piece, piece, send_sem.at[5], out_sem.at[block, i], "band", target)

    for to in (partner, *[along(step) for step in (*GIVE_BESIDE, *GIVE_ACROSS)]):
        for i in given:
            give(band, i, to).start()
    for count, step in enumerate(GIVE_BESIDE):
        origin = along(LINE - step)
        for i in given:
            wait_given(give(origin, i, partner))
            give(origin, i, partner).start()
        if count == 1:
            for i in given:
                wait_given(give(partner, i, partner))
                for across in GIVE_ACROSS:
                    give(partner, i, along(across)).start()
    for step in GIVE_ACROSS:
        for i in given:
            wait_given(give(along(LINE - step), i, partner))
    for step in (*GIVE_BESIDE, *GIVE_ACROSS):
        for i in given:
            wait_given(give(partner_of(along(LINE - step)), i, partner))
    wait_sent("grid", sent_b, send_sem.at[2], sem_b)
    wait_sent("grid", sent_c, send_sem.at[3], sem_c)
    wait_sent("band", sent_a, send_sem.at[1], sem_a)
    wait_sent("band", sent_d, send_sem.at[4], sem_d)
    rest = passed.at[pl.ds(0, len(SUM_BESIDE) + 1)]
    remote(rest, rest, send_sem.at[0], pair_sem.at[0, 0], "band", partner).wait_send()
    rest = passed.at[pl.ds(0, LINE - 1)]
    remote(rest, rest, send_sem.at[6], heard_sem.at[0], "band", partner).wait_send()
    rest = crossed.at[pl.ds(0, len(SUM_ACROSS))]
    remote(rest, rest, send_sem.at[7], cross_sem.at[0], "band", partner).wait_send()
    rest = stage.at[pl.ds(0, PARTS - 1)]
    remote(rest, rest, send_sem.at[5], out_sem.at[0, 0], "band", partner).wait_send()


BLOCKS = (SLOTS, PARTS, 8, 128)


def per_device(partial_density, node_index, node_weight, node_slope, kernel_table):
    constants = jnp.asarray(tables())
    args = [partial_density, node_index, node_weight, node_slope, kernel_table, constants]
    anywhere = pl.BlockSpec(memory_space=pl.ANY)
    vmem = pltpu.VMEM
    return pl.pallas_call(
        body,
        out_shape=pltpu.VMEM((8, N, N), F32),
        in_specs=[anywhere] * len(args),
        out_specs=pl.BlockSpec(memory_space=pltpu.VMEM),
        scratch_shapes=[
            vmem((PARTS, 8, 8, 128), F32),
            *[vmem((LINE, 8, 8, 128), F32)] * 4,
            vmem((8, 8, 128), jnp.int32),
            vmem((4, 8, 8, 128), F32),
            vmem((4, 8, 8, 128), F32),
            vmem(kernel_table.shape, F32),
            vmem(constants.shape, constants.dtype),
            *[vmem(BLOCKS, F32)] * 8,
            vmem((480, 128), F32),
            vmem((480, 256), BF16),
            vmem((TILES, 480, 128), F32),
            vmem((NA, 4, 2, 8, 128), F32),
            vmem((SLOTS, 128, 128), F32),
            pltpu.SemaphoreType.DMA((6,)),
            pltpu.SemaphoreType.DMA((8,)),
            pltpu.SemaphoreType.DMA((LINE, SUM_PIECES)),
            pltpu.SemaphoreType.DMA((LINE,)),
            pltpu.SemaphoreType.DMA((LINE,)),
            *[pltpu.SemaphoreType.DMA((SLOTS,))] * 4,
            pltpu.SemaphoreType.DMA((PARTS, GIVE_PIECES)),
        ],
        compiler_params=pltpu.CompilerParams(
            collective_id=0, has_side_effects=True, vmem_limit_bytes=60000 * 1024
        ),
    )(*args)


def solution(mesh):
    placed = (
        P("band", "grid", None, None),
        P("grid", None, None),
        P(None, "grid", None, None),
        P(None, "grid", None, None),
        P(),
    )
    return jax.shard_map(
        per_device, mesh=mesh, in_specs=placed, out_specs=P("grid", None, None), check_vma=False
    )
```
